16 devices in a mesh: tp: 2 (over z), dp: 8 (over y, x, core).
Axes of the slice: x: 2, y: 2, z: 2, core: 2. Of those that a mesh axis runs over, the one named last changes fastest.
Arguments:
- x_saved: bfloat16 [8, 1536, 1024], P('dp', 'tp')
- dy_out: bfloat16 [8, 1536, 1024], P('dp', 'tp')
- ln_params: float32 [4, 1024], replicated
- w_qkv: bfloat16 [1024, 16, 3, 64], P(None, 'tp')
- w_out: bfloat16 [1024, 1024], P('tp')
- w_up: bfloat16 [1024, 4096], P(None, 'tp')
- w_down: bfloat16 [4096, 1024], P('tp')
Outputs:
- output 1: bfloat16 [8, 1536, 1024], P('dp', 'tp')
- output 2: float32 [4, 1024], replicated
- output 3: float32 [1024, 16, 3, 64], P('dp', 'tp')
- output 4: float32 [1024, 1024], P(('tp', 'dp'))
- output 5: float32 [1024, 4096], P('dp', 'tp')
- output 6: float32 [4096, 1024], P(('tp', 'dp'))
All inputs are finite; a program needn't handle non-finite values.
Results may differ from the reference program's by a relative error of at most 0.00985815.
Values are sent between devices in bfloat16 or wider.
A program may use at most 1 GiB of HBM per device.

```python
import jax
import jax.numpy as jnp
from jax import lax

NUM_SEQS = 8
SEQ_LEN = 1536
D_MODEL = 1024
NUM_HEADS = 16
KV_HEADS = 16
HEAD_DIM = 64
FF_DIM = 4096
Q_PER_GROUP = NUM_HEADS // KV_HEADS
NORM_EPS = 1e-5
ROPE_BASE = 10000.0


def layer_norm(x_rows, norm_gain, norm_shift):
    row_mean = jnp.mean(x_rows, axis=-1, keepdims=True)
    centered = x_rows - row_mean
    row_var = jnp.mean(centered * centered, axis=-1, keepdims=True)
    return (centered * lax.rsqrt(row_var + NORM_EPS) * norm_gain + norm_shift).astype(jnp.bfloat16)


def rope_tables(positions):
    half_dim = HEAD_DIM // 2
    inv_freq = ROPE_BASE ** (-2.0 * jnp.arange(half_dim, dtype=jnp.float32) / HEAD_DIM)
    angles = positions.astype(jnp.float32)[:, None] * inv_freq[None, :]
    return jnp.cos(angles), jnp.sin(angles)


def apply_rope(tensor, cos_t, sin_t):
    half_dim = tensor.shape[-1] // 2
    t_f32 = tensor.astype(jnp.float32)
    lo_half = t_f32[..., :half_dim]
    hi_half = t_f32[..., half_dim:]
    return jnp.concatenate([lo_half * cos_t - hi_half * sin_t, hi_half * cos_t + lo_half * sin_t], axis=-1).astype(jnp.bfloat16)


def attention(qkv_proj):
    positions = jnp.arange(SEQ_LEN)
    cos_t, sin_t = rope_tables(positions)
    rotated = apply_rope(qkv_proj[:, :, :Q_PER_GROUP + 1, :], cos_t[:, None, None, :], sin_t[:, None, None, :])
    query_rot = rotated[:, :, :Q_PER_GROUP, :]
    key_rot = rotated[:, :, Q_PER_GROUP, :]
    values = qkv_proj[:, :, Q_PER_GROUP + 1, :]
    scores = jnp.einsum('tgqh,sgh->gqts', query_rot.astype(jnp.float32), key_rot.astype(jnp.float32)) * (HEAD_DIM ** -0.5)
    causal = positions[:, None] >= positions[None, :]
    attn_probs = jax.nn.softmax(jnp.where(causal, scores, -1e30), axis=-1).astype(jnp.bfloat16)
    return jnp.einsum('gqts,sgh->tgqh', attn_probs.astype(jnp.float32), values.astype(jnp.float32)).astype(jnp.bfloat16)


def layer_forward(x_seq, ln_params, w_qkv, w_out, w_up, w_down):
    x_f32 = x_seq.astype(jnp.float32)
    h_attn = layer_norm(x_f32, ln_params[0], ln_params[1])
    h_mlp = layer_norm(x_f32, ln_params[2], ln_params[3])
    qkv_proj = jnp.dot(h_attn.astype(jnp.float32), w_qkv.reshape(D_MODEL, -1), preferred_element_type=jnp.float32).astype(jnp.bfloat16)
    context = attention(qkv_proj.reshape(SEQ_LEN, KV_HEADS, Q_PER_GROUP + 2, HEAD_DIM))
    attn_out = jnp.dot(context.reshape(SEQ_LEN, NUM_HEADS * HEAD_DIM).astype(jnp.float32), w_out, preferred_element_type=jnp.float32)
    hidden = jnp.dot(h_mlp.astype(jnp.float32), w_up, preferred_element_type=jnp.float32).astype(jnp.bfloat16)
    gelu_out = jax.nn.gelu(hidden.astype(jnp.float32), approximate=False).astype(jnp.bfloat16)
    mlp_out = jnp.dot(gelu_out.astype(jnp.float32), w_down, preferred_element_type=jnp.float32)
    return x_f32 + attn_out + mlp_out


def setup_inputs(seed: int = 0) -> dict:
    key_list = jax.random.split(jax.random.key(seed), 8)
    act_shape = (NUM_SEQS, SEQ_LEN, D_MODEL)
    x_saved = jax.random.normal(key_list[0], act_shape, jnp.float32)
    shared_dir = jax.random.normal(key_list[1], (NUM_SEQS, 1, D_MODEL), jnp.float32)
    dy_out = 0.6 * shared_dir + 0.8 * jax.random.normal(key_list[2], act_shape, jnp.float32)
    ln_base = jnp.array([1.0, 0.0, 1.0, 0.0], jnp.float32)[:, None]
    ln_spread = jnp.array([0.3, 0.5, 0.3, 0.5], jnp.float32)[:, None]
    ln_params = ln_base + ln_spread * jax.random.normal(key_list[3], (4, D_MODEL), jnp.float32)
    w_qkv = jax.random.normal(key_list[4], (D_MODEL, KV_HEADS, Q_PER_GROUP + 2, HEAD_DIM), jnp.float32) * D_MODEL ** -0.5
    w_out = jax.random.normal(key_list[5], (NUM_HEADS * HEAD_DIM, D_MODEL), jnp.float32) * (NUM_HEADS * HEAD_DIM) ** -0.5
    w_up = jax.random.normal(key_list[6], (D_MODEL, FF_DIM), jnp.float32) * D_MODEL ** -0.5
    w_down = jax.random.normal(key_list[7], (FF_DIM, D_MODEL), jnp.float32) * FF_DIM ** -0.5
    return {'x_saved': x_saved.astype(jnp.bfloat16), 'dy_out': dy_out.astype(jnp.bfloat16), 'ln_params': ln_params, 'w_qkv': w_qkv.astype(jnp.bfloat16), 'w_out': w_out.astype(jnp.bfloat16), 'w_up': w_up.astype(jnp.bfloat16), 'w_down': w_down.astype(jnp.bfloat16)}


def reference(x_saved, dy_out, ln_params, w_qkv, w_out, w_up, w_down):
    weights = (ln_params, w_qkv.astype(jnp.float32), w_out.astype(jnp.float32), w_up.astype(jnp.float32), w_down.astype(jnp.float32))

    def seq_step(grad_sums, seq_pair):
        x_seq, dy_seq = seq_pair
        _, pull_back = jax.vjp(layer_forward, x_seq, *weights)
        grads = pull_back(dy_seq.astype(jnp.float32))
        return tuple(grad_total + grad_part for grad_total, grad_part in zip(grad_sums, grads[1:])), grads[0]

    zero_sums = tuple(jnp.zeros_like(weight) for weight in weights)
    grad_sums, grad_x = lax.scan(seq_step, zero_sums, (x_saved, dy_out))
    return (grad_x, grad_sums[0], grad_sums[1], grad_sums[2], grad_sums[3], grad_sums[4])
```

```python
import functools

import jax
import jax.numpy as jnp
from jax import lax
from jax.experimental import pallas as pl
from jax.experimental.pallas import tpu as pltpu
from jax.sharding import PartitionSpec as P

NORM_EPS = 1e-5
ROPE_BASE = 10000.0
BF = jnp.bfloat16
F32 = jnp.float32
SQRT_HALF = 0.7071067811865476
INV_SQRT_2PI = 0.3989422804014327
VMEM_LIMIT = 60 * 1024 * 1024


def dot(a, b, ca, cb):
    return lax.dot_general(a, b, (((ca,), (cb,)), ((), ())), preferred_element_type=F32)


def params():
    return pltpu.CompilerParams(vmem_limit_bytes=VMEM_LIMIT)


def cost(flops, nbytes, trans=0):
    return pl.CostEstimate(flops=int(flops), bytes_accessed=int(nbytes), transcendentals=int(trans))


def normalized(x):
    cen = x - jnp.mean(x, axis=-1, keepdims=True)
    rstd = lax.rsqrt(jnp.mean(cen * cen, axis=-1, keepdims=True) + NORM_EPS)
    return cen * rstd, rstd


def norm_m_kernel(c_ref, x_ref, ln_ref, hm_ref, hk_ref, hs_ref):
    hm = (normalized(x_ref[...].astype(F32))[0] * ln_ref[2:3, :] + ln_ref[3:4, :]).astype(BF)
    hm_ref[...] = hm
    n = hm.shape[1] // 8
    for j in range(4):
        even, odd = hm[:, 2 * j * n:(2 * j + 1) * n].T, hm[:, (2 * j + 1) * n:(2 * j + 2) * n].T
        hk_ref[j * n:(j + 1) * n, :] = jnp.where(c_ref[0] == 0, even, odd)
        hs_ref[j * n:(j + 1) * n, :] = jnp.where(c_ref[0] == 0, odd, even)


def norm_m(core, x, ln, bt=256):
    rows, d = x.shape
    tok = pl.BlockSpec((bt, d), lambda i, c: (i, 0))
    return pl.pallas_call(
        norm_m_kernel,
        grid_spec=pltpu.PrefetchScalarGridSpec(
            num_scalar_prefetch=1,
            grid=(rows // bt,),
            in_specs=[tok, pl.BlockSpec((4, d), lambda i, c: (0, 0))],
            out_specs=[tok] + [pl.BlockSpec((d // 2, bt), lambda i, c: (0, i))] * 2,
        ),
        out_shape=[jax.ShapeDtypeStruct((rows, d), BF)] + [jax.ShapeDtypeStruct((d // 2, rows), BF)] * 2,
        compiler_params=params(),
        cost_estimate=cost(3e9, rows * d * 6),
        name="norm_m",
    )(core, x, ln)


def norm_a_kernel(c_ref, xl_ref, xr_ref, ln_ref, ha_ref, hk_ref, hs_ref, *, nb):
    def run(x_ref):
        ha = (normalized(x_ref[...].astype(F32))[0] * ln_ref[0:1, :] + ln_ref[1:2, :]).astype(BF)
        ha_ref[...] = ha
        n = ha.shape[1] // 8
        for j in range(4):
            even, odd = ha[:, 2 * j * n:(2 * j + 1) * n], ha[:, (2 * j + 1) * n:(2 * j + 2) * n]
            hk_ref[:, j * n:(j + 1) * n] = jnp.where(c_ref[0] == 0, even, odd)
            hs_ref[:, j * n:(j + 1) * n] = jnp.where(c_ref[0] == 0, odd, even)

    pl.when(pl.program_id(0) < nb)(lambda: run(xl_ref))
    pl.when(pl.program_id(0) >= nb)(lambda: run(xr_ref))


def norm_a(core, x_loc, x_rem, ln, bt=256):
    rows, d = x_loc.shape
    nb = rows // bt
    tok = lambda w: pl.BlockSpec((bt, w), lambda i, c: (i, 0))
    return pl.pallas_call(
        functools.partial(norm_a_kernel, nb=nb),
        grid_spec=pltpu.PrefetchScalarGridSpec(
            num_scalar_prefetch=1,
            grid=(2 * nb,),
            in_specs=[
                pl.BlockSpec((bt, d), lambda i, c: (jnp.minimum(i, nb - 1), 0)),
                pl.BlockSpec((bt, d), lambda i, c: (jnp.maximum(i - nb, 0), 0)),
                pl.BlockSpec((4, d), lambda i, c: (0, 0)),
            ],
            out_specs=[tok(d), tok(d // 2), tok(d // 2)],
        ),
        out_shape=[jax.ShapeDtypeStruct((2 * rows, w), BF) for w in (d, d // 2, d // 2)],
        compiler_params=params(),
        cost_estimate=cost(6e9, rows * d * 12),
        name="norm_a",
    )(core, x_loc, x_rem, ln)


def attn_kernel(t_ref, qkv_ref, dol_ref, dor_ref, cos_ref, sin_ref, dqkv_ref, ctx_ref, dk_ref, dv_ref, *, bq, hd):
    t = t_ref[0]
    seq = qkv_ref.shape[1]
    half = hd // 2
    part = dol_ref.shape[1]
    cos, sin = cos_ref[...], sin_ref[...]

    def in_order(own, peer):
        return jnp.concatenate([jnp.where(t == 0, own, peer), jnp.where(t == 0, peer, own)], axis=1)

    def place(lo, n):
        slot = t if lo < part else 1 - t
        return pl.ds(pl.multiple_of(slot * part + lo % part, 128), n)

    def rope(v):
        lo, hi = v[:half].astype(F32), v[half:].astype(F32)
        return jnp.concatenate([lo * cos - hi * sin, hi * cos + lo * sin], axis=0).astype(BF)

    def rope_back(d, c, s):
        lo, hi = d[:half].astype(BF).astype(F32), d[half:].astype(BF).astype(F32)
        return jnp.concatenate([lo * c + hi * s, hi * c - lo * s], axis=0).astype(BF)

    scale = hd ** -0.5
    qkv = in_order(qkv_ref[:, :part], qkv_ref[:, part:])
    q_t = rope(qkv[0:hd])
    k_t = rope(qkv[hd:2 * hd])
    v_t = qkv[2 * hd:3 * hd]
    q_t = (q_t.astype(F32) * scale).astype(BF)
    do_t = in_order(dol_ref[...], dor_ref[...])
    q_n, do_n, k_n, v_n = q_t.T, do_t.T, k_t.T, v_t.T
    tri = lax.broadcasted_iota(jnp.int32, (bq, bq), 0) <= lax.broadcasted_iota(jnp.int32, (bq, bq), 1)
    for i in range(seq // bq):
        lo, nk = i * bq, (i + 1) * bq
        blocks = [slice(j * bq, (j + 1) * bq) for j in range(i + 1)]
        q_b, do_b = q_t[:, lo:nk], do_t[:, lo:nk]
        ss = [dot(k_n[b], q_b, 1, 0) for b in blocks]
        ss[i] = jnp.where(tri, ss[i], -1e30)
        m = functools.reduce(jnp.maximum, [jnp.max(s, axis=0, keepdims=True) for s in ss])
        es = [jnp.exp(s - m) for s in ss]
        r = 1.0 / sum(jnp.sum(e, axis=0, keepdims=True) for e in es)
        ps = [e * r for e in es]
        pbs = [p.astype(BF) for p in ps]
        dps = [dot(v_n[b], do_b, 1, 0).astype(BF) for b in blocks]
        delta = sum(jnp.sum(p * d.astype(F32), axis=0, keepdims=True) for p, d in zip(ps, dps))
        dss = [(p * (d.astype(F32) - delta)).astype(BF) for p, d in zip(ps, dps)]
        ctx_ref[:, place(lo, bq)] = sum(dot(v_t[:, b], p, 1, 0) for b, p in zip(blocks, pbs)).astype(BF)
        dq = sum(dot(k_t[:, b], d, 1, 0) for b, d in zip(blocks, dss)) * scale
        dqkv_ref[0:hd, place(lo, bq)] = rope_back(dq, cos[:, lo:nk], sin[:, lo:nk])
        for j, b in enumerate(blocks):
            dv_new = dot(pbs[j], do_n[lo:nk], 1, 0)
            dk_new = dot(dss[j], q_n[lo:nk], 1, 0)
            if j < i:
                dv_ref[b, :] += dv_new
                dk_ref[b, :] += dk_new
            else:
                dv_ref[b, :] = dv_new
                dk_ref[b, :] = dk_new
    dk = rope_back(dk_ref[...].T, cos, sin)
    dv = dv_ref[...].T.astype(BF)
    for lo in (0, part):
        dqkv_ref[hd:2 * hd, place(lo, part)] = dk[:, lo:lo + part]
        dqkv_ref[2 * hd:3 * hd, place(lo, part)] = dv[:, lo:lo + part]


def attention(t, qkv_t, dol, dor, cos_t, sin_t, hd, first, heads, bq=256):
    seq = qkv_t.shape[1]
    part = dol.shape[1]
    const = lambda g, t: (0, 0)
    row = lambda g, t: (g + first, 0)
    mine = lambda g, t: (g, 0)
    return pl.pallas_call(
        functools.partial(attn_kernel, bq=bq, hd=hd),
        grid_spec=pltpu.PrefetchScalarGridSpec(
            num_scalar_prefetch=1,
            grid=(heads,),
            in_specs=[
                pl.BlockSpec((3 * hd, seq), row),
                pl.BlockSpec((hd, part), row),
                pl.BlockSpec((hd, part), row),
                pl.BlockSpec((hd // 2, seq), const),
                pl.BlockSpec((hd // 2, seq), const),
            ],
            out_specs=[pl.BlockSpec((3 * hd, seq), mine), pl.BlockSpec((hd, seq), mine)],
            scratch_shapes=[pltpu.VMEM((seq, hd), F32), pltpu.VMEM((seq, hd), F32)],
        ),
        out_shape=[jax.ShapeDtypeStruct((heads * 3 * hd, seq), BF), jax.ShapeDtypeStruct((heads * hd, seq), BF)],
        compiler_params=params(),
        cost_estimate=cost(heads * 6e9, heads << 20, seq * seq * heads // 2),
        name="attn",
    )(t, qkv_t, dol, dor, cos_t, sin_t)


def gelu_pair(h_ref, dy_ref, wu, wd, rows):
    u = dot(h_ref[rows, :], wu, 1, 0).astype(BF).astype(F32)
    dg = dot(dy_ref[rows, :], wd, 1, 1).astype(BF).astype(F32)
    cdf = 0.5 + 0.5 * lax.erf(u * SQRT_HALF)
    pdf = jnp.exp(-0.5 * u * u) * INV_SQRT_2PI
    return (u * cdf).astype(BF), (dg * (cdf + u * pdf)).astype(BF)


def mlp_own_kernel(h_ref, dy_ref, wu_ref, wd_ref, at_ref, du_ref, dh_ref, acc_ref, *, tc):
    step = pl.program_id(0)
    wu, wd = wu_ref[...], wd_ref[...]
    for k in range(h_ref.shape[0] // tc):
        rows = pl.ds(k * tc, tc)
        a, du = gelu_pair(h_ref, dy_ref, wu, wd, rows)
        at_ref[:, rows] = a.T
        du_ref[0, rows, :] = du
        add = dot(du, wu, 1, 1)

        @pl.when(step == 0)
        def _():
            acc_ref[rows, :] = add

        @pl.when(step > 0)
        def _():
            acc_ref[rows, :] += add

    @pl.when(step == pl.num_programs(0) - 1)
    def _():
        dh_ref[...] = acc_ref[...].astype(BF)


def mlp_own(h, dy, w_up, w_down, n=4, tc=256):
    seq, d = h.shape
    ff = w_up.shape[1]
    fb = ff // n
    full = pl.BlockSpec((seq, d), lambda i: (0, 0))
    return pl.pallas_call(
        functools.partial(mlp_own_kernel, tc=tc),
        grid=(n,),
        in_specs=[full, full, pl.BlockSpec((d, fb), lambda i: (0, i)), pl.BlockSpec((fb, d), lambda i: (i, 0))],
        out_specs=[pl.BlockSpec((fb, seq), lambda i: (i, 0)), pl.BlockSpec((1, seq, fb), lambda i: (i, 0, 0)), full],
        out_shape=[jax.ShapeDtypeStruct((ff, seq), BF), jax.ShapeDtypeStruct((n, seq, fb), BF), jax.ShapeDtypeStruct((seq, d), BF)],
        scratch_shapes=[pltpu.VMEM((seq, d), F32)],
        compiler_params=params(),
        cost_estimate=cost(6 * seq * d * ff, 20 << 20, 2 * seq * ff),
        name="mlp_own",
    )(h, dy, w_up, w_down)


def mlp_peer_kernel(c_ref, h_ref, dyr_ref, dyl_ref, hkl_ref, hsl_ref, hkr_ref, hsr_ref, wu_ref, wd_ref, at_ref, dul_ref,
                    dka_ref, dkb_ref, dsa_ref, dsb_ref, uka_ref, ukb_ref, usa_ref, usb_ref, dh_ref, acc_ref, a_ref, du_ref, *, tc):
    step = pl.program_id(0)
    wu, wd = wu_ref[...], wd_ref[...]
    fb = wu.shape[1]
    m = fb // 2

    @pl.when(step == 0)
    def _():
        acc_ref[...] = jnp.zeros_like(acc_ref)

    for k in range(h_ref.shape[0] // tc):
        rows = pl.ds(k * tc, tc)
        a, du = gelu_pair(h_ref, dyr_ref, wu, wd, rows)
        a_ref[rows, :] = a
        du_ref[rows, :] = du
        acc_ref[rows, :] += dot(du, wu, 1, 1)
    for side, (ra, rb) in ((c_ref[0], (dka_ref, dkb_ref)), (1 - c_ref[0], (dsa_ref, dsb_ref))):
        block = pl.ds(pl.multiple_of(side * m, 128), m)
        g = dot(at_ref[block, :], dyl_ref[...], 1, 0) + dot(a_ref[:, block], dyr_ref[...], 0, 0)
        w = g.shape[1] // 2
        ra[0] = g[:, :w]
        rb[0] = g[:, w:]
    for hl, hr, ra, rb in ((hkl_ref, hkr_ref, uka_ref, ukb_ref), (hsl_ref, hsr_ref, usa_ref, usb_ref)):
        g = dot(hl[...], dul_ref[0], 1, 0) + dot(hr[...], du_ref[...], 1, 0)
        n = g.shape[0] // 4
        for j in range(4):
            ra[0, j] = g[j * n:(j + 1) * n, :m]
            rb[0, j] = g[j * n:(j + 1) * n, m:]

    @pl.when(step == pl.num_programs(0) - 1)
    def _():
        dh_ref[...] = acc_ref[...].astype(BF)


def mlp_peer(core, h, dy_rem, dy_loc, hts, w_up, w_down, at, du, n=4, tc=256):
    seq, d = h.shape
    ff = w_up.shape[1]
    fb = ff // n
    full = lambda r, w: pl.BlockSpec((r, w), lambda i, c: (0, 0))
    dspec = pl.BlockSpec((1, fb // 2, d // 2), lambda i, c: (i, 0, 0))
    uspec = pl.BlockSpec((1, 4, d // 8, fb // 2), lambda i, c: (i, 0, 0, 0))
    return pl.pallas_call(
        functools.partial(mlp_peer_kernel, tc=tc),
        grid_spec=pltpu.PrefetchScalarGridSpec(
            num_scalar_prefetch=1,
            grid=(n,),
            in_specs=[full(seq, d)] * 3 + [full(d // 2, seq)] * 4 + [
                pl.BlockSpec((d, fb), lambda i, c: (0, i)), pl.BlockSpec((fb, d), lambda i, c: (i, 0)),
                pl.BlockSpec((fb, seq), lambda i, c: (i, 0)), pl.BlockSpec((1, seq, fb), lambda i, c: (i, 0, 0))],
            out_specs=[dspec] * 4 + [uspec] * 4 + [full(seq, d)],
            scratch_shapes=[pltpu.VMEM((seq, d), F32), pltpu.VMEM((seq, fb), BF), pltpu.VMEM((seq, fb), BF)],
        ),
        out_shape=[jax.ShapeDtypeStruct((n, fb // 2, d // 2), F32)] * 4
        + [jax.ShapeDtypeStruct((n, 4, d // 8, fb // 2), F32)] * 4 + [jax.ShapeDtypeStruct((seq, d), BF)],
        compiler_params=params(),
        cost_estimate=cost(14 * seq * d * ff, 40 << 20, 2 * seq * ff),
        name="mlp_peer",
    )(core, h, dy_rem, dy_loc, *hts, w_up, w_down, at, du)


def wg_kernel(hk_ref, hs_ref, da_ref, db_ref, ka_ref, sa_ref, kb_ref, sb_ref):
    for h_ref, refs in ((hs_ref, (sa_ref, sb_ref)), (hk_ref, (ka_ref, kb_ref))):
        for d_ref, o_ref in zip((da_ref, db_ref), refs):
            g = dot(d_ref[...], h_ref[...], 1, 0)
            n = g.shape[1] // 4
            for j in range(4):
                o_ref[j] = g[:, j * n:(j + 1) * n]


def qkv_grads(h_keep, h_send, dq_a, dq_b):
    seq, cols = h_keep.shape
    n = dq_a.shape[0]
    vm = pl.BlockSpec(memory_space=pltpu.VMEM)
    return pl.pallas_call(
        wg_kernel,
        in_specs=[vm] * 4,
        out_specs=[vm] * 4,
        out_shape=[jax.ShapeDtypeStruct((4, n, cols // 4), F32)] * 4,
        compiler_params=params(),
        cost_estimate=cost(8 * cols * seq * n, 12 << 20),
        name="wg",
    )(h_keep, h_send, dq_a, dq_b)


def wo_kernel(c_ref, *refs):
    ctx_refs, (dyl_ref, dyr_ref, ka_ref, sa_ref, kb_ref, sb_ref) = refs[:4], refs[4:]
    hd = ctx_refs[0].shape[0] // 2
    part = dyl_ref.shape[0]
    for flip, oa_ref, ob_ref in ((1, sa_ref, sb_ref), (0, ka_ref, kb_ref)):
        want = c_ref[0] if flip == 0 else 1 - c_ref[0]
        cx = jnp.concatenate([jnp.where(want == 0, r[:hd, :], r[hd:, :]) for r in ctx_refs], axis=0)
        g = dot(cx[:, :part], dyl_ref[...], 1, 0) + dot(cx[:, part:], dyr_ref[...], 1, 0)
        m = g.shape[1] // 2
        for j in range(4):
            oa_ref[j] = g[j * hd:(j + 1) * hd, :m]
            ob_ref[j] = g[j * hd:(j + 1) * hd, m:]


def out_grads(core, ctxs, dy_loc, dy_rem):
    hd, d = ctxs[0].shape[0] // 2, dy_loc.shape[1]
    vm = pl.BlockSpec(memory_space=pltpu.VMEM)
    return pl.pallas_call(
        wo_kernel,
        in_specs=[pl.BlockSpec(memory_space=pltpu.SMEM)] + [vm] * 6,
        out_specs=[vm] * 4,
        out_shape=[jax.ShapeDtypeStruct((4, hd, d // 2), F32)] * 4,
        compiler_params=params(),
        cost_estimate=cost(16 * hd * d * ctxs[0].shape[1], 6 << 20),
        name="wo",
    )(core, *ctxs, dy_loc, dy_rem)


def fin_kernel(*refs, groups):
    dq_refs, (w_ref, x_ref, dhm_ref, ln_ref, dx_ref, sum_ref) = refs[:groups], refs[groups:]
    n = dq_refs[0].shape[0]
    dha = sum(dot(r[...], w_ref[g * n:(g + 1) * n, :], 0, 0) for g, r in enumerate(dq_refs))
    dha = dha.astype(BF).astype(F32)
    dhm = dhm_ref[...].astype(F32)
    xh, _ = normalized(x_ref[...].astype(F32))
    dx_ref[...] = (dha * ln_ref[0:1, :] + dhm * ln_ref[2:3, :]).astype(BF)
    parts = [dha * xh, dha, dhm * xh, dhm]
    new = jnp.concatenate([jnp.sum(p, axis=0, keepdims=True) for p in parts], axis=0)

    @pl.when(pl.program_id(0) == 0)
    def _():
        sum_ref[...] = new

    @pl.when(pl.program_id(0) > 0)
    def _():
        sum_ref[...] += new


def finish(peer, dqs, w_t, x, dhm, ln, bt=256):
    rows, d = x.shape
    n = dqs[0].shape[0]
    off = rows // bt if peer else 0
    tok = lambda i: (i, 0)
    full = lambda i: (0, 0)
    return pl.pallas_call(
        functools.partial(fin_kernel, groups=len(dqs)),
        grid=(rows // bt,),
        in_specs=[pl.BlockSpec((n, bt), lambda i: (0, i + off)) for _ in dqs] + [
            pl.BlockSpec(w_t.shape, full), pl.BlockSpec((bt, d), tok), pl.BlockSpec((bt, d), tok), pl.BlockSpec(ln.shape, full)],
        out_specs=[pl.BlockSpec((bt, d), tok), pl.BlockSpec((4, d), full)],
        out_shape=[jax.ShapeDtypeStruct((rows, d), BF), jax.ShapeDtypeStruct((4, d), F32)],
        compiler_params=params(),
        cost_estimate=cost(2 * rows * d * w_t.shape[0], 8 << 20, rows),
        name="fin",
    )(*dqs, w_t, x, dhm, ln)


def grad_x_kernel(x_ref, dy_ref, a_ref, b_ref, o_ref):
    dxh = a_ref[...].astype(F32) + b_ref[...].astype(F32)
    xh, rstd = normalized(x_ref[...].astype(F32))
    dx = rstd * (dxh - jnp.mean(dxh, -1, keepdims=True) - xh * jnp.mean(dxh * xh, -1, keepdims=True))
    o_ref[...] = (dy_ref[...].astype(F32) + dx).astype(BF)


def grad_x_of(x, dy, a, b, bt=256):
    rows, d = x.shape
    tok = pl.BlockSpec((bt, d), lambda i: (i, 0))
    return pl.pallas_call(
        grad_x_kernel,
        grid=(rows // bt,),
        in_specs=[tok] * 4,
        out_specs=tok,
        out_shape=jax.ShapeDtypeStruct((rows, d), BF),
        compiler_params=params(),
        cost_estimate=cost(1e9, rows * d * 10, rows),
        name="grad_x",
    )(x, dy, a, b)


def solution(mesh):
    dp = mesh.shape["dp"]
    tp = mesh.shape["tp"]

    def swap(v, bit):
        return lax.ppermute(v, "dp", [(i, i ^ bit) for i in range(dp)])

    def swap_tp(v):
        return lax.ppermute(v, "tp", [(i, i ^ 1) for i in range(tp)])

    def take(v, idx, axis):
        return lax.dynamic_index_in_dim(v, idx, axis, keepdims=False)

    def after(v, *deps):
        return lax.optimization_barrier((v,) + deps)[0]

    def local_step(x_loc, dy_loc, ln_params, w_qkv, w_out, w_up, w_down):
        x_loc, dy_loc = x_loc[0], dy_loc[0]
        half, d = x_loc.shape
        seq = half * tp
        heads, hd = w_qkv.shape[1], w_qkv.shape[3]
        t = lax.axis_index("tp")
        me = lax.axis_index("dp")
        c, xx, yy = me % 2, (me // 2) % 2, me // 4
        t1, c1 = t.astype(jnp.int32)[None], c.astype(jnp.int32)[None]

        x_rem = swap_tp(x_loc)
        dy_rem = swap_tp(dy_loc)

        w_t = w_qkv.transpose(1, 2, 3, 0).reshape(heads * 3 * hd, d)
        inv_freq = ROPE_BASE ** (-2.0 * jnp.arange(hd // 2, dtype=F32) / hd)
        ang = inv_freq[:, None] * jnp.arange(seq).astype(F32)[None, :]
        cos_t, sin_t = jnp.cos(ang), jnp.sin(ang)

        hm_loc, hk_loc, hs_loc = norm_m(c1, x_loc, ln_params)
        at_loc, du_loc, dhm_loc = mlp_own(hm_loc, dy_loc, w_up, w_down)
        dctx_loc = dot(w_out, dy_loc, 1, 1).astype(BF)

        x_rem = after(x_rem, dhm_loc, dctx_loc, cos_t, sin_t, w_t)
        hm_rem, hk_rem, hs_rem = norm_m(c1, x_rem, ln_params)
        h_a, h_keep, h_send = norm_a(c1, x_loc, x_rem, ln_params)
        qkv_t = dot(w_t, h_a, 1, 1).astype(BF)

        dy_rem = after(dy_rem, qkv_t, h_keep, hm_rem)
        dka, dkb, dsa, dsb, uka, ukb, usa, usb, dhm_rem = mlp_peer(
            c1, hm_rem, dy_rem, dy_loc, (hk_loc, hs_loc, hk_rem, hs_rem), w_up, w_down, at_loc, du_loc)
        dctx_rem = dot(w_out, after(dy_rem, dhm_rem), 1, 1).astype(BF)

        def half_sum(keep, got, idx, axis):
            send = take(keep, 1 - idx, axis) + take(got, 1 - idx, axis)
            return take(keep, idx, axis) + take(got, idx, axis), send

        class Scatter:
            def __init__(self, keep, send, x_first, lead=0):
                n = lead
                self.ways = ((xx, n + 1, 2), (yy, n, 4)) if x_first else ((yy, n, 4), (xx, n, 2))
                got = swap(send, 1)
                self.keep, self.got = (v.reshape(v.shape[:n] + (2, 2) + v.shape[n + 1:]) for v in (keep, got))

            def step(self, *deps):
                (idx, axis, bit), self.ways = self.ways[0], self.ways[1:]
                keep = after(self.keep, *deps) if deps else self.keep
                self.keep, send = half_sum(keep, self.got, idx, axis)
                self.got = swap(send, bit)
                return send

            def end(self):
                return self.keep + self.got

        def pair(ka, sa, kb, sb, lead=0):
            return [Scatter(ka, sa, True, lead), Scatter(kb, sb, False, lead)]

        def steps(rs, *deps):
            return [r.step(*deps) for r in rs]

        down = pair(dka, dsa, dkb, dsb)
        up = pair(uka, usa, ukb, usb, 1)
        dqs, ctxs = [], []

        def attend(k, *deps):
            dq, ctx = attention(t1, after(qkv_t, *deps), dctx_loc, dctx_rem, cos_t, sin_t, hd, 2 * k, 2)
            dqs.append(dq)
            ctxs.append(ctx)

        s = steps(down)
        attend(0, dhm_rem, *s)
        s = steps(up, dqs[0])
        attend(1, *s)
        g = qkv_grads(h_keep, h_send, dqs[0], dqs[1])
        q1 = pair(*g)
        s = steps(down, dqs[1])
        attend(2, *s, *g)
        s = steps(up, dqs[2]) + steps(q1, dqs[2])
        attend(3, *s)
        s = steps(q1, dqs[3])
        dq3 = after(dqs[3], *s)
        g = qkv_grads(h_keep, h_send, dqs[2], dq3)
        q2 = pair(*g)
        dq3 = after(dq3, *g)
        dxh_send, sum_rem = finish(True, dqs[:3] + [dq3], w_t, x_rem, dhm_rem, ln_params)
        dxh_got = swap_tp(dxh_send)
        g = out_grads(c1, ctxs, dy_loc, after(dy_rem, dxh_send))
        wo = pair(*g)
        s = steps(q2, g[0])
        dq3 = after(dq3, *s)
        dxh_keep, sum_loc = finish(False, dqs[:3] + [dq3], w_t, x_loc, dhm_loc, ln_params)
        steps(wo, dxh_keep)
        steps(q2, dxh_keep)
        steps(wo)

        grad_x = grad_x_of(x_loc, dy_loc, dxh_keep, dxh_got)[None]

        sums = sum_rem + sum_loc
        sums = sums + swap_tp(sums)
        for bit in (1, 2, 4):
            sums = sums + swap(sums, bit)

        g_wdown = jnp.concatenate([r.end() for r in down], axis=1)
        g_wup = jnp.stack([r.end() for r in up], axis=2).transpose(1, 0, 2, 3).reshape(d // dp, -1)
        g_wqkv = jnp.concatenate([r.end() for r in q1 + q2], axis=0).reshape(heads, 3, hd, d // dp).transpose(3, 0, 1, 2)
        g_wout = jnp.concatenate([r.end() for r in wo], axis=1)
        return grad_x, sums, g_wqkv, g_wout, g_wup, g_wdown

    return jax.shard_map(
        local_step,
        mesh=mesh,
        in_specs=(P("dp", "tp"), P("dp", "tp"), P(), P(None, "tp"), P("tp"), P(None, "tp"), P("tp")),
        out_specs=(P("dp", "tp"), P(), P("dp", "tp"), P(("tp", "dp")), P("dp", "tp"), P(("tp", "dp"))),
        check_vma=False,
    )
```

```python
import functools

import jax
import jax.numpy as jnp
from jax import lax
from jax.experimental import pallas as pl
from jax.experimental.pallas import tpu as pltpu
from jax.sharding import PartitionSpec as P

NORM_EPS = 1e-5
ROPE_BASE = 10000.0
BF = jnp.bfloat16
F32 = jnp.float32
SQRT_HALF = 0.7071067811865476
INV_SQRT_2PI = 0.3989422804014327
VMEM_LIMIT = 60 * 1024 * 1024


def dot(a, b, ca, cb):
    return lax.dot_general(a, b, (((ca,), (cb,)), ((), ())), preferred_element_type=F32)


def params():
    return pltpu.CompilerParams(vmem_limit_bytes=VMEM_LIMIT)


def cost(flops, nbytes, trans=0):
    return pl.CostEstimate(flops=int(flops), bytes_accessed=int(nbytes), transcendentals=int(trans))


def normalized(x):
    cen = x - jnp.mean(x, axis=-1, keepdims=True)
    rstd = lax.rsqrt(jnp.mean(cen * cen, axis=-1, keepdims=True) + NORM_EPS)
    return cen * rstd, rstd


def norm_m_kernel(c_ref, x_ref, ln_ref, hm_ref, hk_ref, hs_ref):
    hm = (normalized(x_ref[...].astype(F32))[0] * ln_ref[2:3, :] + ln_ref[3:4, :]).astype(BF)
    hm_ref[...] = hm
    n = hm.shape[1] // 8
    for j in range(4):
        even, odd = hm[:, 2 * j * n:(2 * j + 1) * n].T, hm[:, (2 * j + 1) * n:(2 * j + 2) * n].T
        hk_ref[j * n:(j + 1) * n, :] = jnp.where(c_ref[0] == 0, even, odd)
        hs_ref[j * n:(j + 1) * n, :] = jnp.where(c_ref[0] == 0, odd, even)


def norm_m(core, x, ln, bt=256):
    rows, d = x.shape
    tok = pl.BlockSpec((bt, d), lambda i, c: (i, 0))
    return pl.pallas_call(
        norm_m_kernel,
        grid_spec=pltpu.PrefetchScalarGridSpec(
            num_scalar_prefetch=1,
            grid=(rows // bt,),
            in_specs=[tok, pl.BlockSpec((4, d), lambda i, c: (0, 0))],
            out_specs=[tok] + [pl.BlockSpec((d // 2, bt), lambda i, c: (0, i))] * 2,
        ),
        out_shape=[jax.ShapeDtypeStruct((rows, d), BF)] + [jax.ShapeDtypeStruct((d // 2, rows), BF)] * 2,
        compiler_params=params(),
        cost_estimate=cost(3e9, rows * d * 6),
        name="norm_m",
    )(core, x, ln)


def norm_a_kernel(c_ref, xl_ref, xr_ref, ln_ref, ha_ref, hk_ref, hs_ref, *, nb):
    def run(x_ref):
        ha = (normalized(x_ref[...].astype(F32))[0] * ln_ref[0:1, :] + ln_ref[1:2, :]).astype(BF)
        ha_ref[...] = ha
        n = ha.shape[1] // 8
        for j in range(4):
            even, odd = ha[:, 2 * j * n:(2 * j + 1) * n], ha[:, (2 * j + 1) * n:(2 * j + 2) * n]
            hk_ref[:, j * n:(j + 1) * n] = jnp.where(c_ref[0] == 0, even, odd)
            hs_ref[:, j * n:(j + 1) * n] = jnp.where(c_ref[0] == 0, odd, even)

    pl.when(pl.program_id(0) < nb)(lambda: run(xl_ref))
    pl.when(pl.program_id(0) >= nb)(lambda: run(xr_ref))


def norm_a(core, x_loc, x_rem, ln, bt=256):
    rows, d = x_loc.shape
    nb = rows // bt
    tok = lambda w: pl.BlockSpec((bt, w), lambda i, c: (i, 0))
    return pl.pallas_call(
        functools.partial(norm_a_kernel, nb=nb),
        grid_spec=pltpu.PrefetchScalarGridSpec(
            num_scalar_prefetch=1,
            grid=(2 * nb,),
            in_specs=[
                pl.BlockSpec((bt, d), lambda i, c: (jnp.minimum(i, nb - 1), 0)),
                pl.BlockSpec((bt, d), lambda i, c: (jnp.maximum(i - nb, 0), 0)),
                pl.BlockSpec((4, d), lambda i, c: (0, 0)),
            ],
            out_specs=[tok(d), tok(d // 2), tok(d // 2)],
        ),
        out_shape=[jax.ShapeDtypeStruct((2 * rows, w), BF) for w in (d, d // 2, d // 2)],
        compiler_params=params(),
        cost_estimate=cost(6e9, rows * d * 12),
        name="norm_a",
    )(core, x_loc, x_rem, ln)


def attn_kernel(t_ref, qkv_ref, dol_ref, dor_ref, cos_ref, sin_ref, dqkv_ref, ctx_ref, dk_ref, dv_ref, *, bq, hd):
    t = t_ref[0]
    seq = qkv_ref.shape[1]
    half = hd // 2
    part = dol_ref.shape[1]
    cos, sin = cos_ref[...], sin_ref[...]

    def in_order(own, peer):
        return jnp.concatenate([jnp.where(t == 0, own, peer), jnp.where(t == 0, peer, own)], axis=1)

    def place(lo, n):
        slot = t if lo < part else 1 - t
        return pl.ds(pl.multiple_of(slot * part + lo % part, 128), n)

    def rope(v):
        lo, hi = v[:half].astype(F32), v[half:].astype(F32)
        return jnp.concatenate([lo * cos - hi * sin, hi * cos + lo * sin], axis=0).astype(BF)

    def rope_back(d, c, s):
        lo, hi = d[:half].astype(BF).astype(F32), d[half:].astype(BF).astype(F32)
        return jnp.concatenate([lo * c + hi * s, hi * c - lo * s], axis=0).astype(BF)

    scale = hd ** -0.5
    qkv = in_order(qkv_ref[:, :part], qkv_ref[:, part:])
    q_t = rope(qkv[0:hd])
    k_t = rope(qkv[hd:2 * hd])
    v_t = qkv[2 * hd:3 * hd]
    q_t = (q_t.astype(F32) * scale).astype(BF)
    do_t = in_order(dol_ref[...], dor_ref[...])
    q_n, do_n, k_n, v_n = q_t.T, do_t.T, k_t.T, v_t.T
    tri = lax.broadcasted_iota(jnp.int32, (bq, bq), 0) <= lax.broadcasted_iota(jnp.int32, (bq, bq), 1)
    for i in range(seq // bq):
        lo, nk = i * bq, (i + 1) * bq
        blocks = [slice(j * bq, (j + 1) * bq) for j in range(i + 1)]
        q_b, do_b = q_t[:, lo:nk], do_t[:, lo:nk]
        ss = [dot(k_n[b], q_b, 1, 0) for b in blocks]
        ss[i] = jnp.where(tri, ss[i], -1e30)
        m = functools.reduce(jnp.maximum, [jnp.max(s, axis=0, keepdims=True) for s in ss])
        es = [jnp.exp(s - m) for s in ss]
        r = 1.0 / sum(jnp.sum(e, axis=0, keepdims=True) for e in es)
        ps = [e * r for e in es]
        pbs = [p.astype(BF) for p in ps]
        dps = [dot(v_n[b], do_b, 1, 0).astype(BF) for b in blocks]
        delta = sum(jnp.sum(p * d.astype(F32), axis=0, keepdims=True) for p, d in zip(ps, dps))
        dss = [(p * (d.astype(F32) - delta)).astype(BF) for p, d in zip(ps, dps)]
        ctx_ref[:, place(lo, bq)] = sum(dot(v_t[:, b], p, 1, 0) for b, p in zip(blocks, pbs)).astype(BF)
        dq = sum(dot(k_t[:, b], d, 1, 0) for b, d in zip(blocks, dss)) * scale
        dqkv_ref[0:hd, place(lo, bq)] = rope_back(dq, cos[:, lo:nk], sin[:, lo:nk])
        for j, b in enumerate(blocks):
            dv_new = dot(pbs[j], do_n[lo:nk], 1, 0)
            dk_new = dot(dss[j], q_n[lo:nk], 1, 0)
            if j < i:
                dv_ref[b, :] += dv_new
                dk_ref[b, :] += dk_new
            else:
                dv_ref[b, :] = dv_new
                dk_ref[b, :] = dk_new
    dk = rope_back(dk_ref[...].T, cos, sin)
    dv = dv_ref[...].T.astype(BF)
    for lo in (0, part):
        dqkv_ref[hd:2 * hd, place(lo, part)] = dk[:, lo:lo + part]
        dqkv_ref[2 * hd:3 * hd, place(lo, part)] = dv[:, lo:lo + part]


def attention(t, qkv_t, dol, dor, cos_t, sin_t, hd, first, heads, bq=256):
    seq = qkv_t.shape[1]
    part = dol.shape[1]
    const = lambda g, t: (0, 0)
    row = lambda g, t: (g + first, 0)
    mine = lambda g, t: (g, 0)
    return pl.pallas_call(
        functools.partial(attn_kernel, bq=bq, hd=hd),
        grid_spec=pltpu.PrefetchScalarGridSpec(
            num_scalar_prefetch=1,
            grid=(heads,),
            in_specs=[
                pl.BlockSpec((3 * hd, seq), row),
                pl.BlockSpec((hd, part), row),
                pl.BlockSpec((hd, part), row),
                pl.BlockSpec((hd // 2, seq), const),
                pl.BlockSpec((hd // 2, seq), const),
            ],
            out_specs=[pl.BlockSpec((3 * hd, seq), mine), pl.BlockSpec((hd, seq), mine)],
            scratch_shapes=[pltpu.VMEM((seq, hd), F32), pltpu.VMEM((seq, hd), F32)],
        ),
        out_shape=[jax.ShapeDtypeStruct((heads * 3 * hd, seq), BF), jax.ShapeDtypeStruct((heads * hd, seq), BF)],
        compiler_params=params(),
        cost_estimate=cost(heads * 6e9, heads << 20, seq * seq * heads // 2),
        name="attn",
    )(t, qkv_t, dol, dor, cos_t, sin_t)


def gelu_pair(h_ref, dy_ref, wu, wd, rows):
    u = dot(h_ref[rows, :], wu, 1, 0).astype(BF).astype(F32)
    dg = dot(dy_ref[rows, :], wd, 1, 1).astype(BF).astype(F32)
    cdf = 0.5 + 0.5 * lax.erf(u * SQRT_HALF)
    pdf = jnp.exp(-0.5 * u * u) * INV_SQRT_2PI
    return (u * cdf).astype(BF), (dg * (cdf + u * pdf)).astype(BF)


def mlp_own_kernel(h_ref, dy_ref, wu_ref, wd_ref, at_ref, du_ref, dh_ref, acc_ref, *, tc):
    step = pl.program_id(0)
    wu, wd = wu_ref[...], wd_ref[...]
    for k in range(h_ref.shape[0] // tc):
        rows = pl.ds(k * tc, tc)
        a, du = gelu_pair(h_ref, dy_ref, wu, wd, rows)
        at_ref[:, rows] = a.T
        du_ref[0, rows, :] = du
        add = dot(du, wu, 1, 1)

        @pl.when(step == 0)
        def _():
            acc_ref[rows, :] = add

        @pl.when(step > 0)
        def _():
            acc_ref[rows, :] += add

    @pl.when(step == pl.num_programs(0) - 1)
    def _():
        dh_ref[...] = acc_ref[...].astype(BF)


def mlp_own(h, dy, w_up, w_down, n=4, tc=256):
    seq, d = h.shape
    ff = w_up.shape[1]
    fb = ff // n
    full = pl.BlockSpec((seq, d), lambda i: (0, 0))
    return pl.pallas_call(
        functools.partial(mlp_own_kernel, tc=tc),
        grid=(n,),
        in_specs=[full, full, pl.BlockSpec((d, fb), lambda i: (0, i)), pl.BlockSpec((fb, d), lambda i: (i, 0))],
        out_specs=[pl.BlockSpec((fb, seq), lambda i: (i, 0)), pl.BlockSpec((1, seq, fb), lambda i: (i, 0, 0)), full],
        out_shape=[jax.ShapeDtypeStruct((ff, seq), BF), jax.ShapeDtypeStruct((n, seq, fb), BF), jax.ShapeDtypeStruct((seq, d), BF)],
        scratch_shapes=[pltpu.VMEM((seq, d), F32)],
        compiler_params=params(),
        cost_estimate=cost(6 * seq * d * ff, 20 << 20, 2 * seq * ff),
        name="mlp_own",
    )(h, dy, w_up, w_down)


def mlp_peer_kernel(c_ref, h_ref, dyr_ref, dyl_ref, hkl_ref, hsl_ref, hkr_ref, hsr_ref, wu_ref, wd_ref, at_ref, dul_ref,
                    dka_ref, dkb_ref, dsa_ref, dsb_ref, uka_ref, ukb_ref, usa_ref, usb_ref, dh_ref, acc_ref, a_ref, du_ref, *, tc):
    step = pl.program_id(0)
    wu, wd = wu_ref[...], wd_ref[...]
    fb = wu.shape[1]
    m = fb // 2

    @pl.when(step == 0)
    def _():
        acc_ref[...] = jnp.zeros_like(acc_ref)

    for k in range(h_ref.shape[0] // tc):
        rows = pl.ds(k * tc, tc)
        a, du = gelu_pair(h_ref, dyr_ref, wu, wd, rows)
        a_ref[rows, :] = a
        du_ref[rows, :] = du
        acc_ref[rows, :] += dot(du, wu, 1, 1)
    for side, (ra, rb) in ((c_ref[0], (dka_ref, dkb_ref)), (1 - c_ref[0], (dsa_ref, dsb_ref))):
        block = pl.ds(pl.multiple_of(side * m, 128), m)
        g = dot(at_ref[block, :], dyl_ref[...], 1, 0) + dot(a_ref[:, block], dyr_ref[...], 0, 0)
        w = g.shape[1] // 2
        ra[0] = g[:, :w]
        rb[0] = g[:, w:]
    for hl, hr, ra, rb in ((hkl_ref, hkr_ref, uka_ref, ukb_ref), (hsl_ref, hsr_ref, usa_ref, usb_ref)):
        g = dot(hl[...], dul_ref[0], 1, 0) + dot(hr[...], du_ref[...], 1, 0)
        n = g.shape[0] // 4
        for j in range(4):
            ra[0, j] = g[j * n:(j + 1) * n, :m]
            rb[0, j] = g[j * n:(j + 1) * n, m:]

    @pl.when(step == pl.num_programs(0) - 1)
    def _():
        dh_ref[...] = acc_ref[...].astype(BF)


def mlp_peer(core, h, dy_rem, dy_loc, hts, w_up, w_down, at, du, n=4, tc=256):
    seq, d = h.shape
    ff = w_up.shape[1]
    fb = ff // n
    full = lambda r, w: pl.BlockSpec((r, w), lambda i, c: (0, 0))
    dspec = pl.BlockSpec((1, fb // 2, d // 2), lambda i, c: (i, 0, 0))
    uspec = pl.BlockSpec((1, 4, d // 8, fb // 2), lambda i, c: (i, 0, 0, 0))
    return pl.pallas_call(
        functools.partial(mlp_peer_kernel, tc=tc),
        grid_spec=pltpu.PrefetchScalarGridSpec(
            num_scalar_prefetch=1,
            grid=(n,),
            in_specs=[full(seq, d)] * 3 + [full(d // 2, seq)] * 4 + [
                pl.BlockSpec((d, fb), lambda i, c: (0, i)), pl.BlockSpec((fb, d), lambda i, c: (i, 0)),
                pl.BlockSpec((fb, seq), lambda i, c: (i, 0)), pl.BlockSpec((1, seq, fb), lambda i, c: (i, 0, 0))],
            out_specs=[dspec] * 4 + [uspec] * 4 + [full(seq, d)],
            scratch_shapes=[pltpu.VMEM((seq, d), F32), pltpu.VMEM((seq, fb), BF), pltpu.VMEM((seq, fb), BF)],
        ),
        out_shape=[jax.ShapeDtypeStruct((n, fb // 2, d // 2), F32)] * 4
        + [jax.ShapeDtypeStruct((n, 4, d // 8, fb // 2), F32)] * 4 + [jax.ShapeDtypeStruct((seq, d), BF)],
        compiler_params=params(),
        cost_estimate=cost(14 * seq * d * ff, 40 << 20, 2 * seq * ff),
        name="mlp_peer",
    )(core, h, dy_rem, dy_loc, *hts, w_up, w_down, at, du)


MESH = pl.DeviceIdType.MESH


def tail_kernel(*refs, bt, hd):
    n_in = 18
    hbm, refs = refs[:n_in], refs[n_in:]
    (gx_ref, sums_ref, gq_ref, gw_ref), refs = refs[:4], refs[4:]
    vm, refs = refs[:n_in], refs[n_in:]
    (z_send, z_recv, sum_src, sum_got, q_keep, q_send, q_recv, w_keep, w_send, w_recv,
     q1_send, q1_recv, w1_send, w1_recv, q2_send, q2_recv, w2_send, w2_recv,
     in_sem, send_sem, recv_sem) = refs
    dq, ctx = vm[0:4], vm[4:8]
    hk, hs, wt, xl, xr, dhl, dhr, dyl, dyr, ln = vm[8:18]
    me, t = lax.axis_index("dp"), lax.axis_index("tp")
    c, xx, yy = me % 2, (me // 2) % 2, me // 4
    partner = {"c": {"dp": me + 1 - 2 * c}, "x": {"dp": me + 2 - 4 * xx}, "y": {"dp": me + 4 - 8 * yy}, "z": {"tp": 1 - t}}
    part = xl.shape[0]

    loads = [pltpu.make_async_copy(src, dst, in_sem.at[i]) for i, (src, dst) in enumerate(zip(hbm, vm))]
    order = [0, 1, 2, 3, 10, 12, 14, 17, 9, 8, 4, 5, 6, 7, 15, 16, 11, 13]
    for i in order:
        loads[i].start()
    barrier = pltpu.get_barrier_semaphore()
    for p in "cxyz":
        pl.semaphore_signal(barrier, inc=1, device_id=partner[p], device_id_type=MESH)
    pl.semaphore_wait(barrier, 4)

    count = [0]

    def send(src, dst, way):
        i = count[0]
        count[0] += 1
        copy = pltpu.make_async_remote_copy(
            src_ref=src, dst_ref=dst, send_sem=send_sem.at[i], recv_sem=recv_sem.at[i],
            device_id=partner[way], device_id_type=MESH)
        copy.start()
        return copy

    def need(*idx):
        for i in idx:
            loads[i].wait()

    def block(x_ref, dh_ref, b, peer):
        rows = pl.ds(b * bt, bt)
        cols = pl.ds((part if peer else 0) + b * bt, bt)
        n = dq[0].shape[0]
        dha = sum(dot(r[:, cols], wt[g * n:(g + 1) * n, :], 0, 0) for g, r in enumerate(dq))
        dha = dha.astype(BF).astype(F32)
        dhm = dh_ref[rows, :].astype(F32)
        xh, _ = normalized(x_ref[rows, :].astype(F32))
        dxh = (dha * ln[0:1, :] + dhm * ln[2:3, :]).astype(BF)
        parts = [dha * xh, dha, dhm * xh, dhm]
        return dxh, jnp.concatenate([jnp.sum(p, axis=0, keepdims=True) for p in parts], axis=0)

    def peer_block(b):
        dxh, s = block(xr, dhr, b, True)
        z_send[b] = dxh
        if b == 0:
            sum_src[0] = s
        else:
            sum_src[0] += s
        return send(z_send.at[b], z_recv.at[b], "z")

    def qkv_grad(h_ref, out_ref, g):
        r = dot(dq[g][...], h_ref[...], 1, 0)
        n = r.shape[1] // 4
        for j in range(4):
            out_ref[g, j] = r[:, j * n:(j + 1) * n]

    def out_grad(want, out_ref):
        cx = jnp.concatenate([jnp.where(want == 0, r[:hd, :], r[hd:, :]) for r in ctx], axis=0)
        r = dot(cx[:, :part], dyl[...], 1, 0) + dot(cx[:, part:], dyr[...], 1, 0)
        m = r.shape[1] // 2
        for j in range(4):
            for k in range(2):
                out_ref[k, j] = r[j * hd:(j + 1) * hd, k * m:(k + 1) * m]

    def first(keep, got, out, k):
        for i in range(2):
            s_idx = 2 * i + 1 - xx if k == 0 else 2 * (1 - yy) + i
            k_idx = 2 * i + xx if k == 0 else 2 * yy + i
            out[i] = keep[s_idx] + got[s_idx]
            got[k_idx] = keep[k_idx] + got[k_idx]

    def second(got, got1, out, k):
        mine, other = (yy, 1 - yy) if k == 0 else (xx, 1 - xx)
        at = (lambda i: 2 * i + xx) if k == 0 else (lambda i: 2 * yy + i)
        out[...] = got[at(other)] + got1[other]
        return got[at(mine)] + got1[mine]

    ways = ("x", "y"), ("y", "x")

    need(0, 1, 2, 3, 10, 12, 14, 17)
    zs = [peer_block(0)]
    need(9)
    qc = []
    for g in range(4):
        qkv_grad(hs, q_send, g)
        if g % 2 == 1:
            qc.append(send(q_send.at[pl.ds(g - 1, 2)], q_recv.at[pl.ds(g - 1, 2)], "c"))
    zs.append(peer_block(1))
    need(8)
    for g in (0, 1):
        qkv_grad(hk, q_keep, g)

    q1 = [None] * 4

    def q_first(g):
        first(q_keep.at[g], q_recv.at[g], q1_send.at[g], g % 2)
        q1[g] = send(q1_send.at[g], q1_recv.at[g], ways[g % 2][0])

    qc[0].wait()
    q_first(0)
    q_first(1)
    for g in (2, 3):
        qkv_grad(hk, q_keep, g)
    zs.append(peer_block(2))
    qc[1].wait()
    q_first(2)
    q_first(3)
    need(4, 5, 6, 7, 15, 16)
    out_grad(1 - c, w_send)
    wc = send(w_send, w_recv, "c")
    out_grad(c, w_keep)
    wc.wait()
    w1 = []
    for k in range(2):
        first(w_keep.at[k], w_recv.at[k], w1_send.at[k], k)
        w1.append(send(w1_send.at[k], w1_recv.at[k], ways[k][0]))

    need(11, 13)

    def own_block(b):
        dxh, s = block(xl, dhl, b, False)
        gx_ref[pl.ds(b * bt, bt), :] = dxh
        sum_src[0] += s

    def grad_x(b):
        zs[b].wait()
        rows = pl.ds(b * bt, bt)
        dxh = gx_ref[rows, :].astype(F32) + z_recv[b].astype(F32)
        xh, rstd = normalized(xl[rows, :].astype(F32))
        dx = rstd * (dxh - jnp.mean(dxh, -1, keepdims=True) - xh * jnp.mean(dxh * xh, -1, keepdims=True))
        gx_ref[rows, :] = (dyl[rows, :].astype(F32) + dx).astype(BF)

    q2 = [None] * 4
    n = gq_ref.shape[0] // 4

    def q_second(g):
        q1[g].wait()
        gq_ref[g * n:(g + 1) * n, :] = second(q_recv.at[g], q1_recv.at[g], q2_send.at[g], g % 2)
        q2[g] = send(q2_send.at[g], q2_recv.at[g], ways[g % 2][1])

    own_block(0)
    q_second(0)
    q_second(1)
    own_block(1)
    grad_x(0)
    own_block(2)
    sums = [send(sum_src.at[0], sum_got.at[0], "z")]
    q_second(2)
    q_second(3)
    grad_x(1)

    def sum_next(i, way):
        sums[-1].wait()
        sum_src[i] = sum_src[i - 1] + sum_got[i - 1]
        sums.append(send(sum_src.at[i], sum_got.at[i], way))

    sum_next(1, "c")
    m = gw_ref.shape[1] // 2
    w2 = []
    for k in range(2):
        w1[k].wait()
        gw_ref[:, k * m:(k + 1) * m] = second(w_recv.at[k], w1_recv.at[k], w2_send.at[k], k)
        w2.append(send(w2_send.at[k], w2_recv.at[k], ways[k][1]))
    sum_next(2, "x")
    for g in (0, 1):
        q2[g].wait()
        gq_ref[g * n:(g + 1) * n, :] += q2_recv[g]
    sum_next(3, "y")
    for g in (2, 3):
        q2[g].wait()
        gq_ref[g * n:(g + 1) * n, :] += q2_recv[g]
    for k in range(2):
        w2[k].wait()
        gw_ref[:, k * m:(k + 1) * m] += w2_recv[k]
    sums[-1].wait()
    sums_ref[...] = sum_src[3] + sum_got[3]
    grad_x(2)


def tail(dqs, ctxs, h_keep, h_send, w_t, x_loc, x_rem, dhm_loc, dhm_rem, dy_loc, dy_rem, ln, hd, bt=256):
    ins = [*dqs, *ctxs, h_keep, h_send, w_t, x_loc, x_rem, dhm_loc, dhm_rem, dy_loc, dy_rem, ln]
    part, d = x_loc.shape
    rows = dqs[0].shape[0]
    nb = part // bt
    cols = d // 8
    f = lambda *shape: pltpu.VMEM(shape, F32)
    sds = jax.ShapeDtypeStruct
    scratch = [pltpu.VMEM(v.shape, v.dtype) for v in ins] + [
        pltpu.VMEM((nb, bt, d), BF), pltpu.VMEM((nb, bt, d), BF), f(4, 4, d), f(4, 4, d),
        f(4, 4, rows, cols), f(4, 4, rows, cols), f(4, 4, rows, cols),
        f(2, 4, hd, d // 2), f(2, 4, hd, d // 2), f(2, 4, hd, d // 2),
        f(4, 2, rows, cols), f(4, 2, rows, cols), f(2, 2, hd, d // 2), f(2, 2, hd, d // 2),
        f(4, rows, cols), f(4, rows, cols), f(2, hd, d // 2), f(2, hd, d // 2),
        pltpu.SemaphoreType.DMA((len(ins),)), pltpu.SemaphoreType.DMA((32,)), pltpu.SemaphoreType.DMA((32,)),
    ]
    vm = pl.BlockSpec(memory_space=pltpu.VMEM)
    return pl.pallas_call(
        functools.partial(tail_kernel, bt=bt, hd=hd),
        in_specs=[pl.BlockSpec(memory_space=pl.ANY)] * len(ins),
        out_specs=[vm] * 4,
        out_shape=[sds((part, d), BF), sds((4, d), F32), sds((4 * rows, cols), F32), sds((hd, d), F32)],
        scratch_shapes=scratch,
        compiler_params=pltpu.CompilerParams(vmem_limit_bytes=VMEM_LIMIT, collective_id=0, has_side_effects=True),
        cost_estimate=cost(4e10, 40 << 20),
        name="tail",
    )(*ins)


def solution(mesh):
    dp = mesh.shape["dp"]
    tp = mesh.shape["tp"]

    def swap(v, bit):
        return lax.ppermute(v, "dp", [(i, i ^ bit) for i in range(dp)])

    def swap_tp(v):
        return lax.ppermute(v, "tp", [(i, i ^ 1) for i in range(tp)])

    def take(v, idx, axis):
        return lax.dynamic_index_in_dim(v, idx, axis, keepdims=False)

    def after(v, *deps):
        return lax.optimization_barrier((v,) + deps)[0]

    def local_step(x_loc, dy_loc, ln_params, w_qkv, w_out, w_up, w_down):
        x_loc, dy_loc = x_loc[0], dy_loc[0]
        half, d = x_loc.shape
        seq = half * tp
        heads, hd = w_qkv.shape[1], w_qkv.shape[3]
        t = lax.axis_index("tp")
        me = lax.axis_index("dp")
        c, xx, yy = me % 2, (me // 2) % 2, me // 4
        t1, c1 = t.astype(jnp.int32)[None], c.astype(jnp.int32)[None]

        x_rem = swap_tp(x_loc)
        dy_rem = swap_tp(dy_loc)

        w_t = w_qkv.transpose(1, 2, 3, 0).reshape(heads * 3 * hd, d)
        inv_freq = ROPE_BASE ** (-2.0 * jnp.arange(hd // 2, dtype=F32) / hd)
        ang = inv_freq[:, None] * jnp.arange(seq).astype(F32)[None, :]
        cos_t, sin_t = jnp.cos(ang), jnp.sin(ang)

        hm_loc, hk_loc, hs_loc = norm_m(c1, x_loc, ln_params)
        at_loc, du_loc, dhm_loc = mlp_own(hm_loc, dy_loc, w_up, w_down)
        dctx_loc = dot(w_out, dy_loc, 1, 1).astype(BF)

        x_rem = after(x_rem, dhm_loc, dctx_loc, cos_t, sin_t, w_t)
        hm_rem, hk_rem, hs_rem = norm_m(c1, x_rem, ln_params)
        h_a, h_keep, h_send = norm_a(c1, x_loc, x_rem, ln_params)
        qkv_t = dot(w_t, h_a, 1, 1).astype(BF)

        dy_rem = after(dy_rem, qkv_t, h_keep, hm_rem)
        dka, dkb, dsa, dsb, uka, ukb, usa, usb, dhm_rem = mlp_peer(
            c1, hm_rem, dy_rem, dy_loc, (hk_loc, hs_loc, hk_rem, hs_rem), w_up, w_down, at_loc, du_loc)
        dctx_rem = dot(w_out, after(dy_rem, dhm_rem), 1, 1).astype(BF)

        def half_sum(keep, got, idx, axis):
            send = take(keep, 1 - idx, axis) + take(got, 1 - idx, axis)
            return take(keep, idx, axis) + take(got, idx, axis), send

        class Scatter:
            def __init__(self, keep, send, x_first, lead=0):
                n = lead
                self.ways = ((xx, n + 1, 2), (yy, n, 4)) if x_first else ((yy, n, 4), (xx, n, 2))
                got = swap(send, 1)
                self.keep, self.got = (v.reshape(v.shape[:n] + (2, 2) + v.shape[n + 1:]) for v in (keep, got))

            def step(self, *deps):
                (idx, axis, bit), self.ways = self.ways[0], self.ways[1:]
                keep = after(self.keep, *deps) if deps else self.keep
                self.keep, send = half_sum(keep, self.got, idx, axis)
                self.got = swap(send, bit)
                return send

            def end(self):
                return self.keep + self.got

        def pair(ka, sa, kb, sb, lead=0):
            return [Scatter(ka, sa, True, lead), Scatter(kb, sb, False, lead)]

        def steps(rs, *deps):
            return [r.step(*deps) for r in rs]

        down = pair(dka, dsa, dkb, dsb)
        up = pair(uka, usa, ukb, usb, 1)
        dqs, ctxs = [], []

        def attend(k, *deps):
            dq, ctx = attention(t1, after(qkv_t, *deps), dctx_loc, dctx_rem, cos_t, sin_t, hd, 2 * k, 2)
            dqs.append(dq)
            ctxs.append(ctx)

        s = steps(down)
        attend(0, dhm_rem, *s)
        s = steps(up, dqs[0])
        attend(1, *s)
        s = steps(down, dqs[1])
        attend(2, *s)
        s = steps(up, dqs[2])
        attend(3, *s)
        grad_x, sums, g_wqkv, g_wout = tail(
            dqs, ctxs, h_keep, h_send, w_t, x_loc, x_rem, dhm_loc, dhm_rem, dy_loc, dy_rem, ln_params, hd)
        grad_x = grad_x[None]

        g_wdown = jnp.concatenate([r.end() for r in down], axis=1)
        g_wup = jnp.stack([r.end() for r in up], axis=2).transpose(1, 0, 2, 3).reshape(d // dp, -1)
        g_wqkv = g_wqkv.reshape(heads, 3, hd, d // dp).transpose(3, 0, 1, 2)
        return grad_x, sums, g_wqkv, g_wout, g_wup, g_wdown

    return jax.shard_map(
        local_step,
        mesh=mesh,
        in_specs=(P("dp", "tp"), P("dp", "tp"), P(), P(None, "tp"), P("tp"), P(None, "tp"), P("tp")),
        out_specs=(P("dp", "tp"), P(), P("dp", "tp"), P(("tp", "dp")), P("dp", "tp"), P(("tp", "dp"))),
        check_vma=False,
    )
```

```python
import functools

import jax
import jax.numpy as jnp
from jax import lax
from jax.experimental import pallas as pl
from jax.experimental.pallas import tpu as pltpu
from jax.sharding import PartitionSpec as P

NORM_EPS = 1e-5
ROPE_BASE = 10000.0
BF = jnp.bfloat16
F32 = jnp.float32
SQRT_HALF = 0.7071067811865476
INV_SQRT_2PI = 0.3989422804014327
VMEM_LIMIT = 60 * 1024 * 1024


def dot(a, b, ca, cb):
    return lax.dot_general(a, b, (((ca,), (cb,)), ((), ())), preferred_element_type=F32)


def params():
    return pltpu.CompilerParams(vmem_limit_bytes=VMEM_LIMIT)


def cost(flops, nbytes, trans=0):
    return pl.CostEstimate(flops=int(flops), bytes_accessed=int(nbytes), transcendentals=int(trans))


def normalized(x):
    cen = x - jnp.mean(x, axis=-1, keepdims=True)
    rstd = lax.rsqrt(jnp.mean(cen * cen, axis=-1, keepdims=True) + NORM_EPS)
    return cen * rstd, rstd


def norm_m_kernel(c_ref, x_ref, ln_ref, hm_ref, hk_ref, hs_ref):
    hm = (normalized(x_ref[...].astype(F32))[0] * ln_ref[2:3, :] + ln_ref[3:4, :]).astype(BF)
    hm_ref[...] = hm
    n = hm.shape[1] // 8
    for j in range(4):
        even, odd = hm[:, 2 * j * n:(2 * j + 1) * n].T, hm[:, (2 * j + 1) * n:(2 * j + 2) * n].T
        hk_ref[j * n:(j + 1) * n, :] = jnp.where(c_ref[0] == 0, even, odd)
        hs_ref[j * n:(j + 1) * n, :] = jnp.where(c_ref[0] == 0, odd, even)


def norm_m(core, x, ln, bt=256):
    rows, d = x.shape
    tok = pl.BlockSpec((bt, d), lambda i, c: (i, 0))
    return pl.pallas_call(
        norm_m_kernel,
        grid_spec=pltpu.PrefetchScalarGridSpec(
            num_scalar_prefetch=1,
            grid=(rows // bt,),
            in_specs=[tok, pl.BlockSpec((4, d), lambda i, c: (0, 0))],
            out_specs=[tok] + [pl.BlockSpec((d // 2, bt), lambda i, c: (0, i))] * 2,
        ),
        out_shape=[jax.ShapeDtypeStruct((rows, d), BF)] + [jax.ShapeDtypeStruct((d // 2, rows), BF)] * 2,
        compiler_params=params(),
        cost_estimate=cost(3e9, rows * d * 6),
        name="norm_m",
    )(core, x, ln)


def norm_a_kernel(c_ref, xl_ref, xr_ref, ln_ref, ha_ref, hk_ref, hs_ref, *, nb):
    def run(x_ref):
        ha = (normalized(x_ref[...].astype(F32))[0] * ln_ref[0:1, :] + ln_ref[1:2, :]).astype(BF)
        ha_ref[...] = ha
        n = ha.shape[1] // 8
        for j in range(4):
            even, odd = ha[:, 2 * j * n:(2 * j + 1) * n], ha[:, (2 * j + 1) * n:(2 * j + 2) * n]
            hk_ref[:, j * n:(j + 1) * n] = jnp.where(c_ref[0] == 0, even, odd)
            hs_ref[:, j * n:(j + 1) * n] = jnp.where(c_ref[0] == 0, odd, even)

    pl.when(pl.program_id(0) < nb)(lambda: run(xl_ref))
    pl.when(pl.program_id(0) >= nb)(lambda: run(xr_ref))


def norm_a(core, x_loc, x_rem, ln, bt=256):
    rows, d = x_loc.shape
    nb = rows // bt
    tok = lambda w: pl.BlockSpec((bt, w), lambda i, c: (i, 0))
    return pl.pallas_call(
        functools.partial(norm_a_kernel, nb=nb),
        grid_spec=pltpu.PrefetchScalarGridSpec(
            num_scalar_prefetch=1,
            grid=(2 * nb,),
            in_specs=[
                pl.BlockSpec((bt, d), lambda i, c: (jnp.minimum(i, nb - 1), 0)),
                pl.BlockSpec((bt, d), lambda i, c: (jnp.maximum(i - nb, 0), 0)),
                pl.BlockSpec((4, d), lambda i, c: (0, 0)),
            ],
            out_specs=[tok(d), tok(d // 2), tok(d // 2)],
        ),
        out_shape=[jax.ShapeDtypeStruct((2 * rows, w), BF) for w in (d, d // 2, d // 2)],
        compiler_params=params(),
        cost_estimate=cost(6e9, rows * d * 12),
        name="norm_a",
    )(core, x_loc, x_rem, ln)


MESH = pl.DeviceIdType.MESH


def partners():
    me, t = lax.axis_index("dp"), lax.axis_index("tp")
    c, xx, yy = me % 2, (me // 2) % 2, me // 4
    way = {"c": {"dp": me + 1 - 2 * c}, "x": {"dp": me + 2 - 4 * xx}, "y": {"dp": me + 4 - 8 * yy}, "z": {"tp": 1 - t}}
    return way, t, c, xx, yy


def meet(way, names):
    barrier = pltpu.get_barrier_semaphore()
    for p in names:
        pl.semaphore_signal(barrier, inc=1, device_id=way[p], device_id_type=MESH)
    pl.semaphore_wait(barrier, len(names))


def by_rows(n, chunk, f):
    def body(i, _):
        f(pl.ds(pl.multiple_of(i * chunk, 8), chunk))
        return _

    lax.fori_loop(0, n // chunk, body, 0)


WAYS = ("x", "y"), ("y", "x")


def attn_kernel(qkv_ref, dol_ref, dor_ref, cos_ref, sin_ref,
                dka, dkb, dsa, dsb, uka, ukb, usa, usb,
                dqkv_ref, ctx_ref, gd_ref, us_ref, uk_ref,
                dk_ref, dv_ref, d_keep, d_got, u_keep, u_got, d1_send, d1_got, u1_send, u1_got, d2_send, d2_got,
                load_sem, send_sem, recv_sem, *, bq, hd):
    way, t, _, xx, yy = partners()
    step = pl.program_id(0)
    last = pl.num_programs(0) - 1

    def remote(i, src, dst, w):
        return pltpu.make_async_remote_copy(
            src_ref=src, dst_ref=dst, send_sem=send_sem.at[i], recv_sem=recv_sem.at[i], device_id=way[w], device_id_type=MESH)

    core_d = [remote(k, src, d_got.at[k], "c") for k, src in enumerate((dsa, dsb))]
    core_u = [remote(2 + k, src, u_got.at[k], "c") for k, src in enumerate((usa, usb))]
    first_d = [remote(4 + k, d1_send.at[k], d1_got.at[k], WAYS[k][0]) for k in range(2)]
    first_u = [remote(6 + k, u1_send.at[k], u1_got.at[k], WAYS[k][0]) for k in range(2)]
    second_d = [remote(8 + k, d2_send.at[k], d2_got.at[k], WAYS[k][1]) for k in range(2)]
    load_d = [pltpu.make_async_copy(src, d_keep.at[k], load_sem.at[k]) for k, src in enumerate((dka, dkb))]
    load_u = [pltpu.make_async_copy(src, u_keep.at[k], load_sem.at[2 + k]) for k, src in enumerate((uka, ukb))]

    leave = [lambda i: 2 * i + 1 - xx, lambda i: 2 * (1 - yy) + i]
    stay = [lambda i: 2 * i + xx, lambda i: 2 * yy + i]
    mine = [yy, xx]

    @pl.when(step == 0)
    def _():
        meet(way, "cxy")
        for v in load_d + load_u + core_d + core_u:
            v.start()

    @pl.when(step == 1)
    def _():
        for k in range(2):
            load_d[k].wait()
            core_d[k].wait()
            for i in range(2):
                def add(r):
                    d1_send[k, i, r, :] = d_keep[k, leave[k](i), r, :] + d_got[k, leave[k](i), r, :]
                    d_keep[k, stay[k](i), r, :] += d_got[k, stay[k](i), r, :]

                by_rows(d_keep.shape[2], 32, add)
            first_d[k].start()

    @pl.when(step == 3)
    def _():
        for k in range(2):
            load_u[k].wait()
            core_u[k].wait()
            for i in range(2):
                def add(r):
                    for j in range(u_keep.shape[1]):
                        u1_send[k, i, j, r, :] = u_keep[k, j, leave[k](i), r, :] + u_got[k, j, leave[k](i), r, :]
                        u_keep[k, j, stay[k](i), r, :] += u_got[k, j, stay[k](i), r, :]

                by_rows(u_keep.shape[3], 16, add)
            first_u[k].start()

    @pl.when(step == 5)
    def _():
        for k in range(2):
            first_d[k].wait()
            m = mine[k]

            def add(r):
                d2_send[k, r, :] = d_keep[k, stay[k](1 - m), r, :] + d1_got[k, 1 - m, r, :]
                d_keep[k, stay[k](m), r, :] += d1_got[k, m, r, :]

            by_rows(d_keep.shape[2], 32, add)
            second_d[k].start()

    attn_head(t, qkv_ref, dol_ref, dor_ref, cos_ref, sin_ref, dqkv_ref, ctx_ref, dk_ref, dv_ref, bq, hd)

    @pl.when(step == last)
    def _():
        for k in range(2):
            first_u[k].wait()
            m = mine[k]

            def add(r):
                for j in range(u_keep.shape[1]):
                    us_ref[k, j, r, :] = u_keep[k, j, stay[k](1 - m), r, :] + u1_got[k, 1 - m, j, r, :]
                    uk_ref[k, j, r, :] = u_keep[k, j, stay[k](m), r, :] + u1_got[k, m, j, r, :]

            by_rows(u_keep.shape[3], 16, add)
        w = d_keep.shape[3]
        for k in range(2):
            second_d[k].wait()
            m = mine[k]

            def add(r):
                gd_ref[r, k * w:(k + 1) * w] = d_keep[k, stay[k](m), r, :] + d2_got[k, r, :]

            by_rows(d_keep.shape[2], 32, add)


def attn_head(t, qkv_ref, dol_ref, dor_ref, cos_ref, sin_ref, dqkv_ref, ctx_ref, dk_ref, dv_ref, bq, hd):
    seq = qkv_ref.shape[1]
    half = hd // 2
    part = dol_ref.shape[1]
    cos, sin = cos_ref[...], sin_ref[...]

    def in_order(own, peer):
        return jnp.concatenate([jnp.where(t == 0, own, peer), jnp.where(t == 0, peer, own)], axis=1)

    def place(lo, n):
        slot = t if lo < part else 1 - t
        return pl.ds(pl.multiple_of(slot * part + lo % part, 128), n)

    def rope(v):
        lo, hi = v[:half].astype(F32), v[half:].astype(F32)
        return jnp.concatenate([lo * cos - hi * sin, hi * cos + lo * sin], axis=0).astype(BF)

    def rope_back(d, c, s):
        lo, hi = d[:half].astype(BF).astype(F32), d[half:].astype(BF).astype(F32)
        return jnp.concatenate([lo * c + hi * s, hi * c - lo * s], axis=0).astype(BF)

    scale = hd ** -0.5
    qkv = in_order(qkv_ref[:, :part], qkv_ref[:, part:])
    q_t = rope(qkv[0:hd])
    k_t = rope(qkv[hd:2 * hd])
    v_t = qkv[2 * hd:3 * hd]
    q_t = (q_t.astype(F32) * scale).astype(BF)
    do_t = in_order(dol_ref[...], dor_ref[...])
    q_n, do_n, k_n, v_n = q_t.T, do_t.T, k_t.T, v_t.T
    tri = lax.broadcasted_iota(jnp.int32, (bq, bq), 0) <= lax.broadcasted_iota(jnp.int32, (bq, bq), 1)
    for i in range(seq // bq):
        lo, nk = i * bq, (i + 1) * bq
        blocks = [slice(j * bq, (j + 1) * bq) for j in range(i + 1)]
        q_b, do_b = q_t[:, lo:nk], do_t[:, lo:nk]
        ss = [dot(k_n[b], q_b, 1, 0) for b in blocks]
        ss[i] = jnp.where(tri, ss[i], -1e30)
        m = functools.reduce(jnp.maximum, [jnp.max(s, axis=0, keepdims=True) for s in ss])
        es = [jnp.exp(s - m) for s in ss]
        r = 1.0 / sum(jnp.sum(e, axis=0, keepdims=True) for e in es)
        ps = [e * r for e in es]
        pbs = [p.astype(BF) for p in ps]
        dps = [dot(v_n[b], do_b, 1, 0).astype(BF) for b in blocks]
        delta = sum(jnp.sum(p * d.astype(F32), axis=0, keepdims=True) for p, d in zip(ps, dps))
        dss = [(p * (d.astype(F32) - delta)).astype(BF) for p, d in zip(ps, dps)]
        ctx_ref[:, place(lo, bq)] = sum(dot(v_t[:, b], p, 1, 0) for b, p in zip(blocks, pbs)).astype(BF)
        dq = sum(dot(k_t[:, b], d, 1, 0) for b, d in zip(blocks, dss)) * scale
        dqkv_ref[0:hd, place(lo, bq)] = rope_back(dq, cos[:, lo:nk], sin[:, lo:nk])
        for j, b in enumerate(blocks):
            dv_new = dot(pbs[j], do_n[lo:nk], 1, 0)
            dk_new = dot(dss[j], q_n[lo:nk], 1, 0)
            if j < i:
                dv_ref[b, :] += dv_new
                dk_ref[b, :] += dk_new
            else:
                dv_ref[b, :] = dv_new
                dk_ref[b, :] = dk_new
    dk = rope_back(dk_ref[...].T, cos, sin)
    dv = dv_ref[...].T.astype(BF)
    for lo in (0, part):
        dqkv_ref[hd:2 * hd, place(lo, part)] = dk[:, lo:lo + part]
        dqkv_ref[2 * hd:3 * hd, place(lo, part)] = dv[:, lo:lo + part]


def attention(qkv_t, dol, dor, cos_t, sin_t, down, up, hd, bq=256):
    rows, seq = qkv_t.shape
    heads = rows // (3 * hd)
    part = dol.shape[1]
    const = pl.BlockSpec((hd // 2, seq), lambda g: (0, 0))
    row = lambda r, w: pl.BlockSpec((r, w), lambda g: (g, 0))
    hbm = pl.BlockSpec(memory_space=pl.ANY)
    dsh, ush = down[0].shape, up[0].shape
    dred, ured = dsh[1:], (ush[0],) + ush[2:]
    whole = lambda *shape: pl.BlockSpec(shape, lambda g: (0,) * len(shape))
    f = lambda *shape: pltpu.VMEM(shape, F32)
    sds = jax.ShapeDtypeStruct
    gd_shape = (dred[0], 2 * dred[1])
    return pl.pallas_call(
        functools.partial(attn_kernel, bq=bq, hd=hd),
        grid=(heads,),
        in_specs=[row(3 * hd, seq), row(hd, part), row(hd, part), const, const] + [hbm] * 8,
        out_specs=[row(3 * hd, seq), row(hd, seq), whole(*gd_shape), whole(2, *ured), whole(2, *ured)],
        out_shape=[sds((rows, seq), BF), sds((heads * hd, seq), BF), sds(gd_shape, F32), sds((2,) + ured, F32), sds((2,) + ured, F32)],
        scratch_shapes=[
            f(seq, hd), f(seq, hd), f(2, *dsh), f(2, *dsh), f(2, *ush), f(2, *ush),
            f(2, 2, *dred), f(2, 2, *dred), f(2, 2, *ured), f(2, 2, *ured), f(2, *dred), f(2, *dred),
            pltpu.SemaphoreType.DMA((4,)), pltpu.SemaphoreType.DMA((10,)), pltpu.SemaphoreType.DMA((10,)),
        ],
        compiler_params=pltpu.CompilerParams(vmem_limit_bytes=VMEM_LIMIT, collective_id=1, has_side_effects=True),
        cost_estimate=cost(heads * 6e9, heads << 20, seq * seq * heads // 2),
        name="attn",
    )(qkv_t, dol, dor, cos_t, sin_t, *down, *up)


def gelu_pair(h_ref, dy_ref, wu, wd, rows):
    u = dot(h_ref[rows, :], wu, 1, 0).astype(BF).astype(F32)
    dg = dot(dy_ref[rows, :], wd, 1, 1).astype(BF).astype(F32)
    cdf = 0.5 + 0.5 * lax.erf(u * SQRT_HALF)
    pdf = jnp.exp(-0.5 * u * u) * INV_SQRT_2PI
    return (u * cdf).astype(BF), (dg * (cdf + u * pdf)).astype(BF)


def mlp_own_kernel(h_ref, dy_ref, wu_ref, wd_ref, at_ref, du_ref, dh_ref, acc_ref, *, tc):
    step = pl.program_id(0)
    wu, wd = wu_ref[...], wd_ref[...]
    for k in range(h_ref.shape[0] // tc):
        rows = pl.ds(k * tc, tc)
        a, du = gelu_pair(h_ref, dy_ref, wu, wd, rows)
        at_ref[:, rows] = a.T
        du_ref[0, rows, :] = du
        add = dot(du, wu, 1, 1)

        @pl.when(step == 0)
        def _():
            acc_ref[rows, :] = add

        @pl.when(step > 0)
        def _():
            acc_ref[rows, :] += add

    @pl.when(step == pl.num_programs(0) - 1)
    def _():
        dh_ref[...] = acc_ref[...].astype(BF)


def mlp_own(h, dy, w_up, w_down, n=4, tc=256):
    seq, d = h.shape
    ff = w_up.shape[1]
    fb = ff // n
    full = pl.BlockSpec((seq, d), lambda i: (0, 0))
    return pl.pallas_call(
        functools.partial(mlp_own_kernel, tc=tc),
        grid=(n,),
        in_specs=[full, full, pl.BlockSpec((d, fb), lambda i: (0, i)), pl.BlockSpec((fb, d), lambda i: (i, 0))],
        out_specs=[pl.BlockSpec((fb, seq), lambda i: (i, 0)), pl.BlockSpec((1, seq, fb), lambda i: (i, 0, 0)), full],
        out_shape=[jax.ShapeDtypeStruct((ff, seq), BF), jax.ShapeDtypeStruct((n, seq, fb), BF), jax.ShapeDtypeStruct((seq, d), BF)],
        scratch_shapes=[pltpu.VMEM((seq, d), F32)],
        compiler_params=params(),
        cost_estimate=cost(6 * seq * d * ff, 20 << 20, 2 * seq * ff),
        name="mlp_own",
    )(h, dy, w_up, w_down)


def mlp_peer_kernel(c_ref, h_ref, dyr_ref, dyl_ref, hkl_ref, hsl_ref, hkr_ref, hsr_ref, wu_ref, wd_ref, at_ref, dul_ref,
                    dka_ref, dkb_ref, dsa_ref, dsb_ref, uka_ref, ukb_ref, usa_ref, usb_ref, dh_ref, acc_ref, a_ref, du_ref, *, tc):
    step = pl.program_id(0)
    wu, wd = wu_ref[...], wd_ref[...]
    fb = wu.shape[1]
    m = fb // 2

    @pl.when(step == 0)
    def _():
        acc_ref[...] = jnp.zeros_like(acc_ref)

    for k in range(h_ref.shape[0] // tc):
        rows = pl.ds(k * tc, tc)
        a, du = gelu_pair(h_ref, dyr_ref, wu, wd, rows)
        a_ref[rows, :] = a
        du_ref[rows, :] = du
        acc_ref[rows, :] += dot(du, wu, 1, 1)
    for side, (ra, rb) in ((c_ref[0], (dka_ref, dkb_ref)), (1 - c_ref[0], (dsa_ref, dsb_ref))):
        block = pl.ds(pl.multiple_of(side * m, 128), m)
        g = dot(at_ref[block, :], dyl_ref[...], 1, 0) + dot(a_ref[:, block], dyr_ref[...], 0, 0)
        w = g.shape[1] // 2
        ra[0] = g[:, :w]
        rb[0] = g[:, w:]
    for hl, hr, ra, rb in ((hkl_ref, hkr_ref, uka_ref, ukb_ref), (hsl_ref, hsr_ref, usa_ref, usb_ref)):
        g = dot(hl[...], dul_ref[0], 1, 0) + dot(hr[...], du_ref[...], 1, 0)
        n = g.shape[0] // 4
        for j in range(4):
            ra[0, j] = g[j * n:(j + 1) * n, :m]
            rb[0, j] = g[j * n:(j + 1) * n, m:]

    @pl.when(step == pl.num_programs(0) - 1)
    def _():
        dh_ref[...] = acc_ref[...].astype(BF)


def mlp_peer(core, h, dy_rem, dy_loc, hts, w_up, w_down, at, du, n=4, tc=256):
    seq, d = h.shape
    ff = w_up.shape[1]
    fb = ff // n
    full = lambda r, w: pl.BlockSpec((r, w), lambda i, c: (0, 0))
    dspec = pl.BlockSpec((1, fb // 2, d // 2), lambda i, c: (i, 0, 0))
    uspec = pl.BlockSpec((1, 4, d // 8, fb // 2), lambda i, c: (i, 0, 0, 0))
    return pl.pallas_call(
        functools.partial(mlp_peer_kernel, tc=tc),
        grid_spec=pltpu.PrefetchScalarGridSpec(
            num_scalar_prefetch=1,
            grid=(n,),
            in_specs=[full(seq, d)] * 3 + [full(d // 2, seq)] * 4 + [
                pl.BlockSpec((d, fb), lambda i, c: (0, i)), pl.BlockSpec((fb, d), lambda i, c: (i, 0)),
                pl.BlockSpec((fb, seq), lambda i, c: (i, 0)), pl.BlockSpec((1, seq, fb), lambda i, c: (i, 0, 0))],
            out_specs=[dspec] * 4 + [uspec] * 4 + [full(seq, d)],
            scratch_shapes=[pltpu.VMEM((seq, d), F32), pltpu.VMEM((seq, fb), BF), pltpu.VMEM((seq, fb), BF)],
        ),
        out_shape=[jax.ShapeDtypeStruct((n, fb // 2, d // 2), F32)] * 4
        + [jax.ShapeDtypeStruct((n, 4, d // 8, fb // 2), F32)] * 4 + [jax.ShapeDtypeStruct((seq, d), BF)],
        compiler_params=params(),
        cost_estimate=cost(14 * seq * d * ff, 40 << 20, 2 * seq * ff),
        name="mlp_peer",
    )(core, h, dy_rem, dy_loc, *hts, w_up, w_down, at, du)


def tail_kernel(*refs, bt, hd):
    n_in = 13
    hbm, us_ref, refs = refs[:n_in], refs[n_in], refs[n_in + 1:]
    (gx_ref, sums_ref, gq_ref, gw_ref, gu_ref), refs = refs[:5], refs[5:]
    vm, refs = refs[:n_in], refs[n_in:]
    (z_send, z_recv, sum_src, sum_got, q_keep, q_send, q_recv, w_keep, w_send, w_recv,
     q1_send, q1_recv, w1_send, w1_recv, q2_send, q2_recv, w2_send, w2_recv, u2_recv,
     in_sem, send_sem, recv_sem) = refs
    dq, ctx, hk, hs, wt, xl, xr, dhl, dhr, dyl, dyr, ln, uk = vm
    way_to, t, c, xx, yy = partners()
    part = xl.shape[0]
    gr = dq.shape[0] // 4

    loads = [pltpu.make_async_copy(src, dst, in_sem.at[i]) for i, (src, dst) in enumerate(zip(hbm, vm))]
    for i in (0, 4, 6, 8, 11, 3, 2, 1, 9, 10, 5, 7, 12):
        loads[i].start()
    meet(way_to, "cxyz")

    count = [0]

    def send(src, dst, way):
        i = count[0]
        count[0] += 1
        copy = pltpu.make_async_remote_copy(
            src_ref=src, dst_ref=dst, send_sem=send_sem.at[i], recv_sem=recv_sem.at[i],
            device_id=way_to[way], device_id_type=MESH)
        copy.start()
        return copy

    def need(*idx):
        for i in idx:
            loads[i].wait()

    def block(x_ref, dh_ref, b, peer):
        rows = pl.ds(b * bt, bt)
        cols = pl.ds((part if peer else 0) + b * bt, bt)
        dha = dot(dq[:, cols], wt[...], 0, 0).astype(BF).astype(F32)
        dhm = dh_ref[rows, :].astype(F32)
        xh, rstd = normalized(x_ref[rows, :].astype(F32))
        dxh = (dha * ln[0:1, :] + dhm * ln[2:3, :]).astype(BF)
        parts = [dha * xh, dha, dhm * xh, dhm]
        return dxh, jnp.concatenate([jnp.sum(p, axis=0, keepdims=True) for p in parts], axis=0)

    def peer_block(b):
        dxh, s = block(xr, dhr, b, True)
        z_send[b] = dxh
        if b == 0:
            sum_src[0] = s
        else:
            sum_src[0] += s
        return send(z_send.at[b], z_recv.at[b], "z")

    def qkv_grad(h_ref, out_ref, g):
        r = dot(dq[g * gr:(g + 1) * gr, :], h_ref[...], 1, 0)
        n = r.shape[1] // 4
        for j in range(4):
            out_ref[g, j] = r[:, j * n:(j + 1) * n]

    def out_grad(want, out_ref):
        cx = jnp.concatenate([jnp.where(want == 0, ctx[2 * j * hd:(2 * j + 1) * hd, :], ctx[(2 * j + 1) * hd:(2 * j + 2) * hd, :])
                              for j in range(4)], axis=0)
        r = dot(cx[:, :part], dyl[...], 1, 0) + dot(cx[:, part:], dyr[...], 1, 0)
        m = r.shape[1] // 2
        for j in range(4):
            for k in range(2):
                out_ref[k, j] = r[j * hd:(j + 1) * hd, k * m:(k + 1) * m]

    def first(keep, got, out, k):
        for i in range(2):
            s_idx = 2 * i + 1 - xx if k == 0 else 2 * (1 - yy) + i
            k_idx = 2 * i + xx if k == 0 else 2 * yy + i
            out[i] = keep[s_idx] + got[s_idx]
            got[k_idx] = keep[k_idx] + got[k_idx]

    def second(got, got1, out, k):
        mine, other = (yy, 1 - yy) if k == 0 else (xx, 1 - xx)
        at = (lambda i: 2 * i + xx) if k == 0 else (lambda i: 2 * yy + i)
        out[...] = got[at(other)] + got1[other]
        return got[at(mine)] + got1[mine]

    ways = ("x", "y"), ("y", "x")

    us = [send(us_ref.at[k], u2_recv.at[k], ways[k][1]) for k in range(2)]
    need(0, 4, 6, 8, 11)
    zs = [peer_block(0)]
    need(3)
    qc = []
    for g in range(4):
        qkv_grad(hs, q_send, g)
        if g % 2 == 1:
            qc.append(send(q_send.at[pl.ds(g - 1, 2)], q_recv.at[pl.ds(g - 1, 2)], "c"))
    zs.append(peer_block(1))
    need(2)
    for g in (0, 1):
        qkv_grad(hk, q_keep, g)

    q1 = [None] * 4

    def q_first(g):
        first(q_keep.at[g], q_recv.at[g], q1_send.at[g], g % 2)
        q1[g] = send(q1_send.at[g], q1_recv.at[g], ways[g % 2][0])

    qc[0].wait()
    q_first(0)
    q_first(1)
    for g in (2, 3):
        qkv_grad(hk, q_keep, g)
    zs.append(peer_block(2))
    qc[1].wait()
    q_first(2)
    q_first(3)
    need(1, 9, 10)
    out_grad(1 - c, w_send)
    wc = send(w_send, w_recv, "c")
    out_grad(c, w_keep)
    wc.wait()
    w1 = []
    for k in range(2):
        first(w_keep.at[k], w_recv.at[k], w1_send.at[k], k)
        w1.append(send(w1_send.at[k], w1_recv.at[k], ways[k][0]))

    need(5, 7)

    def own_block(b):
        dxh, s = block(xl, dhl, b, False)
        gx_ref[pl.ds(b * bt, bt), :] = dxh
        sum_src[0] += s

    def grad_x(b):
        zs[b].wait()
        rows = pl.ds(b * bt, bt)
        dxh = gx_ref[rows, :].astype(F32) + z_recv[b].astype(F32)
        xh, rstd = normalized(xl[rows, :].astype(F32))
        dx = rstd * (dxh - jnp.mean(dxh, -1, keepdims=True) - xh * jnp.mean(dxh * xh, -1, keepdims=True))
        gx_ref[rows, :] = (dyl[rows, :].astype(F32) + dx).astype(BF)

    q2 = [None] * 4
    n = gq_ref.shape[0] // 4

    def q_second(g):
        q1[g].wait()
        gq_ref[g * n:(g + 1) * n, :] = second(q_recv.at[g], q1_recv.at[g], q2_send.at[g], g % 2)
        q2[g] = send(q2_send.at[g], q2_recv.at[g], ways[g % 2][1])

    own_block(0)
    q_second(0)
    q_second(1)
    own_block(1)
    grad_x(0)
    own_block(2)
    sums = [send(sum_src.at[0], sum_got.at[0], "z")]
    q_second(2)
    q_second(3)
    grad_x(1)

    def sum_next(i, way):
        sums[-1].wait()
        sum_src[i] = sum_src[i - 1] + sum_got[i - 1]
        sums.append(send(sum_src.at[i], sum_got.at[i], way))

    sum_next(1, "c")
    need(12)
    blocks, m = uk.shape[1], uk.shape[3]
    for k in range(2):
        us[k].wait()
        for j in range(blocks):
            gu_ref[:, (2 * j + k) * m:(2 * j + k + 1) * m] = uk[k, j] + u2_recv[k, j]
    m = gw_ref.shape[1] // 2
    w2 = []
    for k in range(2):
        w1[k].wait()
        gw_ref[:, k * m:(k + 1) * m] = second(w_recv.at[k], w1_recv.at[k], w2_send.at[k], k)
        w2.append(send(w2_send.at[k], w2_recv.at[k], ways[k][1]))
    sum_next(2, "x")
    for g in (0, 1):
        q2[g].wait()
        gq_ref[g * n:(g + 1) * n, :] += q2_recv[g]
    sum_next(3, "y")
    for g in (2, 3):
        q2[g].wait()
        gq_ref[g * n:(g + 1) * n, :] += q2_recv[g]
    for k in range(2):
        w2[k].wait()
        gw_ref[:, k * m:(k + 1) * m] += w2_recv[k]
    sums[-1].wait()
    sums_ref[...] = sum_src[3] + sum_got[3]
    grad_x(2)


def tail(dq, ctx, h_keep, h_send, w_t, x_loc, x_rem, dhm_loc, dhm_rem, dy_loc, dy_rem, ln, u_keep, u_send, hd, bt=256):
    ins = [dq, ctx, h_keep, h_send, w_t, x_loc, x_rem, dhm_loc, dhm_rem, dy_loc, dy_rem, ln, u_keep]
    part, d = x_loc.shape
    rows = dq.shape[0] // 4
    nb = part // bt
    cols = d // 8
    f = lambda *shape: pltpu.VMEM(shape, F32)
    sds = jax.ShapeDtypeStruct
    scratch = [pltpu.VMEM(v.shape, v.dtype) for v in ins] + [
        pltpu.VMEM((nb, bt, d), BF), pltpu.VMEM((nb, bt, d), BF), f(4, 4, d), f(4, 4, d),
        f(4, 4, rows, cols), f(4, 4, rows, cols), f(4, 4, rows, cols),
        f(2, 4, hd, d // 2), f(2, 4, hd, d // 2), f(2, 4, hd, d // 2),
        f(4, 2, rows, cols), f(4, 2, rows, cols), f(2, 2, hd, d // 2), f(2, 2, hd, d // 2),
        f(4, rows, cols), f(4, rows, cols), f(2, hd, d // 2), f(2, hd, d // 2), f(*u_send.shape),
        pltpu.SemaphoreType.DMA((len(ins),)), pltpu.SemaphoreType.DMA((32,)), pltpu.SemaphoreType.DMA((32,)),
    ]
    vm = pl.BlockSpec(memory_space=pltpu.VMEM)
    u_cols = u_keep.shape[0] * u_keep.shape[1] * u_keep.shape[3]
    return pl.pallas_call(
        functools.partial(tail_kernel, bt=bt, hd=hd),
        in_specs=[pl.BlockSpec(memory_space=pl.ANY)] * (len(ins) + 1),
        out_specs=[vm] * 5,
        out_shape=[sds((part, d), BF), sds((4, d), F32), sds((4 * rows, cols), F32), sds((hd, d), F32), sds((u_keep.shape[2], u_cols), F32)],
        scratch_shapes=scratch,
        compiler_params=pltpu.CompilerParams(vmem_limit_bytes=VMEM_LIMIT, collective_id=0, has_side_effects=True),
        cost_estimate=cost(4e10, 40 << 20),
        name="tail",
    )(*ins, u_send)


def solution(mesh):
    dp = mesh.shape["dp"]
    tp = mesh.shape["tp"]

    def swap_tp(v):
        return lax.ppermute(v, "tp", [(i, i ^ 1) for i in range(tp)])

    def after(v, *deps):
        return lax.optimization_barrier((v,) + deps)[0]

    def local_step(x_loc, dy_loc, ln_params, w_qkv, w_out, w_up, w_down):
        x_loc, dy_loc = x_loc[0], dy_loc[0]
        half, d = x_loc.shape
        seq = half * tp
        heads, hd = w_qkv.shape[1], w_qkv.shape[3]
        me = lax.axis_index("dp")
        c1 = (me % 2).astype(jnp.int32)[None]

        x_rem = swap_tp(x_loc)
        dy_rem = swap_tp(dy_loc)

        w_t = w_qkv.transpose(1, 2, 3, 0).reshape(heads * 3 * hd, d)
        inv_freq = ROPE_BASE ** (-2.0 * jnp.arange(hd // 2, dtype=F32) / hd)
        ang = inv_freq[:, None] * jnp.arange(seq).astype(F32)[None, :]
        cos_t, sin_t = jnp.cos(ang), jnp.sin(ang)

        hm_loc, hk_loc, hs_loc = norm_m(c1, x_loc, ln_params)
        at_loc, du_loc, dhm_loc = mlp_own(hm_loc, dy_loc, w_up, w_down)
        dctx_loc = dot(w_out, dy_loc, 1, 1).astype(BF)

        x_rem = after(x_rem, dhm_loc, dctx_loc, cos_t, sin_t, w_t)
        hm_rem, hk_rem, hs_rem = norm_m(c1, x_rem, ln_params)
        h_a, h_keep, h_send = norm_a(c1, x_loc, x_rem, ln_params)
        qkv_t = dot(w_t, h_a, 1, 1).astype(BF)

        dy_rem = after(dy_rem, qkv_t, h_keep, hm_rem)
        dka, dkb, dsa, dsb, uka, ukb, usa, usb, dhm_rem = mlp_peer(
            c1, hm_rem, dy_rem, dy_loc, (hk_loc, hs_loc, hk_rem, hs_rem), w_up, w_down, at_loc, du_loc)
        dctx_rem = dot(w_out, after(dy_rem, dhm_rem), 1, 1).astype(BF)

        dq, ctx, g_wdown, u_send, u_keep = attention(
            qkv_t, dctx_loc, dctx_rem, cos_t, sin_t, (dka, dkb, dsa, dsb), (uka, ukb, usa, usb), hd)
        grad_x, sums, g_wqkv, g_wout, g_wup = tail(
            dq, ctx, h_keep, h_send, w_t, x_loc, x_rem, dhm_loc, dhm_rem, dy_loc, dy_rem, ln_params, u_keep, u_send, hd)
        grad_x = grad_x[None]
        g_wqkv = g_wqkv.reshape(heads, 3, hd, d // dp).transpose(3, 0, 1, 2)
        return grad_x, sums, g_wqkv, g_wout, g_wup, g_wdown

    return jax.shard_map(
        local_step,
        mesh=mesh,
        in_specs=(P("dp", "tp"), P("dp", "tp"), P(), P(None, "tp"), P("tp"), P(None, "tp"), P("tp")),
        out_specs=(P("dp", "tp"), P(), P("dp", "tp"), P(("tp", "dp")), P("dp", "tp"), P(("tp", "dp"))),
        check_vma=False,
    )
```

```python
import functools

import jax
import jax.numpy as jnp
from jax import lax
from jax.experimental import pallas as pl
from jax.experimental.pallas import tpu as pltpu
from jax.sharding import PartitionSpec as P

NORM_EPS = 1e-5
ROPE_BASE = 10000.0
BF = jnp.bfloat16
F32 = jnp.float32
SQRT_HALF = 0.7071067811865476
INV_SQRT_2PI = 0.3989422804014327
VMEM_LIMIT = 60 * 1024 * 1024


def dot(a, b, ca, cb):
    return lax.dot_general(a, b, (((ca,), (cb,)), ((), ())), preferred_element_type=F32)


def params():
    return pltpu.CompilerParams(vmem_limit_bytes=VMEM_LIMIT)


def cost(flops, nbytes, trans=0):
    return pl.CostEstimate(flops=int(flops), bytes_accessed=int(nbytes), transcendentals=int(trans))


def normalized(x):
    cen = x - jnp.mean(x, axis=-1, keepdims=True)
    rstd = lax.rsqrt(jnp.mean(cen * cen, axis=-1, keepdims=True) + NORM_EPS)
    return cen * rstd, rstd


def norm_m_kernel(c_ref, x_ref, ln_ref, hm_ref, hk_ref, hs_ref):
    hm = (normalized(x_ref[...].astype(F32))[0] * ln_ref[2:3, :] + ln_ref[3:4, :]).astype(BF)
    hm_ref[...] = hm
    n = hm.shape[1] // 8
    for j in range(4):
        even, odd = hm[:, 2 * j * n:(2 * j + 1) * n].T, hm[:, (2 * j + 1) * n:(2 * j + 2) * n].T
        hk_ref[j * n:(j + 1) * n, :] = jnp.where(c_ref[0] == 0, even, odd)
        hs_ref[j * n:(j + 1) * n, :] = jnp.where(c_ref[0] == 0, odd, even)


def norm_m(core, x, ln, bt=256):
    rows, d = x.shape
    tok = pl.BlockSpec((bt, d), lambda i, c: (i, 0))
    return pl.pallas_call(
        norm_m_kernel,
        grid_spec=pltpu.PrefetchScalarGridSpec(
            num_scalar_prefetch=1,
            grid=(rows // bt,),
            in_specs=[tok, pl.BlockSpec((4, d), lambda i, c: (0, 0))],
            out_specs=[tok] + [pl.BlockSpec((d // 2, bt), lambda i, c: (0, i))] * 2,
        ),
        out_shape=[jax.ShapeDtypeStruct((rows, d), BF)] + [jax.ShapeDtypeStruct((d // 2, rows), BF)] * 2,
        compiler_params=params(),
        cost_estimate=cost(3e9, rows * d * 6),
        name="norm_m",
    )(core, x, ln)


def norm_a_kernel(c_ref, xl_ref, xr_ref, ln_ref, ha_ref, hk_ref, hs_ref, *, nb):
    def run(x_ref):
        ha = (normalized(x_ref[...].astype(F32))[0] * ln_ref[0:1, :] + ln_ref[1:2, :]).astype(BF)
        ha_ref[...] = ha
        n = ha.shape[1] // 8
        for j in range(4):
            even, odd = ha[:, 2 * j * n:(2 * j + 1) * n], ha[:, (2 * j + 1) * n:(2 * j + 2) * n]
            hk_ref[:, j * n:(j + 1) * n] = jnp.where(c_ref[0] == 0, even, odd)
            hs_ref[:, j * n:(j + 1) * n] = jnp.where(c_ref[0] == 0, odd, even)

    pl.when(pl.program_id(0) < nb)(lambda: run(xl_ref))
    pl.when(pl.program_id(0) >= nb)(lambda: run(xr_ref))


def norm_a(core, x_loc, x_rem, ln, bt=256):
    rows, d = x_loc.shape
    nb = rows // bt
    tok = lambda w: pl.BlockSpec((bt, w), lambda i, c: (i, 0))
    return pl.pallas_call(
        functools.partial(norm_a_kernel, nb=nb),
        grid_spec=pltpu.PrefetchScalarGridSpec(
            num_scalar_prefetch=1,
            grid=(2 * nb,),
            in_specs=[
                pl.BlockSpec((bt, d), lambda i, c: (jnp.minimum(i, nb - 1), 0)),
                pl.BlockSpec((bt, d), lambda i, c: (jnp.maximum(i - nb, 0), 0)),
                pl.BlockSpec((4, d), lambda i, c: (0, 0)),
            ],
            out_specs=[tok(d), tok(d // 2), tok(d // 2)],
        ),
        out_shape=[jax.ShapeDtypeStruct((2 * rows, w), BF) for w in (d, d // 2, d // 2)],
        compiler_params=params(),
        cost_estimate=cost(6e9, rows * d * 12),
        name="norm_a",
    )(core, x_loc, x_rem, ln)


MESH = pl.DeviceIdType.MESH


def partners():
    me, t = lax.axis_index("dp"), lax.axis_index("tp")
    c, xx, yy = me % 2, (me // 2) % 2, me // 4
    way = {"c": {"dp": me + 1 - 2 * c}, "x": {"dp": me + 2 - 4 * xx}, "y": {"dp": me + 4 - 8 * yy}, "z": {"tp": 1 - t}}
    return way, t, c, xx, yy


def meet(way, names):
    barrier = pltpu.get_barrier_semaphore()
    for p in names:
        pl.semaphore_signal(barrier, inc=1, device_id=way[p], device_id_type=MESH)
    pl.semaphore_wait(barrier, len(names))


def by_rows(n, chunk, f):
    def body(i, _):
        f(pl.ds(pl.multiple_of(i * chunk, 8), chunk))
        return _

    lax.fori_loop(0, n // chunk, body, 0)


WAYS = ("x", "y"), ("y", "x")


def attn_kernel(qkv_ref, dol_ref, dor_ref, cos_ref, sin_ref,
                d_out, d_stay, uka, ukb, usa, usb,
                dqkv_ref, ctx_ref, gd_ref, us_ref, uk_ref,
                dk_ref, dv_ref, d_keep, u_keep, u_got, d1_got, u1_send, u1_got, d2_send, d2_got,
                load_sem, send_sem, recv_sem, *, bq, hd):
    way, t, _, xx, yy = partners()
    step = pl.program_id(0)
    last = pl.num_programs(0) - 1

    def remote(i, src, dst, w):
        return pltpu.make_async_remote_copy(
            src_ref=src, dst_ref=dst, send_sem=send_sem.at[i], recv_sem=recv_sem.at[i], device_id=way[w], device_id_type=MESH)

    core_u = [remote(2 + k, src, u_got.at[k], "c") for k, src in enumerate((usa, usb))]
    first_d = [remote(k, d_out.at[k], d1_got.at[k], WAYS[k][0]) for k in range(2)]
    second_d = [remote(4 + k, d2_send.at[k], d2_got.at[k], WAYS[k][1]) for k in range(2)]
    first_u = [remote(6 + k, u1_send.at[k], u1_got.at[k], WAYS[k][0]) for k in range(2)]
    load_d = pltpu.make_async_copy(d_stay, d_keep, load_sem.at[0])
    load_u = [pltpu.make_async_copy(src, u_keep.at[k], load_sem.at[2 + k]) for k, src in enumerate((uka, ukb))]

    leave = [lambda i: 2 * i + 1 - xx, lambda i: 2 * (1 - yy) + i]
    stay = [lambda i: 2 * i + xx, lambda i: 2 * yy + i]
    mine = [yy, xx]

    @pl.when(step == 0)
    def _():
        meet(way, "cxy")
        for v in first_d + core_u + [load_d] + load_u:
            v.start()

    @pl.when(step == 3)
    def _():
        for k in range(2):
            load_u[k].wait()
            core_u[k].wait()
            for i in range(2):
                def add(r):
                    for j in range(u_keep.shape[1]):
                        u1_send[k, i, j, r, :] = u_keep[k, j, leave[k](i), r, :] + u_got[k, j, leave[k](i), r, :]
                        u_keep[k, j, stay[k](i), r, :] += u_got[k, j, stay[k](i), r, :]

                by_rows(u_keep.shape[3], 16, add)
            first_u[k].start()

    @pl.when(step == 4)
    def _():
        load_d.wait()
        for k in range(2):
            first_d[k].wait()
            m = mine[k]

            def add(r):
                d2_send[k, r, :] = d_keep[k, 1 - m, r, :] + d1_got[k, 1 - m, r, :]
                d_keep[k, m, r, :] += d1_got[k, m, r, :]

            by_rows(d_keep.shape[2], 32, add)
            second_d[k].start()

    @pl.when(step == last)
    def _():
        for k in range(2):
            first_u[k].wait()
            m = mine[k]

            def add(r):
                for j in range(u_keep.shape[1]):
                    us_ref[k, j, r, :] = u_keep[k, j, stay[k](1 - m), r, :] + u1_got[k, 1 - m, j, r, :]
                    uk_ref[k, j, r, :] = u_keep[k, j, stay[k](m), r, :] + u1_got[k, m, j, r, :]

            by_rows(u_keep.shape[3], 16, add)

    attn_head(t, qkv_ref, dol_ref, dor_ref, cos_ref, sin_ref, dqkv_ref, ctx_ref, dk_ref, dv_ref, bq, hd)

    @pl.when(step == last)
    def _():
        w = d_keep.shape[3]
        for k in range(2):
            second_d[k].wait()
            m = mine[k]

            def add(r):
                gd_ref[r, k * w:(k + 1) * w] = d_keep[k, m, r, :] + d2_got[k, r, :]

            by_rows(d_keep.shape[2], 32, add)


def attn_head(t, qkv_ref, dol_ref, dor_ref, cos_ref, sin_ref, dqkv_ref, ctx_ref, dk_ref, dv_ref, bq, hd):
    seq = qkv_ref.shape[1]
    half = hd // 2
    part = dol_ref.shape[1]
    cos, sin = cos_ref[...], sin_ref[...]

    def in_order(own, peer):
        return jnp.concatenate([jnp.where(t == 0, own, peer), jnp.where(t == 0, peer, own)], axis=1)

    def place(lo, n):
        slot = t if lo < part else 1 - t
        return pl.ds(pl.multiple_of(slot * part + lo % part, 128), n)

    def rope(v):
        lo, hi = v[:half].astype(F32), v[half:].astype(F32)
        return jnp.concatenate([lo * cos - hi * sin, hi * cos + lo * sin], axis=0).astype(BF)

    def rope_back(d, c, s):
        lo, hi = d[:half].astype(BF).astype(F32), d[half:].astype(BF).astype(F32)
        return jnp.concatenate([lo * c + hi * s, hi * c - lo * s], axis=0).astype(BF)

    scale = hd ** -0.5
    qkv = in_order(qkv_ref[:, :part], qkv_ref[:, part:])
    q_t = rope(qkv[0:hd])
    k_t = rope(qkv[hd:2 * hd])
    v_t = qkv[2 * hd:3 * hd]
    q_t = (q_t.astype(F32) * scale).astype(BF)
    do_t = in_order(dol_ref[...], dor_ref[...])
    q_n, do_n, k_n, v_n = q_t.T, do_t.T, k_t.T, v_t.T
    tri = lax.broadcasted_iota(jnp.int32, (bq, bq), 0) <= lax.broadcasted_iota(jnp.int32, (bq, bq), 1)
    for i in range(seq // bq):
        lo, nk = i * bq, (i + 1) * bq
        blocks = [slice(j * bq, (j + 1) * bq) for j in range(i + 1)]
        q_b, do_b = q_t[:, lo:nk], do_t[:, lo:nk]
        ss = [dot(k_n[b], q_b, 1, 0) for b in blocks]
        ss[i] = jnp.where(tri, ss[i], -1e30)
        m = functools.reduce(jnp.maximum, [jnp.max(s, axis=0, keepdims=True) for s in ss])
        es = [jnp.exp(s - m) for s in ss]
        r = 1.0 / sum(jnp.sum(e, axis=0, keepdims=True) for e in es)
        ps = [e * r for e in es]
        pbs = [p.astype(BF) for p in ps]
        dps = [dot(v_n[b], do_b, 1, 0).astype(BF) for b in blocks]
        delta = sum(jnp.sum(p * d.astype(F32), axis=0, keepdims=True) for p, d in zip(ps, dps))
        dss = [(p * (d.astype(F32) - delta)).astype(BF) for p, d in zip(ps, dps)]
        ctx_ref[:, place(lo, bq)] = sum(dot(v_t[:, b], p, 1, 0) for b, p in zip(blocks, pbs)).astype(BF)
        dq = sum(dot(k_t[:, b], d, 1, 0) for b, d in zip(blocks, dss)) * scale
        dqkv_ref[0:hd, place(lo, bq)] = rope_back(dq, cos[:, lo:nk], sin[:, lo:nk])
        for j, b in enumerate(blocks):
            dv_new = dot(pbs[j], do_n[lo:nk], 1, 0)
            dk_new = dot(dss[j], q_n[lo:nk], 1, 0)
            if j < i:
                dv_ref[b, :] += dv_new
                dk_ref[b, :] += dk_new
            else:
                dv_ref[b, :] = dv_new
                dk_ref[b, :] = dk_new
    dk = rope_back(dk_ref[...].T, cos, sin)
    dv = dv_ref[...].T.astype(BF)
    for lo in (0, part):
        dqkv_ref[hd:2 * hd, place(lo, part)] = dk[:, lo:lo + part]
        dqkv_ref[2 * hd:3 * hd, place(lo, part)] = dv[:, lo:lo + part]


def attention(qkv_t, dol, dor, cos_t, sin_t, down, up, hd, bq=256):
    rows, seq = qkv_t.shape
    heads = rows // (3 * hd)
    part = dol.shape[1]
    const = pl.BlockSpec((hd // 2, seq), lambda g: (0, 0))
    row = lambda r, w: pl.BlockSpec((r, w), lambda g: (g, 0))
    hbm = pl.BlockSpec(memory_space=pl.ANY)
    dsh, ush = down[0].shape, up[0].shape
    dred, ured = dsh[2:], (ush[0],) + ush[2:]
    gd_shape = (dred[0], 2 * dred[1])
    whole = lambda *shape: pl.BlockSpec(shape, lambda g: (0,) * len(shape))
    f = lambda *shape: pltpu.VMEM(shape, F32)
    sds = jax.ShapeDtypeStruct
    return pl.pallas_call(
        functools.partial(attn_kernel, bq=bq, hd=hd),
        grid=(heads,),
        in_specs=[row(3 * hd, seq), row(hd, part), row(hd, part), const, const] + [hbm] * 6,
        out_specs=[row(3 * hd, seq), row(hd, seq), whole(*gd_shape), whole(2, *ured), whole(2, *ured)],
        out_shape=[sds((rows, seq), BF), sds((heads * hd, seq), BF), sds(gd_shape, F32), sds((2,) + ured, F32), sds((2,) + ured, F32)],
        scratch_shapes=[
            f(seq, hd), f(seq, hd), f(*dsh), f(2, *ush), f(2, *ush),
            f(*dsh), f(2, 2, *ured), f(2, 2, *ured), f(2, *dred), f(2, *dred),
            pltpu.SemaphoreType.DMA((4,)), pltpu.SemaphoreType.DMA((10,)), pltpu.SemaphoreType.DMA((10,)),
        ],
        compiler_params=pltpu.CompilerParams(vmem_limit_bytes=VMEM_LIMIT, collective_id=1, has_side_effects=True),
        cost_estimate=cost(heads * 6e9, heads << 20, seq * seq * heads // 2),
        name="attn",
    )(qkv_t, dol, dor, cos_t, sin_t, *down, *up)


def gelu_pair(h_ref, dy_ref, wu, wd, rows):
    u = dot(h_ref[rows, :], wu, 1, 0).astype(BF).astype(F32)
    dg = dot(dy_ref[rows, :], wd, 1, 1).astype(BF).astype(F32)
    cdf = 0.5 + 0.5 * lax.erf(u * SQRT_HALF)
    pdf = jnp.exp(-0.5 * u * u) * INV_SQRT_2PI
    return (u * cdf).astype(BF), (dg * (cdf + u * pdf)).astype(BF)


def mlp_own_kernel(h_ref, dy_ref, wu_ref, wd_ref, at_ref, du_ref, dh_ref, acc_ref, *, tc):
    step = pl.program_id(0)
    wu, wd = wu_ref[...], wd_ref[...]
    for k in range(h_ref.shape[0] // tc):
        rows = pl.ds(k * tc, tc)
        a, du = gelu_pair(h_ref, dy_ref, wu, wd, rows)
        at_ref[:, rows] = a.T
        du_ref[0, rows, :] = du
        add = dot(du, wu, 1, 1)

        @pl.when(step == 0)
        def _():
            acc_ref[rows, :] = add

        @pl.when(step > 0)
        def _():
            acc_ref[rows, :] += add

    @pl.when(step == pl.num_programs(0) - 1)
    def _():
        dh_ref[...] = acc_ref[...].astype(BF)


def mlp_own(h, dy, w_up, w_down, n=4, tc=256):
    seq, d = h.shape
    ff = w_up.shape[1]
    fb = ff // n
    full = pl.BlockSpec((seq, d), lambda i: (0, 0))
    return pl.pallas_call(
        functools.partial(mlp_own_kernel, tc=tc),
        grid=(n,),
        in_specs=[full, full, pl.BlockSpec((d, fb), lambda i: (0, i)), pl.BlockSpec((fb, d), lambda i: (i, 0))],
        out_specs=[pl.BlockSpec((fb, seq), lambda i: (i, 0)), pl.BlockSpec((1, seq, fb), lambda i: (i, 0, 0)), full],
        out_shape=[jax.ShapeDtypeStruct((ff, seq), BF), jax.ShapeDtypeStruct((n, seq, fb), BF), jax.ShapeDtypeStruct((seq, d), BF)],
        scratch_shapes=[pltpu.VMEM((seq, d), F32)],
        compiler_params=params(),
        cost_estimate=cost(6 * seq * d * ff, 20 << 20, 2 * seq * ff),
        name="mlp_own",
    )(h, dy, w_up, w_down)


def mlp_pre_kernel(h_ref, wu_ref, at_ref, gp_ref, *, tc):
    wu = wu_ref[...]
    for k in range(h_ref.shape[0] // tc):
        rows = pl.ds(k * tc, tc)
        u = dot(h_ref[rows, :], wu, 1, 0).astype(BF).astype(F32)
        cdf = 0.5 + 0.5 * lax.erf(u * SQRT_HALF)
        pdf = jnp.exp(-0.5 * u * u) * INV_SQRT_2PI
        at_ref[:, rows] = (u * cdf).astype(BF).T
        gp_ref[0, rows, :] = cdf + u * pdf


def mlp_pre(h, w_up, n=4, tc=256):
    seq, d = h.shape
    ff = w_up.shape[1]
    fb = ff // n
    return pl.pallas_call(
        functools.partial(mlp_pre_kernel, tc=tc),
        grid=(n,),
        in_specs=[pl.BlockSpec((seq, d), lambda i: (0, 0)), pl.BlockSpec((d, fb), lambda i: (0, i))],
        out_specs=[pl.BlockSpec((fb, seq), lambda i: (i, 0)), pl.BlockSpec((1, seq, fb), lambda i: (i, 0, 0))],
        out_shape=[jax.ShapeDtypeStruct((ff, seq), BF), jax.ShapeDtypeStruct((n, seq, fb), F32)],
        compiler_params=params(),
        cost_estimate=cost(2 * seq * d * ff, 16 << 20, 2 * seq * ff),
        name="mlp_pre",
    )(h, w_up)


def mlp_peer_kernel(dyr_ref, dyl_ref, hkl_ref, hsl_ref, hkr_ref, hsr_ref, wu_ref, wd_ref, wo_ref, at_ref, atr_ref, dul_ref, gp_ref,
                    d_out, d_stay, uka_ref, ukb_ref, usa_ref, usb_ref, dh_ref, dctx_ref,
                    acc_ref, du_ref, d_keep, d_send, d_got, send_sem, recv_sem, *, tc):
    way, _, c, xx, yy = partners()
    step = pl.program_id(0)
    last = pl.num_programs(0) - 1
    wu, wd = wu_ref[...], wd_ref[...]
    fb = wu.shape[1]
    m = fb // 2

    def remote(i):
        return pltpu.make_async_remote_copy(
            src_ref=d_send.at[i], dst_ref=d_got.at[i], send_sem=send_sem.at[i], recv_sem=recv_sem.at[i],
            device_id=way["c"], device_id_type=MESH)

    def combine(i):
        remote(i).wait()
        y, x = i // 2, i % 2
        for k, at, go in ((0, y, x != xx), (1, x, y != yy)):
            for ref, cond in ((d_out, go), (d_stay, jnp.logical_not(go))):
                @pl.when(cond)
                def _():
                    def add(r):
                        ref[k, at, r, :] = d_keep[i, k, r, :] + d_got[i, k, r, :]

                    by_rows(m, 32, add)

    pl.when(step == 0)(lambda: meet(way, "c"))
    dctx_ref[...] = dot(wo_ref[...], dyr_ref[...], 1, 1).astype(BF)

    @pl.when(step == 0)
    def _():
        acc_ref[...] = jnp.zeros_like(acc_ref)

    for k in range(dyr_ref.shape[0] // tc):
        rows = pl.ds(k * tc, tc)
        dg = dot(dyr_ref[rows, :], wd, 1, 1).astype(BF).astype(F32)
        du = (dg * gp_ref[0, rows, :]).astype(BF)
        du_ref[rows, :] = du
        acc_ref[rows, :] += dot(du, wu, 1, 1)
    for side, ref in ((1 - c, d_send), (c, d_keep)):
        block = pl.ds(pl.multiple_of(side * m, 128), m)
        g = dot(at_ref[block, :], dyl_ref[...], 1, 0) + dot(atr_ref[block, :], dyr_ref[...], 1, 0)
        w = g.shape[1] // 2
        ref[step, 0] = g[:, :w]
        ref[step, 1] = g[:, w:]
        if ref is d_send:
            remote(step).start()
    for hl, hr, ra, rb in ((hkl_ref, hkr_ref, uka_ref, ukb_ref), (hsl_ref, hsr_ref, usa_ref, usb_ref)):
        g = dot(hl[...], dul_ref[0], 1, 0) + dot(hr[...], du_ref[...], 1, 0)
        n = g.shape[0] // 4
        for j in range(4):
            ra[0, j] = g[j * n:(j + 1) * n, :m]
            rb[0, j] = g[j * n:(j + 1) * n, m:]

    pl.when(step > 0)(lambda: combine(step - 1))

    @pl.when(step == last)
    def _():
        combine(step)
        dh_ref[...] = acc_ref[...].astype(BF)


def mlp_peer(dy_rem, dy_loc, hts, w_up, w_down, w_out, at, at_rem, du, slope, n=4, tc=256):
    seq, d = dy_rem.shape
    ff = w_up.shape[1]
    fb = ff // n
    ctx = w_out.shape[0]
    full = lambda r, w: pl.BlockSpec((r, w), lambda i: (0, 0))
    rows = lambda r, w: pl.BlockSpec((r, w), lambda i: (i, 0))
    dshape = (2, 2, fb // 2, d // 2)
    dspec = pl.BlockSpec(dshape, lambda i: (0, 0, 0, 0))
    uspec = pl.BlockSpec((1, 4, d // 8, fb // 2), lambda i: (i, 0, 0, 0))
    act = pl.BlockSpec((1, seq, fb), lambda i: (i, 0, 0))
    sds = jax.ShapeDtypeStruct
    slots = pltpu.VMEM((n, 2, fb // 2, d // 2), F32)
    return pl.pallas_call(
        functools.partial(mlp_peer_kernel, tc=tc),
        grid=(n,),
        in_specs=[full(seq, d)] * 2 + [full(d // 2, seq)] * 4 + [
            pl.BlockSpec((d, fb), lambda i: (0, i)), rows(fb, d), rows(ctx // n, d), rows(fb, seq), rows(fb, seq), act, act],
        out_specs=[dspec] * 2 + [uspec] * 4 + [full(seq, d), rows(ctx // n, seq)],
        out_shape=[sds(dshape, F32)] * 2 + [sds((n, 4, d // 8, fb // 2), F32)] * 4 + [sds((seq, d), BF), sds((ctx, seq), BF)],
        scratch_shapes=[pltpu.VMEM((seq, d), F32), pltpu.VMEM((seq, fb), BF), slots, slots, slots,
                        pltpu.SemaphoreType.DMA((n,)), pltpu.SemaphoreType.DMA((n,))],
        compiler_params=pltpu.CompilerParams(vmem_limit_bytes=63 * 1024 * 1024, collective_id=2, has_side_effects=True),
        cost_estimate=cost(14 * seq * d * ff, 40 << 20),
        name="mlp_peer",
    )(dy_rem, dy_loc, *hts, w_up, w_down, w_out, at, at_rem, du, slope)


def tail_kernel(*refs, bt, hd):
    n_in = 13
    hbm, us_ref, refs = refs[:n_in], refs[n_in], refs[n_in + 1:]
    (gx_ref, sums_ref, gq_ref, gw_ref, gu_ref), refs = refs[:5], refs[5:]
    vm, refs = refs[:n_in], refs[n_in:]
    (z_send, z_recv, sum_src, sum_got, q_keep, q_send, q_recv, w_keep, w_send, w_recv,
     q1_send, q1_recv, w1_send, w1_recv, q2_send, q2_recv, w2_send, w2_recv, u2_recv,
     in_sem, send_sem, recv_sem) = refs
    dq, ctx, hk, hs, wt, xl, xr, dhl, dhr, dyl, dyr, ln, uk = vm
    way_to, t, c, xx, yy = partners()
    part = xl.shape[0]
    gr = dq.shape[0] // 4

    loads = [pltpu.make_async_copy(src, dst, in_sem.at[i]) for i, (src, dst) in enumerate(zip(hbm, vm))]
    for i in (0, 4, 6, 8, 11, 3, 2, 1, 9, 10, 5, 7, 12):
        loads[i].start()
    meet(way_to, "cxyz")

    count = [0]

    def send(src, dst, way):
        i = count[0]
        count[0] += 1
        copy = pltpu.make_async_remote_copy(
            src_ref=src, dst_ref=dst, send_sem=send_sem.at[i], recv_sem=recv_sem.at[i],
            device_id=way_to[way], device_id_type=MESH)
        copy.start()
        return copy

    def need(*idx):
        for i in idx:
            loads[i].wait()

    def block(x_ref, dh_ref, b, peer):
        rows = pl.ds(b * bt, bt)
        cols = pl.ds((part if peer else 0) + b * bt, bt)
        dha = dot(dq[:, cols], wt[...], 0, 0).astype(BF).astype(F32)
        dhm = dh_ref[rows, :].astype(F32)
        xh, rstd = normalized(x_ref[rows, :].astype(F32))
        dxh = (dha * ln[0:1, :] + dhm * ln[2:3, :]).astype(BF)
        parts = [dha * xh, dha, dhm * xh, dhm]
        return dxh, jnp.concatenate([jnp.sum(p, axis=0, keepdims=True) for p in parts], axis=0)

    def peer_block(b):
        dxh, s = block(xr, dhr, b, True)
        z_send[b] = dxh
        if b == 0:
            sum_src[0] = s
        else:
            sum_src[0] += s
        return send(z_send.at[b], z_recv.at[b], "z")

    def looped(start, n, f):
        def body(i, _):
            f(i)
            return _

        lax.fori_loop(start, start + n, body, 0)

    def qkv_grad(h_ref, out_ref, g):
        r = dot(dq[pl.ds(pl.multiple_of(g * gr, 128), gr), :], h_ref[...], 1, 0)
        n = r.shape[1] // 4
        for j in range(4):
            out_ref[g, j] = r[:, j * n:(j + 1) * n]

    def out_grad(want, out_ref):
        cx = jnp.concatenate([jnp.where(want == 0, ctx[2 * j * hd:(2 * j + 1) * hd, :], ctx[(2 * j + 1) * hd:(2 * j + 2) * hd, :])
                              for j in range(4)], axis=0)
        r = dot(cx[:, :part], dyl[...], 1, 0) + dot(cx[:, part:], dyr[...], 1, 0)
        m = r.shape[1] // 2
        for j in range(4):
            for k in range(2):
                out_ref[k, j] = r[j * hd:(j + 1) * hd, k * m:(k + 1) * m]

    def first(keep, got, out, k):
        for i in range(2):
            s_idx = 2 * i + 1 - xx if k == 0 else 2 * (1 - yy) + i
            k_idx = 2 * i + xx if k == 0 else 2 * yy + i
            out[i] = keep[s_idx] + got[s_idx]
            got[k_idx] = keep[k_idx] + got[k_idx]

    def second(got, got1, out, k):
        mine, other = (yy, 1 - yy) if k == 0 else (xx, 1 - xx)
        at = (lambda i: 2 * i + xx) if k == 0 else (lambda i: 2 * yy + i)
        out[...] = got[at(other)] + got1[other]
        return got[at(mine)] + got1[mine]

    ways = ("x", "y"), ("y", "x")

    us = [send(us_ref.at[k], u2_recv.at[k], ways[k][1]) for k in range(2)]
    need(0, 4, 6, 8, 11)
    zs = [peer_block(0)]
    q1, q2 = [None] * 4, [None] * 4
    n = gq_ref.shape[0] // 4

    def q_first(g):
        first(q_keep.at[g], q_recv.at[g], q1_send.at[g], g % 2)
        q1[g] = send(q1_send.at[g], q1_recv.at[g], ways[g % 2][0])

    def q_second(g):
        q1[g].wait()
        gq_ref[g * n:(g + 1) * n, :] = second(q_recv.at[g], q1_recv.at[g], q2_send.at[g], g % 2)
        q2[g] = send(q2_send.at[g], q2_recv.at[g], ways[g % 2][1])

    need(3)
    for g in (0, 2):
        looped(g, 2, lambda i: qkv_grad(hs, q_send, i))
        qc = send(q_send.at[pl.ds(g, 2)], q_recv.at[pl.ds(g, 2)], "c")
        if g == 0:
            need(2)
        else:
            zs.append(peer_block(1))
        looped(g, 2, lambda i: qkv_grad(hk, q_keep, i))
        qc.wait()
        q_first(g)
        q_first(g + 1)
    zs.append(peer_block(2))
    q_second(0)
    q_second(1)
    need(1, 9, 10)
    out_grad(1 - c, w_send)
    wc = send(w_send, w_recv, "c")
    out_grad(c, w_keep)
    wc.wait()
    w1 = []
    for k in range(2):
        first(w_keep.at[k], w_recv.at[k], w1_send.at[k], k)
        w1.append(send(w1_send.at[k], w1_recv.at[k], ways[k][0]))

    need(5, 7)

    def own_block(b):
        dxh, s = block(xl, dhl, b, False)
        gx_ref[pl.ds(b * bt, bt), :] = dxh
        sum_src[0] += s

    def grad_x(b):
        zs[b].wait()
        rows = pl.ds(b * bt, bt)
        dxh = gx_ref[rows, :].astype(F32) + z_recv[b].astype(F32)
        xh, rstd = normalized(xl[rows, :].astype(F32))
        dx = rstd * (dxh - jnp.mean(dxh, -1, keepdims=True) - xh * jnp.mean(dxh * xh, -1, keepdims=True))
        gx_ref[rows, :] = (dyl[rows, :].astype(F32) + dx).astype(BF)

    own_block(0)
    q_second(2)
    q_second(3)
    own_block(1)
    grad_x(0)
    own_block(2)
    sums = [send(sum_src.at[0], sum_got.at[0], "z")]
    grad_x(1)

    def sum_next(i, way):
        sums[-1].wait()
        sum_src[i] = sum_src[i - 1] + sum_got[i - 1]
        sums.append(send(sum_src.at[i], sum_got.at[i], way))

    sum_next(1, "c")
    need(12)
    blocks, m = uk.shape[1], uk.shape[3]
    for k in range(2):
        us[k].wait()
        for j in range(blocks):
            gu_ref[:, (2 * j + k) * m:(2 * j + k + 1) * m] = uk[k, j] + u2_recv[k, j]
    m = gw_ref.shape[1] // 2
    w2 = []
    for k in range(2):
        w1[k].wait()
        gw_ref[:, k * m:(k + 1) * m] = second(w_recv.at[k], w1_recv.at[k], w2_send.at[k], k)
        w2.append(send(w2_send.at[k], w2_recv.at[k], ways[k][1]))
    sum_next(2, "x")
    for g in (0, 1):
        q2[g].wait()
        gq_ref[g * n:(g + 1) * n, :] += q2_recv[g]
    sum_next(3, "y")
    for g in (2, 3):
        q2[g].wait()
        gq_ref[g * n:(g + 1) * n, :] += q2_recv[g]
    for k in range(2):
        w2[k].wait()
        gw_ref[:, k * m:(k + 1) * m] += w2_recv[k]
    sums[-1].wait()
    sums_ref[...] = sum_src[3] + sum_got[3]
    grad_x(2)


def tail(dq, ctx, h_keep, h_send, w_t, x_loc, x_rem, dhm_loc, dhm_rem, dy_loc, dy_rem, ln, u_keep, u_send, hd, bt=256):
    ins = [dq, ctx, h_keep, h_send, w_t, x_loc, x_rem, dhm_loc, dhm_rem, dy_loc, dy_rem, ln, u_keep]
    part, d = x_loc.shape
    rows = dq.shape[0] // 4
    nb = part // bt
    cols = d // 8
    f = lambda *shape: pltpu.VMEM(shape, F32)
    sds = jax.ShapeDtypeStruct
    scratch = [pltpu.VMEM(v.shape, v.dtype) for v in ins] + [
        pltpu.VMEM((nb, bt, d), BF), pltpu.VMEM((nb, bt, d), BF), f(4, 4, d), f(4, 4, d),
        f(4, 4, rows, cols), f(4, 4, rows, cols), f(4, 4, rows, cols),
        f(2, 4, hd, d // 2), f(2, 4, hd, d // 2), f(2, 4, hd, d // 2),
        f(4, 2, rows, cols), f(4, 2, rows, cols), f(2, 2, hd, d // 2), f(2, 2, hd, d // 2),
        f(4, rows, cols), f(4, rows, cols), f(2, hd, d // 2), f(2, hd, d // 2), f(*u_send.shape),
        pltpu.SemaphoreType.DMA((len(ins),)), pltpu.SemaphoreType.DMA((32,)), pltpu.SemaphoreType.DMA((32,)),
    ]
    vm = pl.BlockSpec(memory_space=pltpu.VMEM)
    u_cols = u_keep.shape[0] * u_keep.shape[1] * u_keep.shape[3]
    return pl.pallas_call(
        functools.partial(tail_kernel, bt=bt, hd=hd),
        in_specs=[pl.BlockSpec(memory_space=pl.ANY)] * (len(ins) + 1),
        out_specs=[vm] * 5,
        out_shape=[sds((part, d), BF), sds((4, d), F32), sds((4 * rows, cols), F32), sds((hd, d), F32), sds((u_keep.shape[2], u_cols), F32)],
        scratch_shapes=scratch,
        compiler_params=pltpu.CompilerParams(vmem_limit_bytes=VMEM_LIMIT, collective_id=0, has_side_effects=True),
        cost_estimate=cost(4e10, 40 << 20),
        name="tail",
    )(*ins, u_send)


def emit_kernel(*refs, n):
    ins, outs, bufs, (sem_in, sem_out) = refs[:n], refs[n:2 * n], refs[2 * n:3 * n], refs[3 * n:]
    get = [pltpu.make_async_copy(ins[i], bufs[i], sem_in.at[i]) for i in range(n)]
    put = [pltpu.make_async_copy(bufs[i], outs[i], sem_out.at[i]) for i in range(n)]
    for v in get:
        v.start()
    for i in range(n):
        get[i].wait()
        put[i].start()
    for v in put:
        v.wait()


def emit(*arrays):
    n = len(arrays)
    hbm = pl.BlockSpec(memory_space=pl.ANY)
    return pl.pallas_call(
        functools.partial(emit_kernel, n=n),
        in_specs=[hbm] * n,
        out_specs=[hbm] * n,
        out_shape=[jax.ShapeDtypeStruct(v.shape, v.dtype) for v in arrays],
        scratch_shapes=[pltpu.VMEM(v.shape, v.dtype) for v in arrays]
        + [pltpu.SemaphoreType.DMA((n,)), pltpu.SemaphoreType.DMA((n,))],
        compiler_params=params(),
        cost_estimate=cost(1e6, 10 << 20),
        name="emit",
    )(*arrays)


def solution(mesh):
    dp = mesh.shape["dp"]
    tp = mesh.shape["tp"]

    def swap_tp(v):
        return lax.ppermute(v, "tp", [(i, i ^ 1) for i in range(tp)])

    def after(v, *deps):
        return lax.optimization_barrier((v,) + deps)[0]

    def local_step(x_loc, dy_loc, ln_params, w_qkv, w_out, w_up, w_down):
        x_loc, dy_loc = x_loc[0], dy_loc[0]
        half, d = x_loc.shape
        seq = half * tp
        heads, hd = w_qkv.shape[1], w_qkv.shape[3]
        me = lax.axis_index("dp")
        c1 = (me % 2).astype(jnp.int32)[None]

        x_rem = swap_tp(x_loc)
        dy_rem = swap_tp(dy_loc)

        w_t = w_qkv.transpose(1, 2, 3, 0).reshape(heads * 3 * hd, d)
        inv_freq = ROPE_BASE ** (-2.0 * jnp.arange(hd // 2, dtype=F32) / hd)
        ang = inv_freq[:, None] * jnp.arange(seq).astype(F32)[None, :]
        cos_t, sin_t = jnp.cos(ang), jnp.sin(ang)

        hm_loc, hk_loc, hs_loc = norm_m(c1, x_loc, ln_params)
        at_loc, du_loc, dhm_loc = mlp_own(hm_loc, dy_loc, w_up, w_down)
        dctx_loc = dot(w_out, dy_loc, 1, 1).astype(BF)

        x_rem = after(x_rem, dhm_loc, dctx_loc, cos_t, sin_t, w_t)
        hm_rem, hk_rem, hs_rem = norm_m(c1, x_rem, ln_params)
        h_a, h_keep, h_send = norm_a(c1, x_loc, x_rem, ln_params)
        qkv_t = dot(w_t, h_a, 1, 1).astype(BF)

        at_rem, slope = mlp_pre(after(hm_rem, qkv_t), w_up)

        dy_rem = after(dy_rem, qkv_t, h_keep, slope)
        d_out, d_stay, uka, ukb, usa, usb, dhm_rem, dctx_rem = mlp_peer(
            dy_rem, dy_loc, (hk_loc, hs_loc, hk_rem, hs_rem), w_up, w_down, w_out, at_loc, at_rem, du_loc, slope)
        dq, ctx, g_wdown, u_send, u_keep = attention(
            qkv_t, dctx_loc, dctx_rem, cos_t, sin_t, (d_out, d_stay), (uka, ukb, usa, usb), hd)
        grad_x, sums, g_wqkv, g_wout, g_wup, g_wdown = emit(*tail(
            dq, ctx, h_keep, h_send, w_t, x_loc, x_rem, dhm_loc, dhm_rem, dy_loc, dy_rem, ln_params, u_keep, u_send, hd), g_wdown)
        grad_x = grad_x[None]
        g_wqkv = g_wqkv.reshape(heads, 3, hd, d // dp).transpose(3, 0, 1, 2)
        return grad_x, sums, g_wqkv, g_wout, g_wup, g_wdown

    return jax.shard_map(
        local_step,
        mesh=mesh,
        in_specs=(P("dp", "tp"), P("dp", "tp"), P(), P(None, "tp"), P("tp"), P(None, "tp"), P("tp")),
        out_specs=(P("dp", "tp"), P(), P("dp", "tp"), P(("tp", "dp")), P("dp", "tp"), P(("tp", "dp"))),
        check_vma=False,
    )
```

```python
import functools

import jax
import jax.numpy as jnp
from jax import lax
from jax.experimental import pallas as pl
from jax.experimental.pallas import tpu as pltpu
from jax.sharding import PartitionSpec as P

NORM_EPS = 1e-5
ROPE_BASE = 10000.0
BF = jnp.bfloat16
F32 = jnp.float32
SQRT_HALF = 0.7071067811865476
INV_SQRT_2PI = 0.3989422804014327
VMEM_LIMIT = 60 * 1024 * 1024


def dot(a, b, ca, cb):
    return lax.dot_general(a, b, (((ca,), (cb,)), ((), ())), preferred_element_type=F32)


def params():
    return pltpu.CompilerParams(vmem_limit_bytes=VMEM_LIMIT)


def cost(flops, nbytes, trans=0):
    return pl.CostEstimate(flops=int(flops), bytes_accessed=int(nbytes), transcendentals=int(trans))


def normalized(x):
    cen = x - jnp.mean(x, axis=-1, keepdims=True)
    rstd = lax.rsqrt(jnp.mean(cen * cen, axis=-1, keepdims=True) + NORM_EPS)
    return cen * rstd, rstd


def norm_m_kernel(c_ref, x_ref, ln_ref, hm_ref, hk_ref, hs_ref):
    hm = (normalized(x_ref[...].astype(F32))[0] * ln_ref[2:3, :] + ln_ref[3:4, :]).astype(BF)
    hm_ref[...] = hm
    n = hm.shape[1] // 8
    for j in range(4):
        even, odd = hm[:, 2 * j * n:(2 * j + 1) * n].T, hm[:, (2 * j + 1) * n:(2 * j + 2) * n].T
        hk_ref[j * n:(j + 1) * n, :] = jnp.where(c_ref[0] == 0, even, odd)
        hs_ref[j * n:(j + 1) * n, :] = jnp.where(c_ref[0] == 0, odd, even)


def norm_m(core, x, ln, bt=256):
    rows, d = x.shape
    tok = pl.BlockSpec((bt, d), lambda i, c: (i, 0))
    return pl.pallas_call(
        norm_m_kernel,
        grid_spec=pltpu.PrefetchScalarGridSpec(
            num_scalar_prefetch=1,
            grid=(rows // bt,),
            in_specs=[tok, pl.BlockSpec((4, d), lambda i, c: (0, 0))],
            out_specs=[tok] + [pl.BlockSpec((d // 2, bt), lambda i, c: (0, i))] * 2,
        ),
        out_shape=[jax.ShapeDtypeStruct((rows, d), BF)] + [jax.ShapeDtypeStruct((d // 2, rows), BF)] * 2,
        compiler_params=params(),
        cost_estimate=cost(3e9, rows * d * 6),
        name="norm_m",
    )(core, x, ln)


def norm_a_kernel(c_ref, xl_ref, xr_ref, ln_ref, ha_ref, hk_ref, hs_ref, *, nb):
    def run(x_ref):
        ha = (normalized(x_ref[...].astype(F32))[0] * ln_ref[0:1, :] + ln_ref[1:2, :]).astype(BF)
        ha_ref[...] = ha
        n = ha.shape[1] // 8
        for j in range(4):
            even, odd = ha[:, 2 * j * n:(2 * j + 1) * n], ha[:, (2 * j + 1) * n:(2 * j + 2) * n]
            hk_ref[:, j * n:(j + 1) * n] = jnp.where(c_ref[0] == 0, even, odd)
            hs_ref[:, j * n:(j + 1) * n] = jnp.where(c_ref[0] == 0, odd, even)

    pl.when(pl.program_id(0) < nb)(lambda: run(xl_ref))
    pl.when(pl.program_id(0) >= nb)(lambda: run(xr_ref))


def norm_a(core, x_loc, x_rem, ln, bt=256):
    rows, d = x_loc.shape
    nb = rows // bt
    tok = lambda w: pl.BlockSpec((bt, w), lambda i, c: (i, 0))
    return pl.pallas_call(
        functools.partial(norm_a_kernel, nb=nb),
        grid_spec=pltpu.PrefetchScalarGridSpec(
            num_scalar_prefetch=1,
            grid=(2 * nb,),
            in_specs=[
                pl.BlockSpec((bt, d), lambda i, c: (jnp.minimum(i, nb - 1), 0)),
                pl.BlockSpec((bt, d), lambda i, c: (jnp.maximum(i - nb, 0), 0)),
                pl.BlockSpec((4, d), lambda i, c: (0, 0)),
            ],
            out_specs=[tok(d), tok(d // 2), tok(d // 2)],
        ),
        out_shape=[jax.ShapeDtypeStruct((2 * rows, w), BF) for w in (d, d // 2, d // 2)],
        compiler_params=params(),
        cost_estimate=cost(6e9, rows * d * 12),
        name="norm_a",
    )(core, x_loc, x_rem, ln)


MESH = pl.DeviceIdType.MESH


def partners():
    me, t = lax.axis_index("dp"), lax.axis_index("tp")
    c, xx, yy = me % 2, (me // 2) % 2, me // 4
    way = {"c": {"dp": me + 1 - 2 * c}, "x": {"dp": me + 2 - 4 * xx}, "y": {"dp": me + 4 - 8 * yy}, "z": {"tp": 1 - t}}
    return way, t, c, xx, yy


def meet(way, names):
    barrier = pltpu.get_barrier_semaphore()
    for p in names:
        pl.semaphore_signal(barrier, inc=1, device_id=way[p], device_id_type=MESH)
    pl.semaphore_wait(barrier, len(names))


def by_rows(n, chunk, f):
    def body(i, _):
        f(pl.ds(pl.multiple_of(i * chunk, 8), chunk))
        return _

    lax.fori_loop(0, n // chunk, body, 0)


WAYS = ("x", "y"), ("y", "x")


def attn_kernel(qkv_ref, dol_ref, dor_ref, cos_ref, sin_ref,
                d_out, d_stay, uka, ukb, usa, usb,
                dqkv_ref, ctx_ref, gd_ref, us_ref, uk_ref,
                dk_ref, dv_ref, d_keep, u_keep, u_got, d1_got, u1_send, u1_got, d2_send, d2_got, us_buf, uk_buf,
                load_sem, store_sem, send_sem, recv_sem, *, bq, hd):
    way, t, _, xx, yy = partners()
    step = pl.program_id(0)
    last = pl.num_programs(0) - 1

    def remote(i, src, dst, w):
        return pltpu.make_async_remote_copy(
            src_ref=src, dst_ref=dst, send_sem=send_sem.at[i], recv_sem=recv_sem.at[i], device_id=way[w], device_id_type=MESH)

    core_u = [remote(2 + k, src, u_got.at[k], "c") for k, src in enumerate((usa, usb))]
    first_d = [remote(k, d_out.at[k], d1_got.at[k], WAYS[k][0]) for k in range(2)]
    second_d = [remote(4 + k, d2_send.at[k], d2_got.at[k], WAYS[k][1]) for k in range(2)]
    first_u = [remote(6 + k, u1_send.at[k], u1_got.at[k], WAYS[k][0]) for k in range(2)]
    load_d = pltpu.make_async_copy(d_stay, d_keep, load_sem.at[0])
    stores = [pltpu.make_async_copy(v, o, store_sem.at[k]) for k, (v, o) in enumerate(((us_buf, us_ref), (uk_buf, uk_ref)))]
    load_u = [pltpu.make_async_copy(src, u_keep.at[k], load_sem.at[2 + k]) for k, src in enumerate((uka, ukb))]

    leave = [lambda i: 2 * i + 1 - xx, lambda i: 2 * (1 - yy) + i]
    stay = [lambda i: 2 * i + xx, lambda i: 2 * yy + i]
    mine = [yy, xx]

    @pl.when(step == 0)
    def _():
        meet(way, "cxy")
        for v in first_d + core_u + [load_d] + load_u:
            v.start()

    @pl.when(step == 3)
    def _():
        for k in range(2):
            load_u[k].wait()
            core_u[k].wait()
            for i in range(2):
                def add(r):
                    for j in range(u_keep.shape[1]):
                        u1_send[k, i, j, r, :] = u_keep[k, j, leave[k](i), r, :] + u_got[k, j, leave[k](i), r, :]
                        u_keep[k, j, stay[k](i), r, :] += u_got[k, j, stay[k](i), r, :]

                by_rows(u_keep.shape[3], 16, add)
            first_u[k].start()

    @pl.when(step == 4)
    def _():
        load_d.wait()
        for k in range(2):
            first_d[k].wait()
            m = mine[k]

            def add(r):
                d2_send[k, r, :] = d_keep[k, 1 - m, r, :] + d1_got[k, 1 - m, r, :]
                d_keep[k, m, r, :] += d1_got[k, m, r, :]

            by_rows(d_keep.shape[2], 32, add)
            second_d[k].start()

    @pl.when(step == last)
    def _():
        for k in range(2):
            first_u[k].wait()
            m = mine[k]

            def add(r):
                for j in range(u_keep.shape[1]):
                    us_buf[k, j, r, :] = u_keep[k, j, stay[k](1 - m), r, :] + u1_got[k, 1 - m, j, r, :]
                    uk_buf[k, j, r, :] = u_keep[k, j, stay[k](m), r, :] + u1_got[k, m, j, r, :]

            by_rows(u_keep.shape[3], 16, add)
        for v in stores:
            v.start()

    attn_head(t, qkv_ref, dol_ref, dor_ref, cos_ref, sin_ref, dqkv_ref, ctx_ref, dk_ref, dv_ref, bq, hd)

    @pl.when(step == last)
    def _():
        for v in stores:
            v.wait()
        w = d_keep.shape[3]
        for k in range(2):
            second_d[k].wait()
            m = mine[k]

            def add(r):
                gd_ref[r, k * w:(k + 1) * w] = d_keep[k, m, r, :] + d2_got[k, r, :]

            by_rows(d_keep.shape[2], 32, add)


def attn_head(t, qkv_ref, dol_ref, dor_ref, cos_ref, sin_ref, dqkv_ref, ctx_ref, dk_ref, dv_ref, bq, hd):
    seq = qkv_ref.shape[1]
    half = hd // 2
    part = dol_ref.shape[1]
    cos, sin = cos_ref[...], sin_ref[...]

    def in_order(own, peer):
        return jnp.concatenate([jnp.where(t == 0, own, peer), jnp.where(t == 0, peer, own)], axis=1)

    def place(lo, n):
        slot = t if lo < part else 1 - t
        return pl.ds(pl.multiple_of(slot * part + lo % part, 128), n)

    def rope(v):
        lo, hi = v[:half].astype(F32), v[half:].astype(F32)
        return jnp.concatenate([lo * cos - hi * sin, hi * cos + lo * sin], axis=0).astype(BF)

    def rope_back(d, c, s):
        lo, hi = d[:half].astype(BF).astype(F32), d[half:].astype(BF).astype(F32)
        return jnp.concatenate([lo * c + hi * s, hi * c - lo * s], axis=0).astype(BF)

    scale = hd ** -0.5
    qkv = in_order(qkv_ref[:, :part], qkv_ref[:, part:])
    q_t = rope(qkv[0:hd])
    k_t = rope(qkv[hd:2 * hd])
    v_t = qkv[2 * hd:3 * hd]
    q_t = (q_t.astype(F32) * scale).astype(BF)
    do_t = in_order(dol_ref[...], dor_ref[...])
    q_n, do_n, k_n, v_n = q_t.T, do_t.T, k_t.T, v_t.T
    tri = lax.broadcasted_iota(jnp.int32, (bq, bq), 0) <= lax.broadcasted_iota(jnp.int32, (bq, bq), 1)
    for i in range(seq // bq):
        lo, nk = i * bq, (i + 1) * bq
        blocks = [slice(j * bq, (j + 1) * bq) for j in range(i + 1)]
        q_b, do_b = q_t[:, lo:nk], do_t[:, lo:nk]
        ss = [dot(k_n[b], q_b, 1, 0) for b in blocks]
        ss[i] = jnp.where(tri, ss[i], -1e30)
        m = functools.reduce(jnp.maximum, [jnp.max(s, axis=0, keepdims=True) for s in ss])
        es = [jnp.exp(s - m) for s in ss]
        r = 1.0 / sum(jnp.sum(e, axis=0, keepdims=True) for e in es)
        ps = [e * r for e in es]
        pbs = [p.astype(BF) for p in ps]
        dps = [dot(v_n[b], do_b, 1, 0).astype(BF) for b in blocks]
        delta = sum(jnp.sum(p * d.astype(F32), axis=0, keepdims=True) for p, d in zip(ps, dps))
        dss = [(p * (d.astype(F32) - delta)).astype(BF) for p, d in zip(ps, dps)]
        ctx_ref[:, place(lo, bq)] = sum(dot(v_t[:, b], p, 1, 0) for b, p in zip(blocks, pbs)).astype(BF)
        dq = sum(dot(k_t[:, b], d, 1, 0) for b, d in zip(blocks, dss)) * scale
        dqkv_ref[0:hd, place(lo, bq)] = rope_back(dq, cos[:, lo:nk], sin[:, lo:nk])
        for j, b in enumerate(blocks):
            dv_new = dot(pbs[j], do_n[lo:nk], 1, 0)
            dk_new = dot(dss[j], q_n[lo:nk], 1, 0)
            if j < i:
                dv_ref[b, :] += dv_new
                dk_ref[b, :] += dk_new
            else:
                dv_ref[b, :] = dv_new
                dk_ref[b, :] = dk_new
    dk = rope_back(dk_ref[...].T, cos, sin)
    dv = dv_ref[...].T.astype(BF)
    for lo in (0, part):
        dqkv_ref[hd:2 * hd, place(lo, part)] = dk[:, lo:lo + part]
        dqkv_ref[2 * hd:3 * hd, place(lo, part)] = dv[:, lo:lo + part]


def attention(qkv_t, dol, dor, cos_t, sin_t, down, up, hd, bq=256):
    rows, seq = qkv_t.shape
    heads = rows // (3 * hd)
    part = dol.shape[1]
    const = pl.BlockSpec((hd // 2, seq), lambda g: (0, 0))
    row = lambda r, w: pl.BlockSpec((r, w), lambda g: (g, 0))
    hbm = pl.BlockSpec(memory_space=pl.ANY)
    dsh, ush = down[0].shape, up[0].shape
    dred, ured = dsh[2:], (ush[0],) + ush[2:]
    gd_shape = (dred[0], 2 * dred[1])
    whole = lambda *shape: pl.BlockSpec(shape, lambda g: (0,) * len(shape))
    f = lambda *shape: pltpu.VMEM(shape, F32)
    sds = jax.ShapeDtypeStruct
    return pl.pallas_call(
        functools.partial(attn_kernel, bq=bq, hd=hd),
        grid=(heads,),
        in_specs=[row(3 * hd, seq), row(hd, part), row(hd, part), const, const] + [hbm] * 6,
        out_specs=[row(3 * hd, seq), row(hd, seq), whole(*gd_shape), hbm, hbm],
        out_shape=[sds((rows, seq), BF), sds((heads * hd, seq), BF), sds(gd_shape, F32), sds((2,) + ured, F32), sds((2,) + ured, F32)],
        scratch_shapes=[
            f(seq, hd), f(seq, hd), f(*dsh), f(2, *ush), f(2, *ush),
            f(*dsh), f(2, 2, *ured), f(2, 2, *ured), f(2, *dred), f(2, *dred), f(2, *ured), f(2, *ured),
            pltpu.SemaphoreType.DMA((4,)), pltpu.SemaphoreType.DMA((2,)), pltpu.SemaphoreType.DMA((10,)), pltpu.SemaphoreType.DMA((10,)),
        ],
        compiler_params=pltpu.CompilerParams(vmem_limit_bytes=VMEM_LIMIT, collective_id=1, has_side_effects=True),
        cost_estimate=cost(heads * 6e9, heads << 20, seq * seq * heads // 2),
        name="attn",
    )(qkv_t, dol, dor, cos_t, sin_t, *down, *up)


def gelu_pair(h_ref, dy_ref, wu, wd, rows):
    u = dot(h_ref[rows, :], wu, 1, 0).astype(BF).astype(F32)
    dg = dot(dy_ref[rows, :], wd, 1, 1).astype(BF).astype(F32)
    cdf = 0.5 + 0.5 * lax.erf(u * SQRT_HALF)
    pdf = jnp.exp(-0.5 * u * u) * INV_SQRT_2PI
    return (u * cdf).astype(BF), (dg * (cdf + u * pdf)).astype(BF)


def mlp_own_kernel(h_ref, dy_ref, wu_ref, wd_ref, at_ref, du_ref, dh_ref, acc_ref, *, tc):
    step = pl.program_id(0)
    wu, wd = wu_ref[...], wd_ref[...]
    for k in range(h_ref.shape[0] // tc):
        rows = pl.ds(k * tc, tc)
        a, du = gelu_pair(h_ref, dy_ref, wu, wd, rows)
        at_ref[:, rows] = a.T
        du_ref[0, rows, :] = du
        add = dot(du, wu, 1, 1)

        @pl.when(step == 0)
        def _():
            acc_ref[rows, :] = add

        @pl.when(step > 0)
        def _():
            acc_ref[rows, :] += add

    @pl.when(step == pl.num_programs(0) - 1)
    def _():
        dh_ref[...] = acc_ref[...].astype(BF)


def mlp_own(h, dy, w_up, w_down, n=4, tc=256):
    seq, d = h.shape
    ff = w_up.shape[1]
    fb = ff // n
    full = pl.BlockSpec((seq, d), lambda i: (0, 0))
    return pl.pallas_call(
        functools.partial(mlp_own_kernel, tc=tc),
        grid=(n,),
        in_specs=[full, full, pl.BlockSpec((d, fb), lambda i: (0, i)), pl.BlockSpec((fb, d), lambda i: (i, 0))],
        out_specs=[pl.BlockSpec((fb, seq), lambda i: (i, 0)), pl.BlockSpec((1, seq, fb), lambda i: (i, 0, 0)), full],
        out_shape=[jax.ShapeDtypeStruct((ff, seq), BF), jax.ShapeDtypeStruct((n, seq, fb), BF), jax.ShapeDtypeStruct((seq, d), BF)],
        scratch_shapes=[pltpu.VMEM((seq, d), F32)],
        compiler_params=params(),
        cost_estimate=cost(6 * seq * d * ff, 20 << 20, 2 * seq * ff),
        name="mlp_own",
    )(h, dy, w_up, w_down)


def mlp_pre_kernel(h_ref, wu_ref, at_ref, gp_ref, *, tc):
    wu = wu_ref[...]
    for k in range(h_ref.shape[0] // tc):
        rows = pl.ds(k * tc, tc)
        u = dot(h_ref[rows, :], wu, 1, 0).astype(BF).astype(F32)
        cdf = 0.5 + 0.5 * lax.erf(u * SQRT_HALF)
        pdf = jnp.exp(-0.5 * u * u) * INV_SQRT_2PI
        at_ref[:, rows] = (u * cdf).astype(BF).T
        gp_ref[0, rows, :] = cdf + u * pdf


def mlp_pre(h, w_up, n=4, tc=256):
    seq, d = h.shape
    ff = w_up.shape[1]
    fb = ff // n
    return pl.pallas_call(
        functools.partial(mlp_pre_kernel, tc=tc),
        grid=(n,),
        in_specs=[pl.BlockSpec((seq, d), lambda i: (0, 0)), pl.BlockSpec((d, fb), lambda i: (0, i))],
        out_specs=[pl.BlockSpec((fb, seq), lambda i: (i, 0)), pl.BlockSpec((1, seq, fb), lambda i: (i, 0, 0))],
        out_shape=[jax.ShapeDtypeStruct((ff, seq), BF), jax.ShapeDtypeStruct((n, seq, fb), F32)],
        compiler_params=params(),
        cost_estimate=cost(2 * seq * d * ff, 16 << 20, 2 * seq * ff),
        name="mlp_pre",
    )(h, w_up)


def mlp_peer_kernel(dyr_ref, dyl_hbm, hkl_hbm, hsl_hbm, hkr_hbm, hsr_hbm, wu_ref, wd_ref, wo_ref, at_ref, atr_ref, dul_ref, gp_ref,
                    d_out, d_stay, uka_ref, ukb_ref, usa_ref, usb_ref, dh_ref, dctx_ref,
                    acc_ref, du_ref, d_keep, d_send, d_got, dyl_ref, hkl_ref, hsl_ref, hkr_ref, hsr_ref,
                    send_sem, recv_sem, load_sem, store_sem, *, tc):
    way, _, c, xx, yy = partners()
    step = pl.program_id(0)
    last = pl.num_programs(0) - 1
    wu, wd = wu_ref[...], wd_ref[...]
    fb = wu.shape[1]
    m = fb // 2

    def remote(i):
        return pltpu.make_async_remote_copy(
            src_ref=d_send.at[i], dst_ref=d_got.at[i], send_sem=send_sem.at[i], recv_sem=recv_sem.at[i],
            device_id=way["c"], device_id_type=MESH)

    def combine(i):
        remote(i).wait()
        for k in range(2):
            def add(r):
                d_keep[i, k, r, :] += d_got[i, k, r, :]

            by_rows(m, 32, add)
        store(i, lambda v: v.start())

    def store(i, f):
        y, x = i // 2, i % 2
        for k, at, go in ((0, y, x != xx), (1, x, y != yy)):
            for ref, cond in ((d_out, go), (d_stay, jnp.logical_not(go))):
                @pl.when(cond)
                def _():
                    f(pltpu.make_async_copy(d_keep.at[i, k], ref.at[k, at], store_sem.at[i, k]))

    late = [pltpu.make_async_copy(src, dst, load_sem.at[k]) for k, (src, dst) in enumerate((
        (dyl_hbm, dyl_ref), (hkl_hbm, hkl_ref), (hsl_hbm, hsl_ref), (hkr_hbm, hkr_ref), (hsr_hbm, hsr_ref)))]

    @pl.when(step == 0)
    def _():
        for v in late:
            v.start()

    pl.when(step == 0)(lambda: meet(way, "c"))
    dctx_ref[...] = dot(wo_ref[...], dyr_ref[...], 1, 1).astype(BF)

    @pl.when(step == 0)
    def _():
        acc_ref[...] = jnp.zeros_like(acc_ref)

    for k in range(dyr_ref.shape[0] // tc):
        rows = pl.ds(k * tc, tc)
        dg = dot(dyr_ref[rows, :], wd, 1, 1).astype(BF).astype(F32)
        du = (dg * gp_ref[0, rows, :]).astype(BF)
        du_ref[rows, :] = du
        acc_ref[rows, :] += dot(du, wu, 1, 1)

    @pl.when(step == 0)
    def _():
        for v in late:
            v.wait()

    for side, ref in ((1 - c, d_send), (c, d_keep)):
        block = pl.ds(pl.multiple_of(side * m, 128), m)
        g = dot(at_ref[block, :], dyl_ref[...], 1, 0) + dot(atr_ref[block, :], dyr_ref[...], 1, 0)
        w = g.shape[1] // 2
        ref[step, 0] = g[:, :w]
        ref[step, 1] = g[:, w:]
        if ref is d_send:
            remote(step).start()
    for hl, hr, ra, rb in ((hkl_ref, hkr_ref, uka_ref, ukb_ref), (hsl_ref, hsr_ref, usa_ref, usb_ref)):
        g = dot(hl[...], dul_ref[0], 1, 0) + dot(hr[...], du_ref[...], 1, 0)
        n = g.shape[0] // 4
        for j in range(4):
            ra[0, j] = g[j * n:(j + 1) * n, :m]
            rb[0, j] = g[j * n:(j + 1) * n, m:]

    pl.when(step > 0)(lambda: combine(step - 1))

    @pl.when(step == last)
    def _():
        combine(step)
        dh_ref[...] = acc_ref[...].astype(BF)
        for i in range(4):
            store(i, lambda v: v.wait())


def mlp_peer(dy_rem, dy_loc, hts, w_up, w_down, w_out, at, at_rem, du, slope, n=4, tc=256):
    seq, d = dy_rem.shape
    ff = w_up.shape[1]
    fb = ff // n
    ctx = w_out.shape[0]
    full = lambda r, w: pl.BlockSpec((r, w), lambda i: (0, 0))
    rows = lambda r, w: pl.BlockSpec((r, w), lambda i: (i, 0))
    dshape = (2, 2, fb // 2, d // 2)
    hbm = pl.BlockSpec(memory_space=pl.ANY)
    uspec = pl.BlockSpec((1, 4, d // 8, fb // 2), lambda i: (i, 0, 0, 0))
    act = pl.BlockSpec((1, seq, fb), lambda i: (i, 0, 0))
    sds = jax.ShapeDtypeStruct
    slots = pltpu.VMEM((n, 2, fb // 2, d // 2), F32)
    return pl.pallas_call(
        functools.partial(mlp_peer_kernel, tc=tc),
        grid=(n,),
        in_specs=[full(seq, d)] + [hbm] * 5 + [
            pl.BlockSpec((d, fb), lambda i: (0, i)), rows(fb, d), rows(ctx // n, d), rows(fb, seq), rows(fb, seq), act, act],
        out_specs=[hbm] * 2 + [uspec] * 4 + [full(seq, d), rows(ctx // n, seq)],
        out_shape=[sds(dshape, F32)] * 2 + [sds((n, 4, d // 8, fb // 2), F32)] * 4 + [sds((seq, d), BF), sds((ctx, seq), BF)],
        scratch_shapes=[pltpu.VMEM((seq, d), F32), pltpu.VMEM((seq, fb), BF), slots, slots, slots,
                        pltpu.VMEM((seq, d), BF)] + [pltpu.VMEM((d // 2, seq), BF)] * 4 + [
                        pltpu.SemaphoreType.DMA((n,)), pltpu.SemaphoreType.DMA((n,)),
                        pltpu.SemaphoreType.DMA((5,)), pltpu.SemaphoreType.DMA((n, 2))],
        compiler_params=pltpu.CompilerParams(vmem_limit_bytes=63 * 1024 * 1024, collective_id=2, has_side_effects=True),
        cost_estimate=cost(14 * seq * d * ff, 40 << 20),
        name="mlp_peer",
    )(dy_rem, dy_loc, *hts, w_up, w_down, w_out, at, at_rem, du, slope)


def tail_kernel(*refs, bt, hd):
    n_in = 13
    hbm, us_ref, refs = refs[:n_in], refs[n_in], refs[n_in + 1:]
    (gx_ref, sums_ref, gq_ref, gw_ref, gu_ref), refs = refs[:5], refs[5:]
    vm, refs = refs[:n_in], refs[n_in:]
    (z_send, z_recv, sum_src, sum_got, q_keep, q_send, q_recv, w_keep, w_send, w_recv,
     q1_send, q1_recv, w1_send, w1_recv, q2_send, q2_recv, w2_send, w2_recv, u2_recv,
     in_sem, send_sem, recv_sem) = refs
    dq, ctx, hk, hs, wt, xl, xr, dhl, dhr, dyl, dyr, ln, uk = vm
    way_to, t, c, xx, yy = partners()
    part = xl.shape[0]
    gr = dq.shape[0] // 4

    loads = [pltpu.make_async_copy(src, dst, in_sem.at[i]) for i, (src, dst) in enumerate(zip(hbm, vm))]
    for i in (0, 4, 6, 8, 11, 3, 2, 1, 9, 10, 5, 7, 12):
        loads[i].start()
    meet(way_to, "cxyz")

    count = [0]

    def send(src, dst, way):
        i = count[0]
        count[0] += 1
        copy = pltpu.make_async_remote_copy(
            src_ref=src, dst_ref=dst, send_sem=send_sem.at[i], recv_sem=recv_sem.at[i],
            device_id=way_to[way], device_id_type=MESH)
        copy.start()
        return copy

    def need(*idx):
        for i in idx:
            loads[i].wait()

    def block(x_ref, dh_ref, b, peer):
        rows = pl.ds(b * bt, bt)
        cols = pl.ds((part if peer else 0) + b * bt, bt)
        dha = dot(dq[:, cols], wt[...], 0, 0).astype(BF).astype(F32)
        dhm = dh_ref[rows, :].astype(F32)
        xh, rstd = normalized(x_ref[rows, :].astype(F32))
        dxh = (dha * ln[0:1, :] + dhm * ln[2:3, :]).astype(BF)
        parts = [dha * xh, dha, dhm * xh, dhm]
        return dxh, jnp.concatenate([jnp.sum(p, axis=0, keepdims=True) for p in parts], axis=0)

    def peer_block(b):
        dxh, s = block(xr, dhr, b, True)
        z_send[b] = dxh
        if b == 0:
            sum_src[0] = s
        else:
            sum_src[0] += s
        return send(z_send.at[b], z_recv.at[b], "z")

    def looped(start, n, f):
        def body(i, _):
            f(i)
            return _

        lax.fori_loop(start, start + n, body, 0)

    def qkv_grad(h_ref, out_ref, g):
        r = dot(dq[pl.ds(pl.multiple_of(g * gr, 128), gr), :], h_ref[...], 1, 0)
        n = r.shape[1] // 4
        for j in range(4):
            out_ref[g, j] = r[:, j * n:(j + 1) * n]

    def out_grad(want, out_ref):
        cx = jnp.concatenate([jnp.where(want == 0, ctx[2 * j * hd:(2 * j + 1) * hd, :], ctx[(2 * j + 1) * hd:(2 * j + 2) * hd, :])
                              for j in range(4)], axis=0)
        r = dot(cx[:, :part], dyl[...], 1, 0) + dot(cx[:, part:], dyr[...], 1, 0)
        m = r.shape[1] // 2
        for j in range(4):
            for k in range(2):
                out_ref[k, j] = r[j * hd:(j + 1) * hd, k * m:(k + 1) * m]

    def first(keep, got, out, k):
        for i in range(2):
            s_idx = 2 * i + 1 - xx if k == 0 else 2 * (1 - yy) + i
            k_idx = 2 * i + xx if k == 0 else 2 * yy + i
            out[i] = keep[s_idx] + got[s_idx]
            got[k_idx] = keep[k_idx] + got[k_idx]

    def second(got, got1, out, k):
        mine, other = (yy, 1 - yy) if k == 0 else (xx, 1 - xx)
        at = (lambda i: 2 * i + xx) if k == 0 else (lambda i: 2 * yy + i)
        out[...] = got[at(other)] + got1[other]
        return got[at(mine)] + got1[mine]

    ways = ("x", "y"), ("y", "x")

    us = [send(us_ref.at[k], u2_recv.at[k], ways[k][1]) for k in range(2)]
    need(0, 4, 6, 8, 11)
    zs = [peer_block(0)]
    q1, q2 = [None] * 4, [None] * 4
    n = gq_ref.shape[0] // 4

    def q_first(g):
        first(q_keep.at[g], q_recv.at[g], q1_send.at[g], g % 2)
        q1[g] = send(q1_send.at[g], q1_recv.at[g], ways[g % 2][0])

    def q_second(g):
        q1[g].wait()
        gq_ref[g * n:(g + 1) * n, :] = second(q_recv.at[g], q1_recv.at[g], q2_send.at[g], g % 2)
        q2[g] = send(q2_send.at[g], q2_recv.at[g], ways[g % 2][1])

    need(3)
    for g in (0, 2):
        looped(g, 2, lambda i: qkv_grad(hs, q_send, i))
        qc = send(q_send.at[pl.ds(g, 2)], q_recv.at[pl.ds(g, 2)], "c")
        if g == 0:
            need(2)
        else:
            zs.append(peer_block(1))
        looped(g, 2, lambda i: qkv_grad(hk, q_keep, i))
        qc.wait()
        q_first(g)
        q_first(g + 1)
    zs.append(peer_block(2))
    q_second(0)
    q_second(1)
    need(1, 9, 10)
    out_grad(1 - c, w_send)
    wc = send(w_send, w_recv, "c")
    out_grad(c, w_keep)
    wc.wait()
    w1 = []
    for k in range(2):
        first(w_keep.at[k], w_recv.at[k], w1_send.at[k], k)
        w1.append(send(w1_send.at[k], w1_recv.at[k], ways[k][0]))

    need(5, 7)

    def own_block(b):
        dxh, s = block(xl, dhl, b, False)
        gx_ref[pl.ds(b * bt, bt), :] = dxh
        sum_src[0] += s

    def grad_x(b):
        zs[b].wait()
        rows = pl.ds(b * bt, bt)
        dxh = gx_ref[rows, :].astype(F32) + z_recv[b].astype(F32)
        xh, rstd = normalized(xl[rows, :].astype(F32))
        dx = rstd * (dxh - jnp.mean(dxh, -1, keepdims=True) - xh * jnp.mean(dxh * xh, -1, keepdims=True))
        gx_ref[rows, :] = (dyl[rows, :].astype(F32) + dx).astype(BF)

    own_block(0)
    q_second(2)
    q_second(3)
    own_block(1)
    grad_x(0)
    own_block(2)
    sums = [send(sum_src.at[0], sum_got.at[0], "z")]
    grad_x(1)

    def sum_next(i, way):
        sums[-1].wait()
        sum_src[i] = sum_src[i - 1] + sum_got[i - 1]
        sums.append(send(sum_src.at[i], sum_got.at[i], way))

    sum_next(1, "c")
    need(12)
    blocks, m = uk.shape[1], uk.shape[3]
    for k in range(2):
        us[k].wait()
        for j in range(blocks):
            gu_ref[:, (2 * j + k) * m:(2 * j + k + 1) * m] = uk[k, j] + u2_recv[k, j]
    m = gw_ref.shape[1] // 2
    w2 = []
    for k in range(2):
        w1[k].wait()
        gw_ref[:, k * m:(k + 1) * m] = second(w_recv.at[k], w1_recv.at[k], w2_send.at[k], k)
        w2.append(send(w2_send.at[k], w2_recv.at[k], ways[k][1]))
    sum_next(2, "x")
    for g in (0, 1):
        q2[g].wait()
        gq_ref[g * n:(g + 1) * n, :] += q2_recv[g]
    sum_next(3, "y")
    for g in (2, 3):
        q2[g].wait()
        gq_ref[g * n:(g + 1) * n, :] += q2_recv[g]
    for k in range(2):
        w2[k].wait()
        gw_ref[:, k * m:(k + 1) * m] += w2_recv[k]
    sums[-1].wait()
    sums_ref[...] = sum_src[3] + sum_got[3]
    grad_x(2)


def tail(dq, ctx, h_keep, h_send, w_t, x_loc, x_rem, dhm_loc, dhm_rem, dy_loc, dy_rem, ln, u_keep, u_send, hd, bt=256):
    ins = [dq, ctx, h_keep, h_send, w_t, x_loc, x_rem, dhm_loc, dhm_rem, dy_loc, dy_rem, ln, u_keep]
    part, d = x_loc.shape
    rows = dq.shape[0] // 4
    nb = part // bt
    cols = d // 8
    f = lambda *shape: pltpu.VMEM(shape, F32)
    sds = jax.ShapeDtypeStruct
    scratch = [pltpu.VMEM(v.shape, v.dtype) for v in ins] + [
        pltpu.VMEM((nb, bt, d), BF), pltpu.VMEM((nb, bt, d), BF), f(4, 4, d), f(4, 4, d),
        f(4, 4, rows, cols), f(4, 4, rows, cols), f(4, 4, rows, cols),
        f(2, 4, hd, d // 2), f(2, 4, hd, d // 2), f(2, 4, hd, d // 2),
        f(4, 2, rows, cols), f(4, 2, rows, cols), f(2, 2, hd, d // 2), f(2, 2, hd, d // 2),
        f(4, rows, cols), f(4, rows, cols), f(2, hd, d // 2), f(2, hd, d // 2), f(*u_send.shape),
        pltpu.SemaphoreType.DMA((len(ins),)), pltpu.SemaphoreType.DMA((32,)), pltpu.SemaphoreType.DMA((32,)),
    ]
    vm = pl.BlockSpec(memory_space=pltpu.VMEM)
    u_cols = u_keep.shape[0] * u_keep.shape[1] * u_keep.shape[3]
    return pl.pallas_call(
        functools.partial(tail_kernel, bt=bt, hd=hd),
        in_specs=[pl.BlockSpec(memory_space=pl.ANY)] * (len(ins) + 1),
        out_specs=[vm] * 5,
        out_shape=[sds((part, d), BF), sds((4, d), F32), sds((4 * rows, cols), F32), sds((hd, d), F32), sds((u_keep.shape[2], u_cols), F32)],
        scratch_shapes=scratch,
        compiler_params=pltpu.CompilerParams(vmem_limit_bytes=VMEM_LIMIT, collective_id=0, has_side_effects=True),
        cost_estimate=cost(4e10, 40 << 20),
        name="tail",
    )(*ins, u_send)


def emit_kernel(*refs, n):
    ins, outs, bufs, (sem_in, sem_out) = refs[:n], refs[n:2 * n], refs[2 * n:3 * n], refs[3 * n:]
    get = [pltpu.make_async_copy(ins[i], bufs[i], sem_in.at[i]) for i in range(n)]
    put = [pltpu.make_async_copy(bufs[i], outs[i], sem_out.at[i]) for i in range(n)]
    for v in get:
        v.start()
    for i in range(n):
        get[i].wait()
        put[i].start()
    for v in put:
        v.wait()


def emit(*arrays):
    n = len(arrays)
    hbm = pl.BlockSpec(memory_space=pl.ANY)
    return pl.pallas_call(
        functools.partial(emit_kernel, n=n),
        in_specs=[hbm] * n,
        out_specs=[hbm] * n,
        out_shape=[jax.ShapeDtypeStruct(v.shape, v.dtype) for v in arrays],
        scratch_shapes=[pltpu.VMEM(v.shape, v.dtype) for v in arrays]
        + [pltpu.SemaphoreType.DMA((n,)), pltpu.SemaphoreType.DMA((n,))],
        compiler_params=params(),
        cost_estimate=cost(1e6, 10 << 20),
        name="emit",
    )(*arrays)


def solution(mesh):
    dp = mesh.shape["dp"]
    tp = mesh.shape["tp"]

    def swap_tp(v):
        return lax.ppermute(v, "tp", [(i, i ^ 1) for i in range(tp)])

    def after(v, *deps):
        return lax.optimization_barrier((v,) + deps)[0]

    def local_step(x_loc, dy_loc, ln_params, w_qkv, w_out, w_up, w_down):
        x_loc, dy_loc = x_loc[0], dy_loc[0]
        half, d = x_loc.shape
        seq = half * tp
        heads, hd = w_qkv.shape[1], w_qkv.shape[3]
        me = lax.axis_index("dp")
        c1 = (me % 2).astype(jnp.int32)[None]

        x_rem = swap_tp(x_loc)
        dy_rem = swap_tp(dy_loc)

        w_t = w_qkv.transpose(1, 2, 3, 0).reshape(heads * 3 * hd, d)
        inv_freq = ROPE_BASE ** (-2.0 * jnp.arange(hd // 2, dtype=F32) / hd)
        ang = inv_freq[:, None] * jnp.arange(seq).astype(F32)[None, :]
        cos_t, sin_t = jnp.cos(ang), jnp.sin(ang)

        hm_loc, hk_loc, hs_loc = norm_m(c1, x_loc, ln_params)
        at_loc, du_loc, dhm_loc = mlp_own(hm_loc, dy_loc, w_up, w_down)
        dctx_loc = dot(w_out, dy_loc, 1, 1).astype(BF)

        x_rem = after(x_rem, dhm_loc, dctx_loc, cos_t, sin_t, w_t)
        hm_rem, hk_rem, hs_rem = norm_m(c1, x_rem, ln_params)
        h_a, h_keep, h_send = norm_a(c1, x_loc, x_rem, ln_params)
        qkv_t = dot(w_t, h_a, 1, 1).astype(BF)

        at_rem, slope = mlp_pre(after(hm_rem, qkv_t), w_up)

        dy_rem = after(dy_rem, qkv_t, h_keep, slope)
        d_out, d_stay, uka, ukb, usa, usb, dhm_rem, dctx_rem = mlp_peer(
            dy_rem, dy_loc, (hk_loc, hs_loc, hk_rem, hs_rem), w_up, w_down, w_out, at_loc, at_rem, du_loc, slope)
        dq, ctx, g_wdown, u_send, u_keep = attention(
            qkv_t, dctx_loc, dctx_rem, cos_t, sin_t, (d_out, d_stay), (uka, ukb, usa, usb), hd)
        grad_x, sums, g_wqkv, g_wout, g_wup, g_wdown = emit(*tail(
            dq, ctx, h_keep, h_send, w_t, x_loc, x_rem, dhm_loc, dhm_rem, dy_loc, dy_rem, ln_params, u_keep, u_send, hd), g_wdown)
        grad_x = grad_x[None]
        g_wqkv = g_wqkv.reshape(heads, 3, hd, d // dp).transpose(3, 0, 1, 2)
        return grad_x, sums, g_wqkv, g_wout, g_wup, g_wdown

    return jax.shard_map(
        local_step,
        mesh=mesh,
        in_specs=(P("dp", "tp"), P("dp", "tp"), P(), P(None, "tp"), P("tp"), P(None, "tp"), P("tp")),
        out_specs=(P("dp", "tp"), P(), P("dp", "tp"), P(("tp", "dp")), P("dp", "tp"), P(("tp", "dp"))),
        check_vma=False,
    )
```

```python
import functools

import jax
import jax.numpy as jnp
from jax import lax
from jax.experimental import pallas as pl
from jax.experimental.pallas import tpu as pltpu
from jax.sharding import PartitionSpec as P

NORM_EPS = 1e-5
ROPE_BASE = 10000.0
BF = jnp.bfloat16
F32 = jnp.float32
SQRT_HALF = 0.7071067811865476
INV_SQRT_2PI = 0.3989422804014327
VMEM_LIMIT = 60 * 1024 * 1024


def dot(a, b, ca, cb):
    return lax.dot_general(a, b, (((ca,), (cb,)), ((), ())), preferred_element_type=F32)


def params():
    return pltpu.CompilerParams(vmem_limit_bytes=VMEM_LIMIT)


def cost(flops, nbytes, trans=0):
    return pl.CostEstimate(flops=int(flops), bytes_accessed=int(nbytes), transcendentals=int(trans))


def normalized(x):
    cen = x - jnp.mean(x, axis=-1, keepdims=True)
    rstd = lax.rsqrt(jnp.mean(cen * cen, axis=-1, keepdims=True) + NORM_EPS)
    return cen * rstd, rstd


def norm_m_kernel(c_ref, x_ref, ln_ref, hm_ref, hk_ref, hs_ref):
    hm = (normalized(x_ref[...].astype(F32))[0] * ln_ref[2:3, :] + ln_ref[3:4, :]).astype(BF)
    hm_ref[...] = hm
    n = hm.shape[1] // 8
    for j in range(4):
        even, odd = hm[:, 2 * j * n:(2 * j + 1) * n].T, hm[:, (2 * j + 1) * n:(2 * j + 2) * n].T
        hk_ref[j * n:(j + 1) * n, :] = jnp.where(c_ref[0] == 0, even, odd)
        hs_ref[j * n:(j + 1) * n, :] = jnp.where(c_ref[0] == 0, odd, even)


def norm_m(core, x, ln, bt=256):
    rows, d = x.shape
    tok = pl.BlockSpec((bt, d), lambda i, c: (i, 0))
    return pl.pallas_call(
        norm_m_kernel,
        grid_spec=pltpu.PrefetchScalarGridSpec(
            num_scalar_prefetch=1,
            grid=(rows // bt,),
            in_specs=[tok, pl.BlockSpec((4, d), lambda i, c: (0, 0))],
            out_specs=[tok] + [pl.BlockSpec((d // 2, bt), lambda i, c: (0, i))] * 2,
        ),
        out_shape=[jax.ShapeDtypeStruct((rows, d), BF)] + [jax.ShapeDtypeStruct((d // 2, rows), BF)] * 2,
        compiler_params=params(),
        cost_estimate=cost(3e9, rows * d * 6),
        name="norm_m",
    )(core, x, ln)


def norm_a_kernel(c_ref, xl_ref, xr_ref, ln_ref, ha_ref, hk_ref, hs_ref, *, nb):
    def run(x_ref):
        ha = (normalized(x_ref[...].astype(F32))[0] * ln_ref[0:1, :] + ln_ref[1:2, :]).astype(BF)
        ha_ref[...] = ha
        n = ha.shape[1] // 8
        for j in range(4):
            even, odd = ha[:, 2 * j * n:(2 * j + 1) * n], ha[:, (2 * j + 1) * n:(2 * j + 2) * n]
            hk_ref[:, j * n:(j + 1) * n] = jnp.where(c_ref[0] == 0, even, odd)
            hs_ref[:, j * n:(j + 1) * n] = jnp.where(c_ref[0] == 0, odd, even)

    pl.when(pl.program_id(0) < nb)(lambda: run(xl_ref))
    pl.when(pl.program_id(0) >= nb)(lambda: run(xr_ref))


def norm_a(core, x_loc, x_rem, ln, bt=256):
    rows, d = x_loc.shape
    nb = rows // bt
    tok = lambda w: pl.BlockSpec((bt, w), lambda i, c: (i, 0))
    return pl.pallas_call(
        functools.partial(norm_a_kernel, nb=nb),
        grid_spec=pltpu.PrefetchScalarGridSpec(
            num_scalar_prefetch=1,
            grid=(2 * nb,),
            in_specs=[
                pl.BlockSpec((bt, d), lambda i, c: (jnp.minimum(i, nb - 1), 0)),
                pl.BlockSpec((bt, d), lambda i, c: (jnp.maximum(i - nb, 0), 0)),
                pl.BlockSpec((4, d), lambda i, c: (0, 0)),
            ],
            out_specs=[tok(d), tok(d // 2), tok(d // 2)],
        ),
        out_shape=[jax.ShapeDtypeStruct((2 * rows, w), BF) for w in (d, d // 2, d // 2)],
        compiler_params=params(),
        cost_estimate=cost(6e9, rows * d * 12),
        name="norm_a",
    )(core, x_loc, x_rem, ln)


MESH = pl.DeviceIdType.MESH


def partners():
    me, t = lax.axis_index("dp"), lax.axis_index("tp")
    c, xx, yy = me % 2, (me // 2) % 2, me // 4
    way = {"c": {"dp": me + 1 - 2 * c}, "x": {"dp": me + 2 - 4 * xx}, "y": {"dp": me + 4 - 8 * yy}, "z": {"tp": 1 - t}}
    return way, t, c, xx, yy


def meet(way, names):
    barrier = pltpu.get_barrier_semaphore()
    for p in names:
        pl.semaphore_signal(barrier, inc=1, device_id=way[p], device_id_type=MESH)
    pl.semaphore_wait(barrier, len(names))


def by_rows(n, chunk, f):
    def body(i, _):
        f(pl.ds(pl.multiple_of(i * chunk, 8), chunk))
        return _

    lax.fori_loop(0, n // chunk, body, 0)


WAYS = ("x", "y"), ("y", "x")


def attn_kernel(qkv_ref, dol_ref, dor_ref, cos_ref, sin_ref,
                d_out, d_stay, uka, ukb, usa, usb,
                dqkv_ref, ctx_ref, gd_ref, us_ref, uk_ref,
                dk_ref, dv_ref, d_keep, u_keep, u_got, d1_got, u1_send, u1_got, d2_send, d2_got, us_buf, uk_buf,
                load_sem, store_sem, send_sem, recv_sem, *, bq, hd):
    way, t, _, xx, yy = partners()
    step = pl.program_id(0)
    last = pl.num_programs(0) - 1

    def remote(i, src, dst, w):
        return pltpu.make_async_remote_copy(
            src_ref=src, dst_ref=dst, send_sem=send_sem.at[i], recv_sem=recv_sem.at[i], device_id=way[w], device_id_type=MESH)

    core_u = [remote(2 + k, src, u_got.at[k], "c") for k, src in enumerate((usa, usb))]
    first_d = [remote(k, d_out.at[k], d1_got.at[k], WAYS[k][0]) for k in range(2)]
    second_d = [remote(4 + k, d2_send.at[k], d2_got.at[k], WAYS[k][1]) for k in range(2)]
    first_u = [remote(6 + k, u1_send.at[k], u1_got.at[k], WAYS[k][0]) for k in range(2)]
    load_d = pltpu.make_async_copy(d_stay, d_keep, load_sem.at[0])
    stores = [pltpu.make_async_copy(v, o, store_sem.at[k]) for k, (v, o) in enumerate(((us_buf, us_ref), (uk_buf, uk_ref)))]
    load_u = [pltpu.make_async_copy(src, u_keep.at[k], load_sem.at[2 + k]) for k, src in enumerate((uka, ukb))]

    leave = [lambda i: 2 * i + 1 - xx, lambda i: 2 * (1 - yy) + i]
    stay = [lambda i: 2 * i + xx, lambda i: 2 * yy + i]
    mine = [yy, xx]

    @pl.when(step == 0)
    def _():
        meet(way, "cxy")
        for v in first_d + core_u + [load_d] + load_u:
            v.start()

    @pl.when(step == 3)
    def _():
        for k in range(2):
            load_u[k].wait()
            core_u[k].wait()
            for i in range(2):
                def add(r):
                    for j in range(u_keep.shape[1]):
                        u1_send[k, i, j, r, :] = u_keep[k, j, leave[k](i), r, :] + u_got[k, j, leave[k](i), r, :]
                        u_keep[k, j, stay[k](i), r, :] += u_got[k, j, stay[k](i), r, :]

                by_rows(u_keep.shape[3], 16, add)
            first_u[k].start()

    @pl.when(step == 4)
    def _():
        load_d.wait()
        for k in range(2):
            first_d[k].wait()
            m = mine[k]

            def add(r):
                d2_send[k, r, :] = d_keep[k, 1 - m, r, :] + d1_got[k, 1 - m, r, :]
                d_keep[k, m, r, :] += d1_got[k, m, r, :]

            by_rows(d_keep.shape[2], 32, add)
            second_d[k].start()

    @pl.when(step == last)
    def _():
        for k in range(2):
            first_u[k].wait()
            m = mine[k]

            def add(r):
                for j in range(u_keep.shape[1]):
                    us_buf[k, j, r, :] = u_keep[k, j, stay[k](1 - m), r, :] + u1_got[k, 1 - m, j, r, :]
                    uk_buf[k, j, r, :] = u_keep[k, j, stay[k](m), r, :] + u1_got[k, m, j, r, :]

            by_rows(u_keep.shape[3], 16, add)
        for v in stores:
            v.start()

    attn_head(t, qkv_ref, dol_ref, dor_ref, cos_ref, sin_ref, dqkv_ref, ctx_ref, dk_ref, dv_ref, bq, hd)

    @pl.when(step == last)
    def _():
        for v in stores:
            v.wait()
        w = d_keep.shape[3]
        for k in range(2):
            second_d[k].wait()
            m = mine[k]

            def add(r):
                gd_ref[r, k * w:(k + 1) * w] = d_keep[k, m, r, :] + d2_got[k, r, :]

            by_rows(d_keep.shape[2], 32, add)


def attn_head(t, qkv_ref, dol_ref, dor_ref, cos_ref, sin_ref, dqkv_ref, ctx_ref, dk_ref, dv_ref, bq, hd):
    seq = qkv_ref.shape[1]
    half = hd // 2
    part = dol_ref.shape[1]
    cos, sin = cos_ref[...], sin_ref[...]

    def in_order(own, peer):
        return jnp.concatenate([jnp.where(t == 0, own, peer), jnp.where(t == 0, peer, own)], axis=1)

    def place(lo, n):
        slot = t if lo < part else 1 - t
        return pl.ds(pl.multiple_of(slot * part + lo % part, 128), n)

    def rope(v):
        lo, hi = v[:half].astype(F32), v[half:].astype(F32)
        return jnp.concatenate([lo * cos - hi * sin, hi * cos + lo * sin], axis=0).astype(BF)

    def rope_back(d, c, s):
        lo, hi = d[:half].astype(BF).astype(F32), d[half:].astype(BF).astype(F32)
        return jnp.concatenate([lo * c + hi * s, hi * c - lo * s], axis=0).astype(BF)

    scale = hd ** -0.5
    qkv = in_order(qkv_ref[:, :part], qkv_ref[:, part:])
    q_t = rope(qkv[0:hd])
    k_t = rope(qkv[hd:2 * hd])
    v_t = qkv[2 * hd:3 * hd]
    q_t = (q_t.astype(F32) * scale).astype(BF)
    do_t = in_order(dol_ref[...], dor_ref[...])
    q_n, do_n, k_n, v_n = q_t.T, do_t.T, k_t.T, v_t.T
    tri = lax.broadcasted_iota(jnp.int32, (bq, bq), 0) <= lax.broadcasted_iota(jnp.int32, (bq, bq), 1)
    for i in range(seq // bq):
        lo, nk = i * bq, (i + 1) * bq
        blocks = [slice(j * bq, (j + 1) * bq) for j in range(i + 1)]
        q_b, do_b = q_t[:, lo:nk], do_t[:, lo:nk]
        ss = [dot(k_n[b], q_b, 1, 0) for b in blocks]
        ss[i] = jnp.where(tri, ss[i], -1e30)
        m = functools.reduce(jnp.maximum, [jnp.max(s, axis=0, keepdims=True) for s in ss])
        es = [jnp.exp(s - m) for s in ss]
        r = 1.0 / sum(jnp.sum(e, axis=0, keepdims=True) for e in es)
        ps = [e * r for e in es]
        pbs = [p.astype(BF) for p in ps]
        dps = [dot(v_n[b], do_b, 1, 0).astype(BF) for b in blocks]
        delta = sum(jnp.sum(p * d.astype(F32), axis=0, keepdims=True) for p, d in zip(ps, dps))
        dss = [(p * (d.astype(F32) - delta)).astype(BF) for p, d in zip(ps, dps)]
        ctx_ref[:, place(lo, bq)] = sum(dot(v_t[:, b], p, 1, 0) for b, p in zip(blocks, pbs)).astype(BF)
        dq = sum(dot(k_t[:, b], d, 1, 0) for b, d in zip(blocks, dss)) * scale
        dqkv_ref[0:hd, place(lo, bq)] = rope_back(dq, cos[:, lo:nk], sin[:, lo:nk])
        for j, b in enumerate(blocks):
            dv_new = dot(pbs[j], do_n[lo:nk], 1, 0)
            dk_new = dot(dss[j], q_n[lo:nk], 1, 0)
            if j < i:
                dv_ref[b, :] += dv_new
                dk_ref[b, :] += dk_new
            else:
                dv_ref[b, :] = dv_new
                dk_ref[b, :] = dk_new
    dk = rope_back(dk_ref[...].T, cos, sin)
    dv = dv_ref[...].T.astype(BF)
    for lo in (0, part):
        dqkv_ref[hd:2 * hd, place(lo, part)] = dk[:, lo:lo + part]
        dqkv_ref[2 * hd:3 * hd, place(lo, part)] = dv[:, lo:lo + part]


def attention(qkv_t, dol, dor, cos_t, sin_t, down, up, hd, bq=256):
    rows, seq = qkv_t.shape
    heads = rows // (3 * hd)
    part = dol.shape[1]
    const = pl.BlockSpec((hd // 2, seq), lambda g: (0, 0))
    row = lambda r, w: pl.BlockSpec((r, w), lambda g: (g, 0))
    hbm = pl.BlockSpec(memory_space=pl.ANY)
    dsh, ush = down[0].shape, up[0].shape
    dred, ured = dsh[2:], (ush[0],) + ush[2:]
    gd_shape = (dred[0], 2 * dred[1])
    whole = lambda *shape: pl.BlockSpec(shape, lambda g: (0,) * len(shape))
    f = lambda *shape: pltpu.VMEM(shape, F32)
    sds = jax.ShapeDtypeStruct
    return pl.pallas_call(
        functools.partial(attn_kernel, bq=bq, hd=hd),
        grid=(heads,),
        in_specs=[row(3 * hd, seq), row(hd, part), row(hd, part), const, const] + [hbm] * 6,
        out_specs=[row(3 * hd, seq), row(hd, seq), whole(*gd_shape), hbm, hbm],
        out_shape=[sds((rows, seq), BF), sds((heads * hd, seq), BF), sds(gd_shape, F32), sds((2,) + ured, F32), sds((2,) + ured, F32)],
        scratch_shapes=[
            f(seq, hd), f(seq, hd), f(*dsh), f(2, *ush), f(2, *ush),
            f(*dsh), f(2, 2, *ured), f(2, 2, *ured), f(2, *dred), f(2, *dred), f(2, *ured), f(2, *ured),
            pltpu.SemaphoreType.DMA((4,)), pltpu.SemaphoreType.DMA((2,)), pltpu.SemaphoreType.DMA((10,)), pltpu.SemaphoreType.DMA((10,)),
        ],
        compiler_params=pltpu.CompilerParams(vmem_limit_bytes=VMEM_LIMIT, collective_id=1, has_side_effects=True),
        cost_estimate=cost(heads * 6e9, heads << 20, seq * seq * heads // 2),
        name="attn",
    )(qkv_t, dol, dor, cos_t, sin_t, *down, *up)


def gelu_pair(h_ref, dy_ref, wu, wd, rows):
    u = dot(h_ref[rows, :], wu, 1, 0).astype(BF).astype(F32)
    dg = dot(dy_ref[rows, :], wd, 1, 1).astype(BF).astype(F32)
    cdf = 0.5 + 0.5 * lax.erf(u * SQRT_HALF)
    pdf = jnp.exp(-0.5 * u * u) * INV_SQRT_2PI
    return (u * cdf).astype(BF), (dg * (cdf + u * pdf)).astype(BF)


def mlp_own_kernel(h_ref, dy_ref, wu_ref, wd_ref, at_ref, du_ref, dh_ref, acc_ref, *, tc):
    step = pl.program_id(0)
    wu, wd = wu_ref[...], wd_ref[...]
    for k in range(h_ref.shape[0] // tc):
        rows = pl.ds(k * tc, tc)
        a, du = gelu_pair(h_ref, dy_ref, wu, wd, rows)
        at_ref[:, rows] = a.T
        du_ref[0, rows, :] = du
        add = dot(du, wu, 1, 1)

        @pl.when(step == 0)
        def _():
            acc_ref[rows, :] = add

        @pl.when(step > 0)
        def _():
            acc_ref[rows, :] += add

    @pl.when(step == pl.num_programs(0) - 1)
    def _():
        dh_ref[...] = acc_ref[...].astype(BF)


def mlp_own(h, dy, w_up, w_down, n=4, tc=256):
    seq, d = h.shape
    ff = w_up.shape[1]
    fb = ff // n
    full = pl.BlockSpec((seq, d), lambda i: (0, 0))
    return pl.pallas_call(
        functools.partial(mlp_own_kernel, tc=tc),
        grid=(n,),
        in_specs=[full, full, pl.BlockSpec((d, fb), lambda i: (0, i)), pl.BlockSpec((fb, d), lambda i: (i, 0))],
        out_specs=[pl.BlockSpec((fb, seq), lambda i: (i, 0)), pl.BlockSpec((1, seq, fb), lambda i: (i, 0, 0)), full],
        out_shape=[jax.ShapeDtypeStruct((ff, seq), BF), jax.ShapeDtypeStruct((n, seq, fb), BF), jax.ShapeDtypeStruct((seq, d), BF)],
        scratch_shapes=[pltpu.VMEM((seq, d), F32)],
        compiler_params=params(),
        cost_estimate=cost(6 * seq * d * ff, 20 << 20, 2 * seq * ff),
        name="mlp_own",
    )(h, dy, w_up, w_down)


def mlp_pre_kernel(h_ref, wu_ref, at_ref, gp_ref, *, tc):
    wu = wu_ref[...]
    for k in range(h_ref.shape[0] // tc):
        rows = pl.ds(k * tc, tc)
        u = dot(h_ref[rows, :], wu, 1, 0).astype(BF).astype(F32)
        cdf = 0.5 + 0.5 * lax.erf(u * SQRT_HALF)
        pdf = jnp.exp(-0.5 * u * u) * INV_SQRT_2PI
        at_ref[:, rows] = (u * cdf).astype(BF).T
        gp_ref[0, rows, :] = cdf + u * pdf


def mlp_pre(h, w_up, n=4, tc=256):
    seq, d = h.shape
    ff = w_up.shape[1]
    fb = ff // n
    return pl.pallas_call(
        functools.partial(mlp_pre_kernel, tc=tc),
        grid=(n,),
        in_specs=[pl.BlockSpec((seq, d), lambda i: (0, 0)), pl.BlockSpec((d, fb), lambda i: (0, i))],
        out_specs=[pl.BlockSpec((fb, seq), lambda i: (i, 0)), pl.BlockSpec((1, seq, fb), lambda i: (i, 0, 0))],
        out_shape=[jax.ShapeDtypeStruct((ff, seq), BF), jax.ShapeDtypeStruct((n, seq, fb), F32)],
        compiler_params=params(),
        cost_estimate=cost(2 * seq * d * ff, 16 << 20, 2 * seq * ff),
        name="mlp_pre",
    )(h, w_up)


def mlp_peer_kernel(dyr_ref, dyl_hbm, hkl_hbm, hsl_hbm, hkr_hbm, hsr_hbm, wu_ref, wd_ref, wo_ref, at_ref, atr_ref, dul_ref, gp_ref,
                    d_out, d_stay, uka_ref, ukb_ref, usa_ref, usb_ref, dh_ref, dctx_ref,
                    acc_ref, du_ref, d_keep, d_send, d_got, dyl_ref, hkl_ref, hsl_ref, hkr_ref, hsr_ref,
                    send_sem, recv_sem, load_sem, store_sem, *, tc):
    way, _, c, xx, yy = partners()
    step = pl.program_id(0)
    last = pl.num_programs(0) - 1
    wu, wd = wu_ref[...], wd_ref[...]
    fb = wu.shape[1]
    m = fb // 2

    def remote(i):
        return pltpu.make_async_remote_copy(
            src_ref=d_send.at[i], dst_ref=d_got.at[i], send_sem=send_sem.at[i], recv_sem=recv_sem.at[i],
            device_id=way["c"], device_id_type=MESH)

    def combine(i):
        remote(i).wait()
        for k in range(2):
            def add(r):
                d_keep[i, k, r, :] += d_got[i, k, r, :]

            by_rows(m, 32, add)
        store(i, lambda v: v.start())

    def store(i, f):
        y, x = i // 2, i % 2
        for k, at, go in ((0, y, x != xx), (1, x, y != yy)):
            for ref, cond in ((d_out, go), (d_stay, jnp.logical_not(go))):
                @pl.when(cond)
                def _():
                    f(pltpu.make_async_copy(d_keep.at[i, k], ref.at[k, at], store_sem.at[i, k]))

    late = [pltpu.make_async_copy(src, dst, load_sem.at[k]) for k, (src, dst) in enumerate((
        (dyl_hbm, dyl_ref), (hkl_hbm, hkl_ref), (hsl_hbm, hsl_ref), (hkr_hbm, hkr_ref), (hsr_hbm, hsr_ref)))]

    @pl.when(step == 0)
    def _():
        for v in late:
            v.start()

    pl.when(step == 0)(lambda: meet(way, "c"))
    dctx_ref[...] = dot(wo_ref[...], dyr_ref[...], 1, 1).astype(BF)

    @pl.when(step == 0)
    def _():
        acc_ref[...] = jnp.zeros_like(acc_ref)

    for k in range(dyr_ref.shape[0] // tc):
        rows = pl.ds(k * tc, tc)
        dg = dot(dyr_ref[rows, :], wd, 1, 1).astype(BF).astype(F32)
        du = (dg * gp_ref[0, rows, :]).astype(BF)
        du_ref[rows, :] = du
        acc_ref[rows, :] += dot(du, wu, 1, 1)

    @pl.when(step == 0)
    def _():
        for v in late:
            v.wait()

    for side, ref in ((1 - c, d_send), (c, d_keep)):
        block = pl.ds(pl.multiple_of(side * m, 128), m)
        g = dot(at_ref[block, :], dyl_ref[...], 1, 0) + dot(atr_ref[block, :], dyr_ref[...], 1, 0)
        w = g.shape[1] // 2
        ref[step, 0] = g[:, :w]
        ref[step, 1] = g[:, w:]
        if ref is d_send:
            remote(step).start()
    for hl, hr, ra, rb in ((hkl_ref, hkr_ref, uka_ref, ukb_ref), (hsl_ref, hsr_ref, usa_ref, usb_ref)):
        g = dot(hl[...], dul_ref[0], 1, 0) + dot(hr[...], du_ref[...], 1, 0)
        n = g.shape[0] // 4
        for j in range(4):
            ra[0, j] = g[j * n:(j + 1) * n, :m]
            rb[0, j] = g[j * n:(j + 1) * n, m:]

    pl.when(step > 0)(lambda: combine(step - 1))

    @pl.when(step == last)
    def _():
        combine(step)
        dh_ref[...] = acc_ref[...].astype(BF)
        for i in range(4):
            store(i, lambda v: v.wait())


def mlp_peer(dy_rem, dy_loc, hts, w_up, w_down, w_out, at, at_rem, du, slope, n=4, tc=256):
    seq, d = dy_rem.shape
    ff = w_up.shape[1]
    fb = ff // n
    ctx = w_out.shape[0]
    full = lambda r, w: pl.BlockSpec((r, w), lambda i: (0, 0))
    rows = lambda r, w: pl.BlockSpec((r, w), lambda i: (i, 0))
    dshape = (2, 2, fb // 2, d // 2)
    hbm = pl.BlockSpec(memory_space=pl.ANY)
    uspec = pl.BlockSpec((1, 4, d // 8, fb // 2), lambda i: (i, 0, 0, 0))
    act = pl.BlockSpec((1, seq, fb), lambda i: (i, 0, 0))
    sds = jax.ShapeDtypeStruct
    slots = pltpu.VMEM((n, 2, fb // 2, d // 2), F32)
    return pl.pallas_call(
        functools.partial(mlp_peer_kernel, tc=tc),
        grid=(n,),
        in_specs=[full(seq, d)] + [hbm] * 5 + [
            pl.BlockSpec((d, fb), lambda i: (0, i)), rows(fb, d), rows(ctx // n, d), rows(fb, seq), rows(fb, seq), act, act],
        out_specs=[hbm] * 2 + [uspec] * 4 + [full(seq, d), rows(ctx // n, seq)],
        out_shape=[sds(dshape, F32)] * 2 + [sds((n, 4, d // 8, fb // 2), F32)] * 4 + [sds((seq, d), BF), sds((ctx, seq), BF)],
        scratch_shapes=[pltpu.VMEM((seq, d), F32), pltpu.VMEM((seq, fb), BF), slots, slots, slots,
                        pltpu.VMEM((seq, d), BF)] + [pltpu.VMEM((d // 2, seq), BF)] * 4 + [
                        pltpu.SemaphoreType.DMA((n,)), pltpu.SemaphoreType.DMA((n,)),
                        pltpu.SemaphoreType.DMA((5,)), pltpu.SemaphoreType.DMA((n, 2))],
        compiler_params=pltpu.CompilerParams(vmem_limit_bytes=63 * 1024 * 1024, collective_id=2, has_side_effects=True),
        cost_estimate=cost(14 * seq * d * ff, 40 << 20),
        name="mlp_peer",
    )(dy_rem, dy_loc, *hts, w_up, w_down, w_out, at, at_rem, du, slope)


def tail_kernel(*refs, bt, hd):
    n_in = 13
    hbm, us_ref, refs = refs[:n_in], refs[n_in], refs[n_in + 1:]
    (gx_out, sums_ref, gq_ref, gw_ref, gu_out), refs = refs[:5], refs[5:]
    vm, refs = refs[:n_in], refs[n_in:]
    (z_send, z_recv, sum_src, sum_got, q_keep, q_send, q_recv, w_keep, w_send, w_recv,
     q1_send, q1_recv, w1_send, w1_recv, q2_send, q2_recv, w2_send, w2_recv, u2_recv, gx_ref, gu_ref,
     out_sem, in_sem, send_sem, recv_sem) = refs
    dq, ctx, hk, hs, wt, xl, xr, dhl, dhr, dyl, dyr, ln, uk = vm
    way_to, t, c, xx, yy = partners()
    part = xl.shape[0]
    gr = dq.shape[0] // 4

    loads = [pltpu.make_async_copy(src, dst, in_sem.at[i]) for i, (src, dst) in enumerate(zip(hbm, vm))]
    for i in (0, 4, 6, 8, 11, 3, 2, 1, 9, 10, 5, 7, 12):
        loads[i].start()
    meet(way_to, "cxyz")

    count = [0]

    def send(src, dst, way):
        i = count[0]
        count[0] += 1
        copy = pltpu.make_async_remote_copy(
            src_ref=src, dst_ref=dst, send_sem=send_sem.at[i], recv_sem=recv_sem.at[i],
            device_id=way_to[way], device_id_type=MESH)
        copy.start()
        return copy

    def need(*idx):
        for i in idx:
            loads[i].wait()

    def block(x_ref, dh_ref, b, peer):
        rows = pl.ds(b * bt, bt)
        cols = pl.ds((part if peer else 0) + b * bt, bt)
        dha = dot(dq[:, cols], wt[...], 0, 0).astype(BF).astype(F32)
        dhm = dh_ref[rows, :].astype(F32)
        xh, rstd = normalized(x_ref[rows, :].astype(F32))
        dxh = (dha * ln[0:1, :] + dhm * ln[2:3, :]).astype(BF)
        parts = [dha * xh, dha, dhm * xh, dhm]
        return dxh, jnp.concatenate([jnp.sum(p, axis=0, keepdims=True) for p in parts], axis=0)

    def peer_block(b):
        dxh, s = block(xr, dhr, b, True)
        z_send[b] = dxh
        if b == 0:
            sum_src[0] = s
        else:
            sum_src[0] += s
        return send(z_send.at[b], z_recv.at[b], "z")

    def looped(start, n, f):
        def body(i, _):
            f(i)
            return _

        lax.fori_loop(start, start + n, body, 0)

    def qkv_grad(h_ref, out_ref, g):
        r = dot(dq[pl.ds(pl.multiple_of(g * gr, 128), gr), :], h_ref[...], 1, 0)
        n = r.shape[1] // 4
        for j in range(4):
            out_ref[g, j] = r[:, j * n:(j + 1) * n]

    def out_grad(want, out_ref):
        cx = jnp.concatenate([jnp.where(want == 0, ctx[2 * j * hd:(2 * j + 1) * hd, :], ctx[(2 * j + 1) * hd:(2 * j + 2) * hd, :])
                              for j in range(4)], axis=0)
        r = dot(cx[:, :part], dyl[...], 1, 0) + dot(cx[:, part:], dyr[...], 1, 0)
        m = r.shape[1] // 2
        for j in range(4):
            for k in range(2):
                out_ref[k, j] = r[j * hd:(j + 1) * hd, k * m:(k + 1) * m]

    def first(keep, got, out, k):
        for i in range(2):
            s_idx = 2 * i + 1 - xx if k == 0 else 2 * (1 - yy) + i
            k_idx = 2 * i + xx if k == 0 else 2 * yy + i
            out[i] = keep[s_idx] + got[s_idx]
            got[k_idx] = keep[k_idx] + got[k_idx]

    def second(got, got1, out, k):
        mine, other = (yy, 1 - yy) if k == 0 else (xx, 1 - xx)
        at = (lambda i: 2 * i + xx) if k == 0 else (lambda i: 2 * yy + i)
        out[...] = got[at(other)] + got1[other]
        return got[at(mine)] + got1[mine]

    ways = ("x", "y"), ("y", "x")

    us = [send(us_ref.at[k], u2_recv.at[k], ways[k][1]) for k in range(2)]
    need(0, 4, 6, 8, 11)
    zs = [peer_block(0)]
    q1, q2 = [None] * 4, [None] * 4
    n = gq_ref.shape[0] // 4

    def q_first(g):
        first(q_keep.at[g], q_recv.at[g], q1_send.at[g], g % 2)
        q1[g] = send(q1_send.at[g], q1_recv.at[g], ways[g % 2][0])

    def q_second(g):
        q1[g].wait()
        gq_ref[g * n:(g + 1) * n, :] = second(q_recv.at[g], q1_recv.at[g], q2_send.at[g], g % 2)
        q2[g] = send(q2_send.at[g], q2_recv.at[g], ways[g % 2][1])

    need(3)
    for g in (0, 2):
        looped(g, 2, lambda i: qkv_grad(hs, q_send, i))
        qc = send(q_send.at[pl.ds(g, 2)], q_recv.at[pl.ds(g, 2)], "c")
        if g == 0:
            need(2)
        else:
            zs.append(peer_block(1))
        looped(g, 2, lambda i: qkv_grad(hk, q_keep, i))
        qc.wait()
        q_first(g)
        q_first(g + 1)
    zs.append(peer_block(2))
    q_second(0)
    q_second(1)
    need(1, 9, 10)
    out_grad(1 - c, w_send)
    wc = send(w_send, w_recv, "c")
    out_grad(c, w_keep)
    wc.wait()
    w1 = []
    for k in range(2):
        first(w_keep.at[k], w_recv.at[k], w1_send.at[k], k)
        w1.append(send(w1_send.at[k], w1_recv.at[k], ways[k][0]))

    need(5, 7)

    def own_block(b):
        dxh, s = block(xl, dhl, b, False)
        gx_ref[pl.ds(b * bt, bt), :] = dxh
        sum_src[0] += s

    stores = []

    def grad_x(b):
        zs[b].wait()
        rows = pl.ds(b * bt, bt)
        dxh = gx_ref[rows, :].astype(F32) + z_recv[b].astype(F32)
        xh, rstd = normalized(xl[rows, :].astype(F32))
        dx = rstd * (dxh - jnp.mean(dxh, -1, keepdims=True) - xh * jnp.mean(dxh * xh, -1, keepdims=True))
        gx_ref[rows, :] = (dyl[rows, :].astype(F32) + dx).astype(BF)
        stores.append(pltpu.make_async_copy(gx_ref.at[rows], gx_out.at[rows], out_sem.at[b]))
        stores[-1].start()

    own_block(0)
    q_second(2)
    q_second(3)
    own_block(1)
    grad_x(0)
    own_block(2)
    sums = [send(sum_src.at[0], sum_got.at[0], "z")]
    grad_x(1)

    def sum_next(i, way):
        sums[-1].wait()
        sum_src[i] = sum_src[i - 1] + sum_got[i - 1]
        sums.append(send(sum_src.at[i], sum_got.at[i], way))

    sum_next(1, "c")
    need(12)
    blocks, m = uk.shape[1], uk.shape[3]
    for k in range(2):
        us[k].wait()
        for j in range(blocks):
            gu_ref[:, (2 * j + k) * m:(2 * j + k + 1) * m] = uk[k, j] + u2_recv[k, j]
    stores.append(pltpu.make_async_copy(gu_ref, gu_out, out_sem.at[part // bt]))
    stores[-1].start()
    m = gw_ref.shape[1] // 2
    w2 = []
    for k in range(2):
        w1[k].wait()
        gw_ref[:, k * m:(k + 1) * m] = second(w_recv.at[k], w1_recv.at[k], w2_send.at[k], k)
        w2.append(send(w2_send.at[k], w2_recv.at[k], ways[k][1]))
    sum_next(2, "x")
    for g in (0, 1):
        q2[g].wait()
        gq_ref[g * n:(g + 1) * n, :] += q2_recv[g]
    sum_next(3, "y")
    for g in (2, 3):
        q2[g].wait()
        gq_ref[g * n:(g + 1) * n, :] += q2_recv[g]
    for k in range(2):
        w2[k].wait()
        gw_ref[:, k * m:(k + 1) * m] += w2_recv[k]
    sums[-1].wait()
    sums_ref[...] = sum_src[3] + sum_got[3]
    grad_x(2)
    for v in stores:
        v.wait()


def tail(dq, ctx, h_keep, h_send, w_t, x_loc, x_rem, dhm_loc, dhm_rem, dy_loc, dy_rem, ln, u_keep, u_send, hd, bt=256):
    ins = [dq, ctx, h_keep, h_send, w_t, x_loc, x_rem, dhm_loc, dhm_rem, dy_loc, dy_rem, ln, u_keep]
    part, d = x_loc.shape
    rows = dq.shape[0] // 4
    nb = part // bt
    cols = d // 8
    u_cols = u_keep.shape[0] * u_keep.shape[1] * u_keep.shape[3]
    f = lambda *shape: pltpu.VMEM(shape, F32)
    sds = jax.ShapeDtypeStruct
    scratch = [pltpu.VMEM(v.shape, v.dtype) for v in ins] + [
        pltpu.VMEM((nb, bt, d), BF), pltpu.VMEM((nb, bt, d), BF), f(4, 4, d), f(4, 4, d),
        f(4, 4, rows, cols), f(4, 4, rows, cols), f(4, 4, rows, cols),
        f(2, 4, hd, d // 2), f(2, 4, hd, d // 2), f(2, 4, hd, d // 2),
        f(4, 2, rows, cols), f(4, 2, rows, cols), f(2, 2, hd, d // 2), f(2, 2, hd, d // 2),
        f(4, rows, cols), f(4, rows, cols), f(2, hd, d // 2), f(2, hd, d // 2), f(*u_send.shape), pltpu.VMEM((part, d), BF), f(u_keep.shape[2], u_cols),
        pltpu.SemaphoreType.DMA((nb + 1,)),
        pltpu.SemaphoreType.DMA((len(ins),)), pltpu.SemaphoreType.DMA((32,)), pltpu.SemaphoreType.DMA((32,)),
    ]
    vm = pl.BlockSpec(memory_space=pltpu.VMEM)
    return pl.pallas_call(
        functools.partial(tail_kernel, bt=bt, hd=hd),
        in_specs=[pl.BlockSpec(memory_space=pl.ANY)] * (len(ins) + 1),
        out_specs=[pl.BlockSpec(memory_space=pl.ANY), vm, vm, vm, pl.BlockSpec(memory_space=pl.ANY)],
        out_shape=[sds((part, d), BF), sds((4, d), F32), sds((4 * rows, cols), F32), sds((hd, d), F32), sds((u_keep.shape[2], u_cols), F32)],
        scratch_shapes=scratch,
        compiler_params=pltpu.CompilerParams(vmem_limit_bytes=VMEM_LIMIT, collective_id=0, has_side_effects=True),
        cost_estimate=cost(4e10, 40 << 20),
        name="tail",
    )(*ins, u_send)


def emit_kernel(*refs, n):
    ins, outs, bufs, (sem_in, sem_out) = refs[:n], refs[n:2 * n], refs[2 * n:3 * n], refs[3 * n:]
    get = [pltpu.make_async_copy(ins[i], bufs[i], sem_in.at[i]) for i in range(n)]
    put = [pltpu.make_async_copy(bufs[i], outs[i], sem_out.at[i]) for i in range(n)]
    for v in get:
        v.start()
    for i in range(n):
        get[i].wait()
        put[i].start()
    for v in put:
        v.wait()


def emit(*arrays):
    n = len(arrays)
    hbm = pl.BlockSpec(memory_space=pl.ANY)
    return pl.pallas_call(
        functools.partial(emit_kernel, n=n),
        in_specs=[hbm] * n,
        out_specs=[hbm] * n,
        out_shape=[jax.ShapeDtypeStruct(v.shape, v.dtype) for v in arrays],
        scratch_shapes=[pltpu.VMEM(v.shape, v.dtype) for v in arrays]
        + [pltpu.SemaphoreType.DMA((n,)), pltpu.SemaphoreType.DMA((n,))],
        compiler_params=params(),
        cost_estimate=cost(1e6, 10 << 20),
        name="emit",
    )(*arrays)


def solution(mesh):
    dp = mesh.shape["dp"]
    tp = mesh.shape["tp"]

    def swap_tp(v):
        return lax.ppermute(v, "tp", [(i, i ^ 1) for i in range(tp)])

    def after(v, *deps):
        return lax.optimization_barrier((v,) + deps)[0]

    def local_step(x_loc, dy_loc, ln_params, w_qkv, w_out, w_up, w_down):
        x_loc, dy_loc = x_loc[0], dy_loc[0]
        half, d = x_loc.shape
        seq = half * tp
        heads, hd = w_qkv.shape[1], w_qkv.shape[3]
        me = lax.axis_index("dp")
        c1 = (me % 2).astype(jnp.int32)[None]

        x_rem = swap_tp(x_loc)
        dy_rem = swap_tp(dy_loc)

        w_t = w_qkv.transpose(1, 2, 3, 0).reshape(heads * 3 * hd, d)
        inv_freq = ROPE_BASE ** (-2.0 * jnp.arange(hd // 2, dtype=F32) / hd)
        ang = inv_freq[:, None] * jnp.arange(seq).astype(F32)[None, :]
        cos_t, sin_t = jnp.cos(ang), jnp.sin(ang)

        hm_loc, hk_loc, hs_loc = norm_m(c1, x_loc, ln_params)
        at_loc, du_loc, dhm_loc = mlp_own(hm_loc, dy_loc, w_up, w_down)
        dctx_loc = dot(w_out, dy_loc, 1, 1).astype(BF)

        x_rem = after(x_rem, dhm_loc, dctx_loc, cos_t, sin_t, w_t)
        hm_rem, hk_rem, hs_rem = norm_m(c1, x_rem, ln_params)
        h_a, h_keep, h_send = norm_a(c1, x_loc, x_rem, ln_params)
        qkv_t = dot(w_t, h_a, 1, 1).astype(BF)

        at_rem, slope = mlp_pre(after(hm_rem, qkv_t), w_up)

        dy_rem = after(dy_rem, qkv_t, h_keep, slope)
        d_out, d_stay, uka, ukb, usa, usb, dhm_rem, dctx_rem = mlp_peer(
            dy_rem, dy_loc, (hk_loc, hs_loc, hk_rem, hs_rem), w_up, w_down, w_out, at_loc, at_rem, du_loc, slope)
        dq, ctx, g_wdown, u_send, u_keep = attention(
            qkv_t, dctx_loc, dctx_rem, cos_t, sin_t, (d_out, d_stay), (uka, ukb, usa, usb), hd)
        grad_x, sums, g_wqkv, g_wout, g_wup, g_wdown = emit(*tail(
            dq, ctx, h_keep, h_send, w_t, x_loc, x_rem, dhm_loc, dhm_rem, dy_loc, dy_rem, ln_params, u_keep, u_send, hd), g_wdown)
        grad_x = grad_x[None]
        g_wqkv = g_wqkv.reshape(heads, 3, hd, d // dp).transpose(3, 0, 1, 2)
        return grad_x, sums, g_wqkv, g_wout, g_wup, g_wdown

    return jax.shard_map(
        local_step,
        mesh=mesh,
        in_specs=(P("dp", "tp"), P("dp", "tp"), P(), P(None, "tp"), P("tp"), P(None, "tp"), P("tp")),
        out_specs=(P("dp", "tp"), P(), P("dp", "tp"), P(("tp", "dp")), P("dp", "tp"), P(("tp", "dp"))),
        check_vma=False,
    )
```
